512 devices in a mesh: groups: 2 (over y), expert: 32 (over z, core), tensor: 8 (over x).
Axes of the slice: x: 8, y: 2, z: 16, core: 2. Of those that a mesh axis runs over, the one named last changes fastest.
The devices are a block of a 8x8x16 slice.
Arguments:
- queries: bfloat16 [2048, 4096], P(('groups', 'expert')), parts along dimension 0, may hold values from -200 to 200
- own_kv: bfloat16 [2048, 1024], P(('groups', 'expert')), parts along dimension 0, may hold values from -6 to 6
- prompt_cache: bfloat16 [64, 256, 1024], P(('groups', 'expert'), 'tensor'), parts along dimension 0, may hold values from -8 to 8
- prompt_len: int32 [64], P(('groups', 'expert')), parts along dimension 0, may hold values from 2 to 256
- token_prompt: int32 [2048], P(('groups', 'expert')), parts along dimension 0, may hold values from 0 to 31, as said below
- residual: bfloat16 [2048, 2048], P(('groups', 'expert')), parts along dimension 0, may hold values from -3 to 3
- out_weight: bfloat16 [4096, 2048], P('tensor', 'expert'), may hold values from -0.1875 to 0.1875
- route_ids: int32 [2048, 8], P(('groups', 'expert')), parts along dimension 0, may hold values from 0 to 63, all different within a row; in each aligned block of 32 rows (0 to 31, 32 to 63, ...) at most 6 rows name the same one
- route_weights: float32 [2048, 8], P(('groups', 'expert')), parts along dimension 0, may hold values from 0.05 to 0.3
- w_gate: bfloat16 [64, 2048, 1024], P('expert', None, 'tensor'), may hold values from -0.125 to 0.125
- w_up: bfloat16 [64, 2048, 1024], P('expert', None, 'tensor'), may hold values from -0.125 to 0.125
- w_down: bfloat16 [64, 1024, 2048], P('expert', 'tensor'), may hold values from -0.25 to 0.25
Outputs:
- mixed: bfloat16 [2048, 2048], P(('groups', 'expert'), 'tensor'), parts along dimension 0
The draws below stay inside these ranges and needn't reach their ends.
There are 2 independent parts, one for each index of `groups`. The reference program is written for one: setup_inputs(seed, part) draws one part's arguments, and reference() takes and returns one part's arrays. A program takes and returns all parts, laid end to end along the dimension named above; an argument that names none is the same for every part. Nothing has to cross between parts.
Inputs may be any that keep to these rules, and one draw needn't show every extreme that they name: `token_prompt`: each index of the expert axis holds 2 tokens of each of 16 prompts and none of the others; each prompt has tokens on exactly 16 indices. `route_ids`: A row names distinct experts. Within the 32 rows of one index of the expert axis no expert is named more than 6 times, and in some of these blocks one is named exactly 6 times.
All inputs are finite; a program needn't handle non-finite values.
Results may differ from the reference program's by a relative error of at most 0.015.
Values may be sent and summed in bfloat16 or wider, within the bound.
No kernel may reach another device: no remote copies, remote signals or barrier semaphores. Data moves between devices by JAX's collectives and lax.ppermute only.
A program may use at most 64 MiB of HBM per device.

```python
import math
import jax
import jax.numpy as jnp
import numpy as np
from jax import lax

D = 2048
H = 32
KVH = 4
HD = 128
FF = 1024
TOPK = 8
P_SIZE = 256
TOK_DEV = 32
E = 64
NPROMPT = 32
FAN = 16
TOKENS = 1024
CAP = 6
FF_DEV = 128
N_EXPERT = 32
N_TENSOR = 8


def prompt_table(key):
    base = jax.random.fold_in(key, 11)
    key_one, key_two, key_three = jax.random.split(base, 3)
    order_a = jax.random.permutation(key_one, NPROMPT)
    order_b = jax.random.permutation(key_two, NPROMPT)
    inverse_a = jnp.argsort(order_a)
    offsets = jnp.tile(jnp.arange(TOK_DEV, dtype=jnp.int32) % FAN, (NPROMPT, 1))
    offsets = jax.random.permutation(key_three, offsets, axis=1, independent=True)
    chosen = (order_b[:, None] + offsets) % NPROMPT
    return inverse_a[chosen].reshape(-1).astype(jnp.int32)


def cache_table(key):
    base = jax.random.fold_in(key, 23)
    key_main = jax.random.fold_in(base, 0)
    cache_vals = jnp.clip(jax.random.normal(key_main, (NPROMPT, P_SIZE, 2 * KVH * HD), jnp.float32), -6.0, 6.0)
    return cache_vals


def draw_token_prompt(key, part):
    return prompt_table(key)


def draw_prompt_cache(key, part):
    return cache_table(key).astype(jnp.bfloat16)


def draw_queries(key, part):
    base = jax.random.fold_in(key, 37)
    key_main = jax.random.fold_in(base, 0)
    values = jnp.clip(jax.random.normal(key_main, (TOKENS, H * HD), jnp.float32), -6.0, 6.0)
    return values.astype(jnp.bfloat16)


def touch_ends(result, key, smallest, high):
    spot = [jax.random.randint(jax.random.fold_in(key, axis), (), 0, length) for axis, length in enumerate(result.shape)]
    main_axis = result.shape.index(max(result.shape))
    neighbour = spot[:main_axis] + [(spot[main_axis] + 1) % result.shape[main_axis]] + spot[main_axis + 1:]
    return result.at[tuple(spot)].set(smallest).at[tuple(neighbour)].set(high)


def with_spikes(values, own_key, source, target, parts, factor):
    owner, partner = [(jnp.arange(values.shape[axis_at]) // (values.shape[axis_at] // parts)).reshape([-1 if axis == axis_at else 1 for axis in range(values.ndim)]) for axis_at in (source, target)]
    chosen = jax.random.permutation(own_key, parts)[partner]
    strong = (owner == chosen) | (owner == (partner + parts // 2) % parts)
    return jnp.where(strong, factor * values, values)


def shard_levels(key, extent, cuts, low, top_value):
    level, own = 1.0, jax.random.fold_in(key, 6)
    for axis_at, parts in cuts:
        draws = jnp.exp(jax.random.uniform(jax.random.fold_in(own, axis_at), (parts,), jnp.float32, low / len(cuts), top_value / len(cuts)))
        level = level * jnp.repeat(draws, extent[axis_at] // parts).reshape([-1 if axis == axis_at else 1 for axis in range(len(extent))])
    return level


def assign_block(own_key, own, number, rows, count, top, limit, slope):
    order = jax.random.permutation(own_key, count)
    heavy_load, common = portions_of(count, rows * top, limit, slope, True), portions_of(count, rows * top, limit, slope, False)
    places = jnp.arange(count)

    def named(sizes, offset_by):
        used = int((sizes > 0).sum())
        fixed = max(1, used // 4)
        moved = fixed + (places - fixed + offset_by * (used - fixed)) % max(1, count - fixed)
        return jnp.zeros((count,), jnp.int32).at[order[jnp.where(places < fixed, places, moved)]].set(jnp.asarray(sizes, jnp.int32))

    sizes = jnp.where(number % 4 == 0, named(heavy_load, number // 4), named(common, number - number // 4 - 1))
    mixed = jax.random.permutation(jax.random.fold_in(own, 3), count)
    giver, sink = mixed[0:count // 2 * 2:2], mixed[1:count // 2 * 2:2]
    room = jnp.minimum(sizes[giver] - 1, limit - sizes[sink]) // 2
    room = jnp.where((giver == order[0]) | (sink == order[0]) | (sizes[sink] == 0), 0, jnp.maximum(room, 0))
    moved = jax.random.randint(jax.random.fold_in(own, 4), (count // 2,), 0, 1 << 20) % (room + 1)
    sizes = sizes.at[giver].add(-moved).at[sink].add(moved)
    labels = jnp.searchsorted(jnp.cumsum(sizes), jnp.arange(rows * top), side="right").astype(jnp.int32)
    grid = labels.reshape(top, rows).T
    grid = grid[jax.random.permutation(jax.random.fold_in(own, 1), rows)]
    offset_by = jax.random.randint(jax.random.fold_in(own, 2), (rows, 1), 0, top)
    return jnp.take_along_axis(grid, (jnp.arange(top)[None, :] + offset_by) % top, axis=1)


def portions_of(number_of, total, reach, slope, full):
    loads = [(1 << 20) // math.isqrt(grade ** slope) + 1 for grade in range(1, number_of + 1)]
    largest = reach if full else min(reach, max(-(-total // number_of), total * loads[0] // sum(loads)))
    least = 1 if total - largest >= number_of - 1 else 0
    holding, rest = [largest] + [least] * (number_of - 1), total - largest - least * (number_of - 1)
    while rest > 0:
        free = [i for i in range(1, number_of) if holding[i] < largest] or [i for i in range(1, number_of) if holding[i] < reach]
        mass, remaining = sum([loads[i] for i in free]), rest
        for i in free:
            extra = min(reach - holding[i], max(1, remaining * loads[i] // mass), rest)
            holding[i] = holding[i] + extra
            rest = rest - extra
    return np.array(holding)


def normal_values(stream_key, shape, deviation, limit, cuts=(), held_as=jnp.bfloat16):
    result = jax.random.normal(stream_key, shape, jnp.float32) * deviation
    if len(cuts) > 0:
        result = shard_levels(stream_key, shape, cuts, -0.22, 0.18) * result
    return jnp.clip(result, min=-limit, max=limit).astype(held_as)


def noise_with(stream_key, dims, deviation, reach, cuts, heavy, kind=jnp.bfloat16):
    values = deviation * jax.random.normal(stream_key, dims, jnp.float32)
    if cuts:
        values = values * shard_levels(stream_key, dims, cuts, -0.22, 0.18)
    return jnp.clip(with_spikes(values, jax.random.fold_in(stream_key, 3), *heavy), -reach, reach).astype(kind)


def setup_inputs(seed: int = 0, part: int = 0) -> dict:
    arg_keys = jax.random.split(jax.random.key(seed), 13)
    part_keys = jax.random.split(jax.random.fold_in(arg_keys[12], part), 13)
    queries = draw_queries(jax.random.fold_in(jax.random.fold_in(arg_keys[12], part), 71), part)
    own_kv = normal_values(part_keys[1], (TOKENS, 2 * KVH * HD), 1.0, 6.0, ((0, 32),))
    prompt_cache = draw_prompt_cache(jax.random.fold_in(jax.random.fold_in(arg_keys[12], part), 71), part)
    prompt_len = touch_ends(jax.random.randint(part_keys[3], (NPROMPT,), 2, P_SIZE + 1), jax.random.fold_in(part_keys[3], 1), 2, P_SIZE).astype(jnp.int32)
    token_prompt = draw_token_prompt(jax.random.fold_in(jax.random.fold_in(arg_keys[12], part), 71), part)
    residual = normal_values(part_keys[5], (TOKENS, D), 0.5, 3.0, ((0, 32),))
    out_weight = noise_with(arg_keys[6], (H * HD, D), (H * HD) ** -0.5, 0.1875, ((0, 8), (1, 32)), (0, 1, 32, 2.75))
    route_ids_keys = jax.random.split(jax.random.fold_in(part_keys[7], 1), TOKENS // TOK_DEV)
    route_ids_turns = jax.random.permutation(jax.random.fold_in(part_keys[7], 3), TOKENS // TOK_DEV)
    route_ids = jax.vmap(lambda own, number: assign_block(jax.random.fold_in(part_keys[7], 2), own, number, TOK_DEV, E, TOPK, CAP, 2))(route_ids_keys, route_ids_turns).reshape((TOKENS, TOPK))
    route_weights = jnp.clip(0.05 + 0.25 * jax.random.uniform(part_keys[8], (TOKENS, TOPK), jnp.float32) ** shard_levels(part_keys[8], (TOKENS, TOPK), ((0, 32),), -0.2, 0.2), 0.05, 0.3)
    w_gate = normal_values(arg_keys[9], (E, D, FF), D ** -0.5, 0.125, ((0, 32), (2, 8)))
    w_up = normal_values(arg_keys[10], (E, D, FF), D ** -0.5, 0.125, ((0, 32), (2, 8)))
    w_down = noise_with(arg_keys[11], (E, FF, D), FF ** -0.5, 0.25, ((0, 32), (1, 8)), (1, 2, 8, 2.0))
    return dict(queries=queries, own_kv=own_kv, prompt_cache=prompt_cache, prompt_len=prompt_len, token_prompt=token_prompt, residual=residual, out_weight=out_weight, route_ids=route_ids, route_weights=route_weights, w_gate=w_gate, w_up=w_up, w_down=w_down)


MASKED_SCORE = -1e30


def prompt_attention(inputs):
    query_rows, own_keys, own_values, key_rows, value_rows, length = inputs
    score_scale = HD ** -0.5
    score_rows = jnp.einsum('tgjd,pgd->tgjp', query_rows, key_rows, precision=lax.Precision.HIGHEST) * score_scale
    visible = jnp.arange(P_SIZE) < length
    score_rows = jnp.where(visible, score_rows, MASKED_SCORE)
    own_score = jnp.einsum('tgjd,tgd->tgj', query_rows, own_keys, precision=lax.Precision.HIGHEST) * score_scale
    top_score = jnp.maximum(jnp.max(score_rows, -1), own_score)
    weights = jnp.where(visible, jnp.exp(score_rows - top_score[..., None]), 0.0)
    own_weight = jnp.exp(own_score - top_score)
    weight_sum = jnp.sum(weights, -1) + own_weight
    value_sum = jnp.einsum('tgjp,pgd->tgjd', weights, value_rows, precision=lax.Precision.HIGHEST)
    value_sum = value_sum + own_weight[..., None] * own_values[:, :, None, :]
    return value_sum / weight_sum[..., None]


def expert_layer(inputs):
    rows_in, gate_weight, up_weight, down_weight = inputs
    gate_proj = jnp.dot(rows_in, gate_weight, preferred_element_type=jnp.float32)
    up_proj = jnp.dot(rows_in, up_weight, preferred_element_type=jnp.float32)
    activated = (jax.nn.silu(gate_proj) * up_proj).astype(jnp.bfloat16)
    row_count = rows_in.shape[0]
    act_blocks = activated.astype(jnp.float32).reshape(row_count, N_TENSOR, FF_DEV)
    down_blocks = down_weight.astype(jnp.float32).reshape(N_TENSOR, FF_DEV, D)
    partials = jnp.einsum('rnf,nfd->nrd', act_blocks, down_blocks, precision=lax.Precision.HIGHEST)
    partials = partials.astype(jnp.bfloat16).astype(jnp.float32)
    return jnp.sum(partials, 0).astype(jnp.bfloat16)


def reference(queries, own_kv, prompt_cache, prompt_len, token_prompt, residual, out_weight, route_ids, route_weights, w_gate, w_up, w_down):
    group_size = H // KVH
    half_cols = KVH * HD
    order = jnp.argsort(token_prompt, stable=True).astype(jnp.int32)
    grouped = order.reshape(NPROMPT, TOK_DEV)
    query_all = queries.astype(jnp.float32).reshape(TOKENS, KVH, group_size, HD)
    own_all = own_kv.astype(jnp.float32)
    own_keys = own_all[:, :half_cols].reshape(TOKENS, KVH, HD)
    own_values = own_all[:, half_cols:].reshape(TOKENS, KVH, HD)
    cache_all = prompt_cache.astype(jnp.float32)
    key_rows = cache_all[:, :, :half_cols].reshape(NPROMPT, P_SIZE, KVH, HD)
    value_rows = cache_all[:, :, half_cols:].reshape(NPROMPT, P_SIZE, KVH, HD)
    results = lax.map(prompt_attention, (query_all[grouped], own_keys[grouped], own_values[grouped], key_rows, value_rows, prompt_len))
    attn = jnp.zeros((TOKENS, H * HD), jnp.float32).at[order].set(results.reshape(TOKENS, H * HD)).astype(jnp.bfloat16)
    attn_out = jnp.dot(attn, out_weight, preferred_element_type=jnp.float32)
    hidden = (residual.astype(jnp.float32) + attn_out).astype(jnp.bfloat16)

    flat_ids = route_ids.reshape(N_EXPERT, TOK_DEV * TOPK)
    expert_marks = (flat_ids[..., None] == jnp.arange(E, dtype=jnp.int32)).astype(jnp.int32)
    slot_index = jnp.sum((jnp.cumsum(expert_marks, 1) - expert_marks) * expert_marks, -1).astype(jnp.int32)
    destination = (flat_ids * CAP + slot_index).astype(jnp.int32)
    source_rows = (jnp.arange(TOK_DEV * TOPK) // TOPK).astype(jnp.int32)
    block_ids = jnp.arange(N_EXPERT, dtype=jnp.int32)[:, None]
    hidden_blocks = hidden.reshape(N_EXPERT, TOK_DEV, D)
    buffers = jnp.zeros((N_EXPERT, E * CAP, D), jnp.bfloat16)
    buffers = buffers.at[block_ids, destination].set(hidden_blocks[block_ids, source_rows[None, :]])
    expert_in = buffers.reshape(N_EXPERT, E, CAP, D).transpose(1, 0, 2, 3).reshape(E, N_EXPERT * CAP, D)
    expert_out = lax.map(expert_layer, (expert_in, w_gate, w_up, w_down)).reshape(E, N_EXPERT, CAP, D)
    picked = expert_out[flat_ids, block_ids, slot_index].reshape(TOKENS, TOPK, D).astype(jnp.float32)
    expert_mix = jnp.sum(route_weights[:, :, None] * picked, 1)
    return (hidden.astype(jnp.float32) + expert_mix).astype(jnp.bfloat16)
```

```python
import jax
import jax.numpy as jnp
from jax import lax
from jax.sharding import PartitionSpec as P

HD = 128
MASKED_SCORE = -1e30


def exchange(tiles, axis):
    return lax.all_to_all(tiles, axis, split_axis=0, concat_axis=0, tiled=True)


def local(
    queries,
    own_kv,
    prompt_cache,
    prompt_len,
    token_prompt,
    residual,
    out_weight,
    route_ids,
    route_weights,
    w_gate,
    w_up,
    w_down,
):
    f32, bf16 = jnp.float32, jnp.bfloat16
    n_e = lax.axis_size("expert")
    n_x = lax.axis_size("tensor")
    pos_x = lax.axis_index("tensor")
    tokens = queries.shape[0]
    half_cols = own_kv.shape[1] // 2
    kv_heads = half_cols // HD
    head_count = queries.shape[1] // HD
    group_size = head_count // kv_heads
    heads_here = head_count // n_x
    q_cols = heads_here * HD
    per_prompt = tokens // (n_e // 2)
    block_len = prompt_cache.shape[1]
    model_width = residual.shape[1]
    col_width = model_width // n_x

    experts_here = w_gate.shape[0]
    keep = pos_x % experts_here
    give = 1 - keep
    swap = [(i, i ^ 1) for i in range(n_x)]
    up_pair = jnp.stack(
        [
            lax.dynamic_index_in_dim(w_gate, give, 0, keepdims=False),
            lax.dynamic_index_in_dim(w_up, give, 0, keepdims=False),
        ]
    )
    got_up = lax.ppermute(up_pair, "tensor", swap)
    got_down = lax.ppermute(
        lax.dynamic_index_in_dim(w_down, give, 0, keepdims=False), "tensor", swap
    )
    all_out = lax.all_gather(out_weight.T, "expert", axis=0, tiled=True)

    kv_pos = (pos_x * heads_here) // group_size
    payload = jnp.concatenate(
        [
            lax.dynamic_slice_in_dim(queries, pos_x * q_cols, q_cols, 1),
            lax.dynamic_slice_in_dim(own_kv, kv_pos * HD, HD, 1),
            lax.dynamic_slice_in_dim(own_kv, half_cols + kv_pos * HD, HD, 1),
        ],
        1,
    )
    earlier = jnp.arange(tokens)[None, :] < jnp.arange(tokens)[:, None]
    same = token_prompt[:, None] == token_prompt[None, :]
    rank = jnp.sum((same & earlier).astype(jnp.int32), 1)
    place = token_prompt * per_prompt + rank
    rows = n_e * per_prompt
    pick = (jnp.arange(rows)[:, None] == place[None, :]).astype(bf16)
    sent = jnp.dot(pick, payload, preferred_element_type=f32).astype(bf16)
    got = exchange(sent.reshape(n_e, per_prompt, q_cols + 2 * HD), "expert")
    got = got.reshape(rows, q_cols + 2 * HD)

    cache = prompt_cache[0].reshape(block_len, 2, kv_heads, HD)
    by_head = jnp.transpose(cache, (2, 0, 1, 3)).reshape(kv_heads, block_len, 2 * HD)
    by_head = jnp.repeat(by_head, n_x // kv_heads, axis=0)
    cache_all = exchange(by_head, "tensor").reshape(n_x * block_len, 2 * HD)
    keys, values = cache_all[:, :HD], cache_all[:, HD:]

    q_rows = got[:, :q_cols].reshape(rows, heads_here, HD)
    k_own = got[:, q_cols : q_cols + HD].astype(f32)
    v_own = got[:, q_cols + HD :].astype(f32)
    scale = HD ** (-0.5)
    scores = jnp.einsum("rhd,pd->rhp", q_rows, keys, preferred_element_type=f32) * scale
    own = jnp.sum(q_rows.astype(f32) * k_own[:, None, :], -1) * scale
    inside = jnp.arange(n_x * block_len) < prompt_len[0]
    scores = jnp.where(inside, scores, MASKED_SCORE)
    top = jnp.maximum(jnp.max(scores, -1), own)
    weights = jnp.where(inside, jnp.exp(scores - top[..., None]), 0.0)
    own_weight = jnp.exp(own - top)
    total = jnp.sum(weights, -1) + own_weight
    mix = jnp.einsum("rhp,pd->rhd", weights.astype(bf16), values, preferred_element_type=f32)
    mix = mix + own_weight[..., None] * v_own[:, None, :]
    attn = (mix / total[..., None]).astype(bf16)

    back = exchange(attn.reshape(n_e, per_prompt, q_cols), "expert").reshape(rows, q_cols)
    attn_home = lax.dot_general(
        pick, back, (((0,), (0,)), ((), ())), preferred_element_type=f32
    ).astype(bf16)
    partial = lax.dot_general(
        attn_home, all_out, (((1,), (1,)), ((), ())), preferred_element_type=f32
    ).astype(bf16)
    partial = jnp.transpose(partial.reshape(tokens, n_x, col_width), (1, 0, 2))
    head_total = jnp.sum(exchange(partial, "tensor").astype(f32), 0)
    resid_cols = lax.dynamic_slice_in_dim(residual, pos_x * col_width, col_width, 1)
    hidden = (resid_cols.astype(f32) + head_total).astype(bf16)

    experts = experts_here * n_e
    picks = route_ids.shape[1]
    capacity = min(tokens, 3 * tokens * picks // (2 * experts))
    hit = route_ids[:, :, None] == jnp.arange(experts, dtype=jnp.int32)
    marks = jnp.any(hit, 1)
    mark_weight = jnp.sum(jnp.where(hit, route_weights[:, :, None], 0.0), 1)
    slot = jnp.dot(
        earlier.astype(bf16), marks.astype(bf16), preferred_element_type=f32
    ).astype(jnp.int32)
    slot = jnp.where(marks, slot, -1)
    chosen = slot[:, :, None] == jnp.arange(capacity, dtype=jnp.int32)
    send_rows = chosen.reshape(tokens, experts * capacity).astype(bf16)
    mix_rows = (chosen * mark_weight[:, :, None]).reshape(tokens, experts * capacity)

    outgoing = lax.dot_general(
        send_rows, hidden, (((0,), (0,)), ((), ())), preferred_element_type=f32
    ).astype(bf16)
    arrived = exchange(outgoing.reshape(n_e, experts_here, capacity, col_width), "expert")
    by_expert = jnp.transpose(arrived, (1, 0, 2, 3)).reshape(
        experts_here, n_e * capacity, col_width
    )
    by_dest = jnp.tile(by_expert, (n_x // experts_here, 1, 1))
    rows_in = exchange(by_dest, "tensor")

    own_gate = lax.dynamic_index_in_dim(w_gate, keep, 0, keepdims=False)
    own_up = lax.dynamic_index_in_dim(w_up, keep, 0, keepdims=False)
    own_down = lax.dynamic_index_in_dim(w_down, keep, 0, keepdims=False)

    def project(weight):
        return jnp.einsum(
            "srd,sdf->rf",
            rows_in,
            weight.reshape(n_x, col_width, weight.shape[1]),
            preferred_element_type=f32,
        )

    def act_of(gate, up):
        return (jax.nn.silu(gate) * up).astype(bf16)

    act_own = act_of(project(own_gate), project(own_up))
    act_got = act_of(project(got_up[0]), project(got_up[1]))
    out = jnp.dot(act_own, own_down, preferred_element_type=f32) + jnp.dot(
        act_got, got_down, preferred_element_type=f32
    )
    out = jnp.transpose(out.astype(bf16).reshape(-1, n_x, col_width), (1, 0, 2))
    parts = exchange(out, "tensor")
    parts = parts.reshape(n_x // experts_here, experts_here, n_e, capacity, col_width)
    summed = jnp.sum(parts.astype(f32), 0).astype(bf16)
    returned = exchange(jnp.transpose(summed, (1, 0, 2, 3)), "expert")
    expert_mix = jnp.dot(
        mix_rows,
        returned.reshape(experts * capacity, col_width).astype(f32),
        precision=lax.Precision.HIGHEST,
    )
    return (hidden.astype(f32) + expert_mix).astype(bf16)


def solution(mesh):
    whole = ("groups", "expert")
    return jax.shard_map(
        local,
        mesh=mesh,
        in_specs=(
            P(whole, None),
            P(whole, None),
            P(whole, "tensor", None),
            P(whole),
            P(whole),
            P(whole, None),
            P("tensor", "expert"),
            P(whole, None),
            P(whole, None),
            P("expert", None, "tensor"),
            P("expert", None, "tensor"),
            P("expert", "tensor", None),
        ),
        out_specs=P(whole, "tensor"),
        check_vma=False,
    )
```

```python
import jax
import jax.numpy as jnp
from jax import lax
from jax.experimental import pallas as pl
from jax.experimental.pallas import tpu as pltpu
from jax.sharding import Mesh
from jax.sharding import PartitionSpec as P

HD = 128
CORES = 2
EXPERT = ("chip", "core")
MASKED_SCORE = -1e30
f32, bf16, i32 = jnp.float32, jnp.bfloat16, jnp.int32


def exchange(tiles, axis):
    return lax.all_to_all(tiles, axis, split_axis=0, concat_axis=0, tiled=True)


def from_chip(x, shift):
    n = lax.axis_size("chip")
    return lax.ppermute(x, "chip", [(i, (i - shift) % n) for i in range(n)])


def other_core(x):
    return lax.ppermute(x, "core", [(0, 1), (1, 0)])


def count_earlier(marks):
    n = marks.shape[-1]
    before = (jnp.arange(n)[:, None] < jnp.arange(n)[None, :]).astype(bf16)
    return jnp.dot(marks.astype(bf16), before, preferred_element_type=f32).astype(i32)


def pick_rows(index, rows):
    chosen = (index[:, None] == jnp.arange(rows.shape[0], dtype=i32)).astype(bf16)
    return jnp.dot(chosen, rows, preferred_element_type=f32).astype(bf16)


def projection_kernel(at, attn, mine, theirs, out):
    chips = mine.shape[0]
    quarter = chips // 4
    first = at[1] == 0
    rows = attn[...]
    per_out = out.shape[2] // (2 * mine.shape[1])
    for dest in range(out.shape[0]):
        blocks = []
        for near in range(per_out):
            m = lax.rem(dest * per_out + near + chips - at[0], chips)
            k, kind = lax.div(m, 4), lax.rem(m, 4)
            place = jnp.where(kind == 1, quarter + k, k)
            place = jnp.where(kind == 2, 3 * quarter + k, place)
            place = jnp.where(kind == 3, 2 * quarter + lax.rem(k + 1, quarter), place)
            a, b = mine[place], theirs[place]
            blocks += [jnp.where(first, a, b), jnp.where(first, b, a)]
        weight = jnp.concatenate(blocks, 0)
        out[dest] = lax.dot_general(
            rows, weight, (((1,), (1,)), ((), ())), preferred_element_type=f32
        ).astype(bf16)


def project_out(chip, core, attn, mine, theirs, n_x, col_width):
    vmem = pl.BlockSpec(memory_space=pltpu.VMEM)
    flops = 2 * attn.shape[0] * 2 * mine.size
    return pl.pallas_call(
        projection_kernel,
        out_shape=jax.ShapeDtypeStruct((n_x, attn.shape[0], col_width), bf16),
        in_specs=[pl.BlockSpec(memory_space=pltpu.SMEM), vmem, vmem, vmem],
        out_specs=vmem,
        cost_estimate=pl.CostEstimate(
            flops=flops, bytes_accessed=4 * mine.size, transcendentals=0
        ),
        compiler_params=pltpu.CompilerParams(vmem_limit_bytes=8 << 20),
        name="project_out",
    )(jnp.stack([chip, core]).astype(i32), attn, mine, theirs)


def expert_kernel(keep, rows, gate, up, down, got_up, got_down, out):
    n_x, count, col_width = rows.shape
    ff = gate.shape[2]
    total = jnp.zeros((count, 4 * ff), f32)
    for s in range(n_x):
        at = pl.ds(s * col_width, col_width)
        weight = jnp.concatenate(
            [gate[0, at, :], got_up[0, at, :], up[0, at, :], got_up[1, at, :]], 1
        )
        total = total + jnp.dot(rows[s], weight, preferred_element_type=f32)
    gates, ups = total[:, : 2 * ff], total[:, 2 * ff :]
    act = (gates / (1.0 + jnp.exp(-gates)) * ups).astype(bf16)
    for d in range(n_x):
        at = pl.ds(d * col_width, col_width)
        weight = jnp.concatenate([down[0, :, at], got_down[:, at]], 0)
        out[d] = jnp.dot(act, weight, preferred_element_type=f32).astype(bf16)


def run_expert(keep, rows, gate, up, down, got_up, got_down):
    def whole(x):
        return pl.BlockSpec(x.shape, lambda i, k: (0,) * x.ndim)

    def kept(x):
        return pl.BlockSpec((1, *x.shape[1:]), lambda i, k: (k[0], 0, 0))

    flops = 2 * rows.size * got_up.shape[2] * 4 + 2 * rows.size * got_down.shape[0] * 2
    moved = 2 * (2 * rows.size + got_up.size + got_down.size) + 3 * gate.size
    return pl.pallas_call(
        expert_kernel,
        out_shape=jax.ShapeDtypeStruct(rows.shape, bf16),
        grid_spec=pltpu.PrefetchScalarGridSpec(
            num_scalar_prefetch=1,
            grid=(1,),
            in_specs=[
                whole(rows),
                kept(gate),
                kept(up),
                kept(down),
                whole(got_up),
                whole(got_down),
            ],
            out_specs=whole(rows),
        ),
        cost_estimate=pl.CostEstimate(
            flops=flops, bytes_accessed=moved, transcendentals=rows.shape[1] * 2 * HD
        ),
        compiler_params=pltpu.CompilerParams(vmem_limit_bytes=16 << 20),
        name="run_expert",
    )(jnp.reshape(keep, (1,)).astype(i32), rows, gate, up, down, got_up, got_down)


def layer(
    queries,
    own_kv,
    prompt_cache,
    prompt_len,
    token_prompt,
    residual,
    out_weight,
    route_ids,
    route_weights,
    w_gate,
    w_up,
    w_down,
):
    n_e = lax.axis_size(EXPERT)
    n_x = lax.axis_size("tensor")
    chips = lax.axis_size("chip")
    pos_x = lax.axis_index("tensor")
    chip = lax.axis_index("chip")
    core = lax.axis_index("core")
    pos_e = chip * CORES + core
    tokens = queries.shape[0]
    half_cols = own_kv.shape[1] // 2
    kv_heads = half_cols // HD
    head_count = queries.shape[1] // HD
    group_size = head_count // kv_heads
    heads_here = head_count // n_x
    q_cols = heads_here * HD
    per_prompt = tokens // (n_e // 2)
    block_len = prompt_cache.shape[1]
    model_width = residual.shape[1]
    col_width = model_width // n_x
    picks = route_ids.shape[1]
    experts_here = w_gate.shape[0]
    experts = experts_here * n_e
    capacity = min(tokens, 3 * tokens * picks // (2 * experts))

    cache = prompt_cache[0].reshape(block_len, 2, kv_heads, HD)
    by_head = jnp.transpose(cache, (2, 0, 1, 3)).reshape(kv_heads, block_len, 2 * HD)
    by_head = jnp.repeat(by_head, n_x // kv_heads, axis=0)
    cache_all = exchange(by_head, "tensor")
    cache_all = cache_all.reshape(n_x * block_len, 2 * HD)

    w_own = out_weight.T
    far = from_chip(w_own, chips // 2)
    ahead = from_chip(w_own, chips // 4)
    behind = from_chip(w_own, -(chips // 4))
    quarter = jnp.stack([w_own, ahead, far, behind])
    next_one = from_chip(quarter, 1)
    last_one = from_chip(quarter, -1)
    next_two = from_chip(quarter[:2], 2)
    last_two = from_chip(jnp.stack([quarter[3], quarter[0]]), -2)
    mine = jnp.concatenate([quarter, next_one, last_one, next_two, last_two])
    theirs = other_core(mine)

    kv_pos = (pos_x * heads_here) // group_size
    payload = jnp.concatenate(
        [
            lax.dynamic_slice_in_dim(queries, pos_x * q_cols, q_cols, 1),
            lax.dynamic_slice_in_dim(own_kv, kv_pos * HD, HD, 1),
            lax.dynamic_slice_in_dim(own_kv, half_cols + kv_pos * HD, HD, 1),
            lax.dynamic_slice_in_dim(residual, pos_x * col_width, col_width, 1),
        ],
        1,
    )
    width = payload.shape[1]
    same = token_prompt[:, None] == token_prompt[None, :]
    earlier = jnp.arange(tokens)[None, :] < jnp.arange(tokens)[:, None]
    rank = jnp.sum((same & earlier).astype(i32), 1)
    place = token_prompt * per_prompt + rank
    rows = n_e * per_prompt
    pick = (jnp.arange(rows)[:, None] == place[None, :]).astype(bf16)
    sent = jnp.dot(pick, payload, preferred_element_type=f32).astype(bf16)
    table = jnp.concatenate([token_prompt, route_ids.reshape(-1)]).astype(bf16)
    entries = table.shape[0]
    table_cols = -(-entries // (per_prompt * HD)) * HD
    table = jnp.pad(table, (0, per_prompt * table_cols - entries))
    table = jnp.broadcast_to(
        table.reshape(1, per_prompt, table_cols), (n_e, per_prompt, table_cols)
    )
    sent = jnp.concatenate([sent.reshape(n_e, per_prompt, width), table], 2)
    sent, cache_all = lax.optimization_barrier((sent, cache_all))
    keys, values = cache_all[:, :HD], cache_all[:, HD:]
    got = exchange(sent, EXPERT)
    table = got[:, :, width:].reshape(n_e, per_prompt * table_cols)[:, :entries].astype(i32)
    prompts = table[:, :tokens]
    routes = table[:, tokens:].reshape(n_e, tokens, picks)

    owner = jnp.arange(n_e, dtype=i32)
    holds = jnp.any(prompts[None, :, :] == owner[:, None, None], -1)
    order = count_earlier(holds)
    peers = prompts[:, :, None] == prompts[:, None, :]
    rank_all = jnp.sum((peers & earlier[None]).astype(i32), 2)
    block_order = jnp.sum(
        jnp.where(prompts[:, :, None] == owner, order.T[:, None, :], 0), 2
    )
    source = jnp.where(prompts % CORES == core, 0, chips) + prompts // CORES
    source = source * tokens + block_order * per_prompt + rank_all

    own_holds = jnp.any(prompts == pos_e, 1)
    own_order = count_earlier(own_holds[None])[0]
    slot_here = own_order[:, None] * per_prompt + jnp.arange(per_prompt, dtype=i32)
    slot_here = jnp.where(own_holds[:, None], slot_here, -1).reshape(rows)
    compact = (jnp.arange(tokens, dtype=i32)[:, None] == slot_here[None, :]).astype(bf16)
    got = jnp.dot(
        compact, got[:, :, :width].reshape(rows, width), preferred_element_type=f32
    ).astype(bf16)

    q_rows = got[:, :q_cols].reshape(tokens, heads_here, HD)
    k_own = got[:, q_cols : q_cols + HD].astype(f32)
    v_own = got[:, q_cols + HD : q_cols + 2 * HD].astype(f32)
    resid = got[:, q_cols + 2 * HD :].astype(f32)
    scale = HD ** (-0.5)
    scores = jnp.einsum("rhd,pd->rhp", q_rows, keys, preferred_element_type=f32) * scale
    own = jnp.sum(q_rows.astype(f32) * k_own[:, None, :], -1) * scale
    inside = jnp.arange(n_x * block_len) < prompt_len[0]
    scores = jnp.where(inside, scores, MASKED_SCORE)
    top = jnp.maximum(jnp.max(scores, -1), own)
    weights = jnp.where(inside, jnp.exp(scores - top[..., None]), 0.0)
    own_weight = jnp.exp(own - top)
    total = jnp.sum(weights, -1) + own_weight
    mix = jnp.einsum("rhp,pd->rhd", weights.astype(bf16), values, preferred_element_type=f32)
    mix = mix + own_weight[..., None] * v_own[:, None, :]
    attn = (mix / total[..., None]).astype(bf16).reshape(tokens, q_cols)

    partial = project_out(chip, core, attn, mine, theirs, n_x, col_width)
    parts = exchange(partial, "tensor")
    hidden = (resid + jnp.sum(parts.astype(f32), 0)).astype(bf16)

    keep = pos_x % experts_here
    give = 1 - keep
    swap = [(i, i ^ 1) for i in range(n_x)]
    up_pair = jnp.stack(
        [
            lax.dynamic_index_in_dim(w_gate, give, 0, keepdims=False),
            lax.dynamic_index_in_dim(w_up, give, 0, keepdims=False),
        ]
    )
    got_up = lax.ppermute(up_pair, "tensor", swap)
    down = lax.dynamic_index_in_dim(w_down, give, 0, keepdims=False)
    got_down = lax.ppermute(down, "tensor", swap)

    near = exchange(jnp.broadcast_to(hidden, (chips, *hidden.shape)), "chip")
    across = other_core(near)
    everyone = jnp.concatenate([near, across], 0).reshape(n_e * tokens, col_width)
    mine_e = pos_e * experts_here + jnp.arange(experts_here, dtype=i32)
    named = jnp.any(routes[None] == mine_e[:, None, None, None], -1)
    slot = jnp.where(named, count_earlier(named), -1)
    filled = slot[:, :, None, :] == jnp.arange(capacity, dtype=i32)[None, None, :, None]
    expert_rows = jnp.sum(jnp.where(filled, source[None, :, None, :] + 1, 0), -1) - 1
    home_rows = lax.dynamic_index_in_dim(source, pos_e, 0, keepdims=False)
    hidden_home = pick_rows(home_rows, everyone)
    by_expert = pick_rows(expert_rows.reshape(-1), everyone)
    by_expert = by_expert.reshape(experts_here, n_e * capacity, col_width)
    by_dest = jnp.tile(by_expert, (n_x // experts_here, 1, 1))
    rows_in = exchange(by_dest, "tensor")

    out = run_expert(keep, rows_in, w_gate, w_up, w_down, got_up, got_down)
    parts = exchange(out, "tensor")
    parts = parts.reshape(n_x // experts_here, experts_here, n_e, capacity, col_width)
    summed = jnp.sum(parts.astype(f32), 0).astype(bf16)
    returned = exchange(jnp.transpose(summed, (1, 0, 2, 3)), EXPERT)

    hit = route_ids[:, :, None] == jnp.arange(experts, dtype=i32)
    marks = jnp.any(hit, 1)
    mark_weight = jnp.sum(jnp.where(hit, route_weights[:, :, None], 0.0), 1)
    slot = jnp.dot(
        earlier.astype(bf16), marks.astype(bf16), preferred_element_type=f32
    ).astype(i32)
    slot = jnp.where(marks, slot, -1)
    chosen = slot[:, :, None] == jnp.arange(capacity, dtype=i32)
    mix_rows = (chosen * mark_weight[:, :, None]).reshape(tokens, experts * capacity)
    expert_mix = jnp.dot(
        mix_rows,
        returned.reshape(experts * capacity, col_width).astype(f32),
        precision=lax.Precision.HIGHEST,
    )
    return (hidden_home.astype(f32) + expert_mix).astype(bf16)


def solution(mesh):
    split = Mesh(
        mesh.devices.reshape(
            mesh.shape["groups"],
            mesh.shape["expert"] // CORES,
            CORES,
            mesh.shape["tensor"],
        ),
        ("groups", *EXPERT, "tensor"),
    )
    whole = ("groups", *EXPERT)
    return jax.shard_map(
        layer,
        mesh=split,
        in_specs=(
            P(whole, None),
            P(whole, None),
            P(whole, "tensor", None),
            P(whole),
            P(whole),
            P(whole, None),
            P("tensor", EXPERT),
            P(whole, None),
            P(whole, None),
            P(EXPERT, None, "tensor"),
            P(EXPERT, None, "tensor"),
            P(EXPERT, "tensor", None),
        ),
        out_specs=P(whole, "tensor"),
        check_vma=False,
    )
```

```python
import jax
import jax.numpy as jnp
from jax import lax
from jax.experimental import pallas as pl
from jax.experimental.pallas import tpu as pltpu
from jax.sharding import Mesh
from jax.sharding import PartitionSpec as P

HD = 128
CORES = 2
EXPERT = ("chip", "core")
MASKED_SCORE = -1e30
f32, bf16, i32 = jnp.float32, jnp.bfloat16, jnp.int32


def exchange(tiles, axis):
    return lax.all_to_all(tiles, axis, split_axis=0, concat_axis=0, tiled=True)


def along_chips(x, shift):
    n = lax.axis_size("chip")
    moves = []
    for c in range(n):
        moves.append((c * CORES, (c - shift) % n * CORES))
        moves.append((c * CORES + 1, (c + shift) % n * CORES + 1))
    return lax.ppermute(x, EXPERT, moves)


def across_chips(x):
    n = lax.axis_size("chip")
    moves = []
    for c in range(n):
        moves.append((c * CORES, (c + 1) % n * CORES + 1))
        moves.append((c * CORES + 1, (c - 1) % n * CORES))
    return lax.ppermute(x, EXPERT, moves)


def other_core(x):
    return lax.ppermute(x, "core", [(0, 1), (1, 0)])


def count_earlier(marks):
    n = marks.shape[-1]
    before = (jnp.arange(n)[:, None] < jnp.arange(n)[None, :]).astype(bf16)
    return jnp.dot(marks.astype(bf16), before, preferred_element_type=f32).astype(i32)


def pick_rows(index, rows):
    chosen = (index[:, None] == jnp.arange(rows.shape[0], dtype=i32)).astype(bf16)
    return jnp.dot(chosen, rows, preferred_element_type=f32).astype(bf16)


def projection_kernel(at, attn, mine, theirs, out):
    chips = mine.shape[0]
    half = chips // 2
    first = at[1] == 0
    rows = attn[...]
    per_out = out.shape[2] // (2 * mine.shape[1])

    def block(use_zero, offset, kind):
        spot, n, bit = 0, 1, half // 2
        while bit:
            spot = spot + lax.rem(lax.div(offset, n), 2) * bit
            n, bit = 2 * n, bit // 2
        spot = spot * 2 + kind
        return jnp.where(use_zero == first, mine[spot], theirs[spot])

    for dest in range(out.shape[0]):
        blocks = []
        for near in range(per_out):
            ahead = lax.rem(dest * per_out + near + chips - at[0], chips)
            behind = lax.rem(chips - ahead, chips)
            zero = ahead < half
            blocks.append(
                block(zero, jnp.where(zero, ahead, behind - 1), jnp.where(zero, 0, 1))
            )
            one = (ahead >= 1) & (ahead <= half)
            blocks.append(
                block(one, jnp.where(one, ahead - 1, behind), jnp.where(one, 1, 0))
            )
        weight = jnp.concatenate(blocks, 0)
        out[dest] = lax.dot_general(
            rows, weight, (((1,), (1,)), ((), ())), preferred_element_type=f32
        ).astype(bf16)


def project_out(chip, core, attn, mine, theirs, n_x, col_width):
    vmem = pl.BlockSpec(memory_space=pltpu.VMEM)
    flops = 2 * attn.shape[0] * 2 * mine.size
    return pl.pallas_call(
        projection_kernel,
        out_shape=jax.ShapeDtypeStruct((n_x, attn.shape[0], col_width), bf16),
        in_specs=[pl.BlockSpec(memory_space=pltpu.SMEM), vmem, vmem, vmem],
        out_specs=vmem,
        cost_estimate=pl.CostEstimate(
            flops=flops, bytes_accessed=4 * mine.size, transcendentals=0
        ),
        compiler_params=pltpu.CompilerParams(vmem_limit_bytes=8 << 20),
        name="project_out",
    )(jnp.stack([chip, core]).astype(i32), attn, mine, theirs)


def expert_kernel(keep, rows, gate, up, down, got_up, got_down, out):
    n_x, count, col_width = rows.shape
    ff = gate.shape[2]
    total = jnp.zeros((count, 4 * ff), f32)
    for s in range(n_x):
        at = pl.ds(s * col_width, col_width)
        weight = jnp.concatenate(
            [gate[0, at, :], got_up[0, at, :], up[0, at, :], got_up[1, at, :]], 1
        )
        total = total + jnp.dot(rows[s], weight, preferred_element_type=f32)
    gates, ups = total[:, : 2 * ff], total[:, 2 * ff :]
    act = (gates / (1.0 + jnp.exp(-gates)) * ups).astype(bf16)
    for d in range(n_x):
        at = pl.ds(d * col_width, col_width)
        weight = jnp.concatenate([down[0, :, at], got_down[:, at]], 0)
        out[d] = jnp.dot(act, weight, preferred_element_type=f32).astype(bf16)


def run_expert(keep, rows, gate, up, down, got_up, got_down):
    def whole(x):
        return pl.BlockSpec(x.shape, lambda i, k: (0,) * x.ndim)

    def kept(x):
        return pl.BlockSpec((1, *x.shape[1:]), lambda i, k: (k[0], 0, 0))

    flops = 2 * rows.size * got_up.shape[2] * 4 + 2 * rows.size * got_down.shape[0] * 2
    moved = 2 * (2 * rows.size + got_up.size + got_down.size) + 3 * gate.size
    return pl.pallas_call(
        expert_kernel,
        out_shape=jax.ShapeDtypeStruct(rows.shape, bf16),
        grid_spec=pltpu.PrefetchScalarGridSpec(
            num_scalar_prefetch=1,
            grid=(1,),
            in_specs=[
                whole(rows),
                kept(gate),
                kept(up),
                kept(down),
                whole(got_up),
                whole(got_down),
            ],
            out_specs=whole(rows),
        ),
        cost_estimate=pl.CostEstimate(
            flops=flops, bytes_accessed=moved, transcendentals=rows.shape[1] * 2 * HD
        ),
        compiler_params=pltpu.CompilerParams(vmem_limit_bytes=16 << 20),
        name="run_expert",
    )(jnp.reshape(keep, (1,)).astype(i32), rows, gate, up, down, got_up, got_down)


def layer(
    queries,
    own_kv,
    prompt_cache,
    prompt_len,
    token_prompt,
    residual,
    out_weight,
    route_ids,
    route_weights,
    w_gate,
    w_up,
    w_down,
):
    n_e = lax.axis_size(EXPERT)
    n_x = lax.axis_size("tensor")
    chips = lax.axis_size("chip")
    pos_x = lax.axis_index("tensor")
    chip = lax.axis_index("chip")
    core = lax.axis_index("core")
    pos_e = chip * CORES + core
    tokens = queries.shape[0]
    half_cols = own_kv.shape[1] // 2
    kv_heads = half_cols // HD
    head_count = queries.shape[1] // HD
    group_size = head_count // kv_heads
    heads_here = head_count // n_x
    q_cols = heads_here * HD
    per_prompt = tokens // (n_e // 2)
    block_len = prompt_cache.shape[1]
    model_width = residual.shape[1]
    col_width = model_width // n_x
    picks = route_ids.shape[1]
    experts_here = w_gate.shape[0]
    experts = experts_here * n_e
    capacity = min(tokens, 3 * tokens * picks // (2 * experts))

    cache = prompt_cache[0].reshape(block_len, 2, kv_heads, HD)
    by_head = jnp.transpose(cache, (2, 0, 1, 3)).reshape(kv_heads, block_len, 2 * HD)
    by_head = jnp.repeat(by_head, n_x // kv_heads, axis=0)
    cache_all = exchange(by_head, "tensor")
    cache_all = cache_all.reshape(n_x * block_len, 2 * HD)

    w_own = out_weight.T
    mine = jnp.stack([w_own, across_chips(w_own)])
    shift = chips // 4
    while shift:
        mine = jnp.concatenate([mine, along_chips(mine, shift)])
        shift //= 2
    theirs = other_core(mine)

    kv_pos = (pos_x * heads_here) // group_size
    payload = jnp.concatenate(
        [
            lax.dynamic_slice_in_dim(queries, pos_x * q_cols, q_cols, 1),
            lax.dynamic_slice_in_dim(own_kv, kv_pos * HD, HD, 1),
            lax.dynamic_slice_in_dim(own_kv, half_cols + kv_pos * HD, HD, 1),
            lax.dynamic_slice_in_dim(residual, pos_x * col_width, col_width, 1),
        ],
        1,
    )
    width = payload.shape[1]
    same = token_prompt[:, None] == token_prompt[None, :]
    earlier = jnp.arange(tokens)[None, :] < jnp.arange(tokens)[:, None]
    rank = jnp.sum((same & earlier).astype(i32), 1)
    place = token_prompt * per_prompt + rank
    rows = n_e * per_prompt
    pick = (jnp.arange(rows)[:, None] == place[None, :]).astype(bf16)
    sent = jnp.dot(pick, payload, preferred_element_type=f32).astype(bf16)
    table = jnp.concatenate([token_prompt, route_ids.reshape(-1)]).astype(bf16)
    entries = table.shape[0]
    table_cols = -(-entries // (per_prompt * HD)) * HD
    table = jnp.pad(table, (0, per_prompt * table_cols - entries))
    table = jnp.broadcast_to(
        table.reshape(1, per_prompt, table_cols), (n_e, per_prompt, table_cols)
    )
    sent = jnp.concatenate([sent.reshape(n_e, per_prompt, width), table], 2)
    sent, cache_all = lax.optimization_barrier((sent, cache_all))
    keys, values = cache_all[:, :HD], cache_all[:, HD:]
    got = exchange(sent, EXPERT)
    table = got[:, :, width:].reshape(n_e, per_prompt * table_cols)[:, :entries].astype(i32)
    prompts = table[:, :tokens]
    routes = table[:, tokens:].reshape(n_e, tokens, picks)

    owner = jnp.arange(n_e, dtype=i32)
    holds = jnp.any(prompts[None, :, :] == owner[:, None, None], -1)
    order = count_earlier(holds)
    peers = prompts[:, :, None] == prompts[:, None, :]
    rank_all = jnp.sum((peers & earlier[None]).astype(i32), 2)
    block_order = jnp.sum(
        jnp.where(prompts[:, :, None] == owner, order.T[:, None, :], 0), 2
    )
    source = jnp.where(prompts % CORES == core, 0, chips) + prompts // CORES
    source = source * tokens + block_order * per_prompt + rank_all

    own_holds = jnp.any(prompts == pos_e, 1)
    own_order = count_earlier(own_holds[None])[0]
    slot_here = own_order[:, None] * per_prompt + jnp.arange(per_prompt, dtype=i32)
    slot_here = jnp.where(own_holds[:, None], slot_here, -1).reshape(rows)
    compact = (jnp.arange(tokens, dtype=i32)[:, None] == slot_here[None, :]).astype(bf16)
    got = jnp.dot(
        compact, got[:, :, :width].reshape(rows, width), preferred_element_type=f32
    ).astype(bf16)

    q_rows = got[:, :q_cols].reshape(tokens, heads_here, HD)
    k_own = got[:, q_cols : q_cols + HD].astype(f32)
    v_own = got[:, q_cols + HD : q_cols + 2 * HD].astype(f32)
    resid = got[:, q_cols + 2 * HD :].astype(f32)
    scale = HD ** (-0.5)
    scores = jnp.einsum("rhd,pd->rhp", q_rows, keys, preferred_element_type=f32) * scale
    own = jnp.sum(q_rows.astype(f32) * k_own[:, None, :], -1) * scale
    inside = jnp.arange(n_x * block_len) < prompt_len[0]
    scores = jnp.where(inside, scores, MASKED_SCORE)
    top = jnp.maximum(jnp.max(scores, -1), own)
    weights = jnp.where(inside, jnp.exp(scores - top[..., None]), 0.0)
    own_weight = jnp.exp(own - top)
    total = jnp.sum(weights, -1) + own_weight
    mix = jnp.einsum("rhp,pd->rhd", weights.astype(bf16), values, preferred_element_type=f32)
    mix = mix + own_weight[..., None] * v_own[:, None, :]
    attn = (mix / total[..., None]).astype(bf16).reshape(tokens, q_cols)

    partial = project_out(chip, core, attn, mine, theirs, n_x, col_width)
    parts = exchange(partial, "tensor")
    hidden = (resid + jnp.sum(parts.astype(f32), 0)).astype(bf16)

    keep = pos_x % experts_here
    give = 1 - keep
    swap = [(i, i ^ 1) for i in range(n_x)]
    up_pair = jnp.stack(
        [
            lax.dynamic_index_in_dim(w_gate, give, 0, keepdims=False),
            lax.dynamic_index_in_dim(w_up, give, 0, keepdims=False),
        ]
    )
    got_up = lax.ppermute(up_pair, "tensor", swap)
    down = lax.dynamic_index_in_dim(w_down, give, 0, keepdims=False)
    got_down = lax.ppermute(down, "tensor", swap)

    near = exchange(jnp.broadcast_to(hidden, (chips, *hidden.shape)), "chip")
    across = other_core(near)
    everyone = jnp.concatenate([near, across], 0).reshape(n_e * tokens, col_width)
    mine_e = pos_e * experts_here + jnp.arange(experts_here, dtype=i32)
    named = jnp.any(routes[None] == mine_e[:, None, None, None], -1)
    slot = jnp.where(named, count_earlier(named), -1)
    filled = slot[:, :, None, :] == jnp.arange(capacity, dtype=i32)[None, None, :, None]
    expert_rows = jnp.sum(jnp.where(filled, source[None, :, None, :] + 1, 0), -1) - 1
    home_rows = lax.dynamic_index_in_dim(source, pos_e, 0, keepdims=False)
    hidden_home = pick_rows(home_rows, everyone)
    by_expert = pick_rows(expert_rows.reshape(-1), everyone)
    by_expert = by_expert.reshape(experts_here, n_e * capacity, col_width)
    by_dest = jnp.tile(by_expert, (n_x // experts_here, 1, 1))
    rows_in = exchange(by_dest, "tensor")

    out = run_expert(keep, rows_in, w_gate, w_up, w_down, got_up, got_down)
    parts = exchange(out, "tensor")
    parts = parts.reshape(n_x // experts_here, experts_here, n_e, capacity, col_width)
    summed = jnp.sum(parts.astype(f32), 0).astype(bf16)
    returned = exchange(jnp.transpose(summed, (1, 0, 2, 3)), EXPERT)

    hit = route_ids[:, :, None] == jnp.arange(experts, dtype=i32)
    marks = jnp.any(hit, 1)
    mark_weight = jnp.sum(jnp.where(hit, route_weights[:, :, None], 0.0), 1)
    slot = jnp.dot(
        earlier.astype(bf16), marks.astype(bf16), preferred_element_type=f32
    ).astype(i32)
    slot = jnp.where(marks, slot, -1)
    chosen = slot[:, :, None] == jnp.arange(capacity, dtype=i32)
    mix_rows = (chosen * mark_weight[:, :, None]).reshape(tokens, experts * capacity)
    expert_mix = jnp.dot(
        mix_rows,
        returned.reshape(experts * capacity, col_width).astype(f32),
        precision=lax.Precision.HIGHEST,
    )
    return (hidden_home.astype(f32) + expert_mix).astype(bf16)


def solution(mesh):
    split = Mesh(
        mesh.devices.reshape(
            mesh.shape["groups"],
            mesh.shape["expert"] // CORES,
            CORES,
            mesh.shape["tensor"],
        ),
        ("groups", *EXPERT, "tensor"),
    )
    whole = ("groups", *EXPERT)
    return jax.shard_map(
        layer,
        mesh=split,
        in_specs=(
            P(whole, None),
            P(whole, None),
            P(whole, "tensor", None),
            P(whole),
            P(whole),
            P(whole, None),
            P("tensor", EXPERT),
            P(whole, None),
            P(whole, None),
            P(EXPERT, None, "tensor"),
            P(EXPERT, None, "tensor"),
            P(EXPERT, "tensor", None),
        ),
        out_specs=P(whole, "tensor"),
        check_vma=False,
    )
```

```python
import jax
import jax.numpy as jnp
from jax import lax
from jax.experimental import pallas as pl
from jax.experimental.pallas import tpu as pltpu
from jax.sharding import Mesh
from jax.sharding import PartitionSpec as P

HD = 128
CORES = 2
EXPERT = ("chip", "core")
MASKED_SCORE = -1e30
f32, bf16, i32 = jnp.float32, jnp.bfloat16, jnp.int32


def exchange(tiles, axis):
    return lax.all_to_all(tiles, axis, split_axis=0, concat_axis=0, tiled=True)


def along_chips(x, shift):
    n = lax.axis_size("chip")
    moves = []
    for c in range(n):
        moves.append((c * CORES, (c - shift) % n * CORES))
        moves.append((c * CORES + 1, (c + shift) % n * CORES + 1))
    return lax.ppermute(x, EXPERT, moves)


def across_chips(x):
    n = lax.axis_size("chip")
    moves = []
    for c in range(n):
        moves.append((c * CORES, (c + 1) % n * CORES + 1))
        moves.append((c * CORES + 1, (c - 1) % n * CORES))
    return lax.ppermute(x, EXPERT, moves)


def other_core(x):
    return lax.ppermute(x, "core", [(0, 1), (1, 0)])


def count_earlier(marks):
    n = marks.shape[-1]
    before = (jnp.arange(n)[:, None] < jnp.arange(n)[None, :]).astype(bf16)
    return jnp.dot(marks.astype(bf16), before, preferred_element_type=f32).astype(i32)


def one_hot(at, shape, dim):
    return jnp.where(lax.broadcasted_iota(i32, shape, dim) == at, 1.0, 0.0).astype(bf16)


def grouped_iota(groups, size, lanes, dim):
    at = lax.broadcasted_iota(i32, (groups, size, lanes), dim)
    return at.reshape(groups * size, lanes)


def payload_kernel(places, target, q, k, v, resid, table, out):
    chunks = [q[:, c : c + HD] for c in range(0, q.shape[1], HD)]
    chunks += [k[...], v[...]]
    chunks += [resid[:, c : c + HD] for c in range(0, resid.shape[1], HD)]
    rows = jnp.concatenate([*chunks, table[...]], 0)
    count, depth = out.shape[0], rows.shape[0]
    groups = q.shape[0]
    whole = lax.broadcasted_iota(i32, (count, depth), 0) == target[0:1, :]
    local_row = grouped_iota(groups, count // groups, depth, 1) == target[1:2, :]
    chosen = jnp.where(whole | local_row, 1.0, 0.0).astype(bf16)
    out[...] = jnp.dot(chosen, rows, preferred_element_type=f32).astype(bf16)


def build_payload(places, target, queries, own_kv, residual, table, q_cols, col_width, count):
    tokens = queries.shape[0]

    def cols(width, which):
        return pl.BlockSpec((tokens, width), lambda i, at: (0, at[which]))

    def whole(x):
        return pl.BlockSpec(x.shape, lambda i, at: (0,) * x.ndim)

    return pl.pallas_call(
        payload_kernel,
        out_shape=jax.ShapeDtypeStruct((count, HD), bf16),
        grid_spec=pltpu.PrefetchScalarGridSpec(
            num_scalar_prefetch=1,
            grid=(1,),
            in_specs=[
                whole(target),
                cols(q_cols, 0),
                cols(HD, 1),
                cols(HD, 2),
                cols(col_width, 0),
                whole(table),
            ],
            out_specs=pl.BlockSpec((count, HD), lambda i, at: (0, 0)),
        ),
        cost_estimate=pl.CostEstimate(
            flops=2 * count * target.shape[1] * HD,
            bytes_accessed=4 * count * HD,
            transcendentals=0,
        ),
        compiler_params=pltpu.CompilerParams(vmem_limit_bytes=8 << 20),
        name="build_payload",
    )(places, target, queries, own_kv, own_kv, residual, table)


def attention_kernel(at, got, cache, attn, resid):
    tokens = attn.shape[0]
    heads = attn.shape[1] // HD
    chunks = heads + 2 + resid.shape[1] // HD
    blocks = tokens
    size = got.shape[0] // blocks
    rows = got[...]
    table_row = one_hot(
        lax.broadcasted_iota(i32, (blocks, got.shape[0]), 0) * size + 2 * chunks,
        (blocks, got.shape[0]),
        1,
    )
    prompts = jnp.dot(table_row, rows, preferred_element_type=f32)[:, :tokens]
    holds = jnp.max(jnp.where(prompts == at[0].astype(f32), 1.0, 0.0), 1, keepdims=True)
    before = jnp.where(
        lax.broadcasted_iota(i32, (blocks, blocks), 1)
        < lax.broadcasted_iota(i32, (blocks, blocks), 0),
        1.0,
        0.0,
    ).astype(bf16)
    wide = jnp.broadcast_to(holds, (blocks, HD)).astype(bf16)
    order = jnp.dot(before, wide, preferred_element_type=f32)
    order = jnp.where(wide > 0, order * 2.0, -1024.0).astype(bf16)
    spread = jnp.where(
        grouped_iota(blocks, size, blocks, 0)
        == lax.broadcasted_iota(i32, (blocks * size, blocks), 1),
        1.0,
        0.0,
    ).astype(bf16)
    order = jnp.dot(spread, order, preferred_element_type=f32)[:, :1].astype(i32)
    place = grouped_iota(blocks, size, 1, 1)
    second = jnp.where(place >= chunks, 1, 0)
    target = (place - second * chunks) * tokens + order + second
    target = jnp.where(place < 2 * chunks, target, -1)
    chosen = one_hot(target, (got.shape[0], chunks * tokens), 1)
    mine = lax.dot_general(
        chosen, rows, (((0,), (0,)), ((), ())), preferred_element_type=f32
    )

    def chunk(c):
        return mine[c * tokens : (c + 1) * tokens, :]

    k_own, v_own = chunk(heads), chunk(heads + 1)
    positions = cache.shape[0] * cache.shape[1]
    both = cache[...].reshape(positions, cache.shape[2])
    keys, values = both[:, :HD], both[:, HD:]
    inside = lax.broadcasted_iota(i32, (tokens, positions), 1) < at[1]
    scale = HD ** (-0.5)
    for h in range(heads):
        q = chunk(h)
        scores = (
            lax.dot_general(
                q.astype(bf16), keys, (((1,), (1,)), ((), ())), preferred_element_type=f32
            )
            * scale
        )
        scores = jnp.where(inside, scores, MASKED_SCORE)
        own = jnp.sum(q * k_own, 1, keepdims=True) * scale
        top = jnp.maximum(jnp.max(scores, 1, keepdims=True), own)
        weights = jnp.where(inside, jnp.exp(scores - top), 0.0)
        own_weight = jnp.exp(own - top)
        total = jnp.sum(weights, 1, keepdims=True) + own_weight
        mix = jnp.dot(weights.astype(bf16), values, preferred_element_type=f32)
        mix = (mix + own_weight * v_own) / total
        attn[:, h * HD : (h + 1) * HD] = mix.astype(bf16)
    for c in range(resid.shape[1] // HD):
        resid[:, c * HD : (c + 1) * HD] = chunk(heads + 2 + c).astype(bf16)


def attend(at, got, cache, tokens, q_cols, col_width):
    vmem = pl.BlockSpec(memory_space=pltpu.VMEM)
    return pl.pallas_call(
        attention_kernel,
        out_shape=(
            jax.ShapeDtypeStruct((tokens, q_cols), bf16),
            jax.ShapeDtypeStruct((tokens, col_width), bf16),
        ),
        in_specs=[pl.BlockSpec(memory_space=pltpu.SMEM), vmem, vmem],
        out_specs=(vmem, vmem),
        cost_estimate=pl.CostEstimate(
            flops=4 * got.size * 256, bytes_accessed=2 * got.size, transcendentals=0
        ),
        compiler_params=pltpu.CompilerParams(vmem_limit_bytes=8 << 20),
        name="attend",
    )(at, got, cache)


def hidden_kernel(parts, resid, out):
    hidden = resid[...].astype(f32)
    for s in range(parts.shape[0]):
        hidden = hidden + parts[s].astype(f32)
    hidden = hidden.astype(bf16)
    for d in range(out.shape[0]):
        out[d] = hidden


def hidden_copies(parts, resid, copies):
    vmem = pl.BlockSpec(memory_space=pltpu.VMEM)
    return pl.pallas_call(
        hidden_kernel,
        out_shape=jax.ShapeDtypeStruct((copies, *resid.shape), bf16),
        in_specs=[vmem, vmem],
        out_specs=vmem,
        cost_estimate=pl.CostEstimate(
            flops=parts.size, bytes_accessed=4 * parts.size, transcendentals=0
        ),
        compiler_params=pltpu.CompilerParams(vmem_limit_bytes=4 << 20),
        name="hidden_copies",
    )(parts, resid)


def select_kernel(experts_at, home_at, near, across, by_dest, home):
    half = near.shape[0]

    def picked(at):
        shape = (at.shape[0], half)
        return (
            jnp.dot(one_hot(at, shape, 1), near[...], preferred_element_type=f32)
            + jnp.dot(one_hot(at - half, shape, 1), across[...], preferred_element_type=f32)
        ).astype(bf16)

    home[...] = picked(home_at[...])
    count = by_dest.shape[1]
    kinds = experts_at.shape[0] // count
    for kind in range(kinds):
        rows = picked(experts_at[kind * count : (kind + 1) * count, :])
        for d in range(kind, by_dest.shape[0], kinds):
            by_dest[d] = rows


def select_rows(experts_at, home_at, near, across, n_x, kinds):
    vmem = pl.BlockSpec(memory_space=pltpu.VMEM)
    count, width = experts_at.shape[0] // kinds, near.shape[1]
    return pl.pallas_call(
        select_kernel,
        out_shape=(
            jax.ShapeDtypeStruct((n_x, count, width), bf16),
            jax.ShapeDtypeStruct((home_at.shape[0], width), bf16),
        ),
        in_specs=[vmem] * 4,
        out_specs=(vmem, vmem),
        cost_estimate=pl.CostEstimate(
            flops=4 * experts_at.shape[0] * near.size,
            bytes_accessed=4 * near.size,
            transcendentals=0,
        ),
        compiler_params=pltpu.CompilerParams(vmem_limit_bytes=8 << 20),
        name="select_rows",
    )(experts_at, home_at, near, across)


def projection_kernel(at, attn, mine_a, mine_b, theirs_a, theirs_b, out):
    half = mine_a.shape[0]
    chips = 2 * half
    first = at[1] == 0
    rows = attn[...]
    per_out = out.shape[2] // (2 * mine_a.shape[1])

    def block(use_zero, offset, kind):
        spot, n, bit = 0, 1, half // 2
        while bit:
            spot = spot + lax.rem(lax.div(offset, n), 2) * bit
            n, bit = 2 * n, bit // 2
        spot = spot * 2 + kind
        low = spot < half
        a, b = jnp.minimum(spot, half - 1), jnp.maximum(spot - half, 0)
        ours = jnp.where(low, mine_a[a], mine_b[b])
        return jnp.where(use_zero == first, ours, jnp.where(low, theirs_a[a], theirs_b[b]))

    for dest in range(out.shape[0]):
        blocks = []
        for near in range(per_out):
            ahead = lax.rem(dest * per_out + near + chips - at[0], chips)
            behind = lax.rem(chips - ahead, chips)
            zero = ahead < half
            blocks.append(
                block(zero, jnp.where(zero, ahead, behind - 1), jnp.where(zero, 0, 1))
            )
            one = (ahead >= 1) & (ahead <= half)
            blocks.append(
                block(one, jnp.where(one, ahead - 1, behind), jnp.where(one, 1, 0))
            )
        weight = jnp.concatenate(blocks, 0)
        out[dest] = lax.dot_general(
            rows, weight, (((1,), (1,)), ((), ())), preferred_element_type=f32
        ).astype(bf16)


def project_out(at, attn, halves, n_x, col_width):
    vmem = pl.BlockSpec(memory_space=pltpu.VMEM)
    size = sum(h.size for h in halves)
    return pl.pallas_call(
        projection_kernel,
        out_shape=jax.ShapeDtypeStruct((n_x, attn.shape[0], col_width), bf16),
        in_specs=[pl.BlockSpec(memory_space=pltpu.SMEM), *[vmem] * 5],
        out_specs=vmem,
        cost_estimate=pl.CostEstimate(
            flops=2 * attn.shape[0] * size, bytes_accessed=2 * size, transcendentals=0
        ),
        compiler_params=pltpu.CompilerParams(vmem_limit_bytes=8 << 20),
        name="project_out",
    )(at, attn, *halves)


def expert_kernel(keep, rows, gate, up, down, got_up, got_down, out):
    n_x, count, col_width = rows.shape
    ff = gate.shape[2]
    total = jnp.zeros((count, 4 * ff), f32)
    for s in range(n_x):
        at = pl.ds(s * col_width, col_width)
        weight = jnp.concatenate(
            [gate[0, at, :], got_up[0, at, :], up[0, at, :], got_up[1, at, :]], 1
        )
        total = total + jnp.dot(rows[s], weight, preferred_element_type=f32)
    gates, ups = total[:, : 2 * ff], total[:, 2 * ff :]
    act = (gates / (1.0 + jnp.exp(-gates)) * ups).astype(bf16)
    for d in range(n_x):
        at = pl.ds(d * col_width, col_width)
        weight = jnp.concatenate([down[0, :, at], got_down[:, at]], 0)
        out[d] = jnp.dot(act, weight, preferred_element_type=f32).astype(bf16)


def run_expert(keep, rows, gate, up, down, got_up, got_down):
    def whole(x):
        return pl.BlockSpec(x.shape, lambda i, k: (0,) * x.ndim)

    def kept(x):
        return pl.BlockSpec((1, *x.shape[1:]), lambda i, k: (k[0], 0, 0))

    flops = 2 * rows.size * got_up.shape[2] * 4 + 2 * rows.size * got_down.shape[0] * 2
    moved = 2 * (2 * rows.size + got_up.size + got_down.size) + 3 * gate.size
    return pl.pallas_call(
        expert_kernel,
        out_shape=jax.ShapeDtypeStruct(rows.shape, bf16),
        grid_spec=pltpu.PrefetchScalarGridSpec(
            num_scalar_prefetch=1,
            grid=(1,),
            in_specs=[
                whole(rows),
                kept(gate),
                kept(up),
                kept(down),
                whole(got_up),
                whole(got_down),
            ],
            out_specs=whole(rows),
        ),
        cost_estimate=pl.CostEstimate(
            flops=flops, bytes_accessed=moved, transcendentals=rows.shape[1] * 2 * HD
        ),
        compiler_params=pltpu.CompilerParams(vmem_limit_bytes=16 << 20),
        name="run_expert",
    )(jnp.reshape(keep, (1,)).astype(i32), rows, gate, up, down, got_up, got_down)


def layer(
    queries,
    own_kv,
    prompt_cache,
    prompt_len,
    token_prompt,
    residual,
    out_weight,
    route_ids,
    route_weights,
    w_gate,
    w_up,
    w_down,
):
    n_e = lax.axis_size(EXPERT)
    n_x = lax.axis_size("tensor")
    chips = lax.axis_size("chip")
    pos_x = lax.axis_index("tensor")
    chip = lax.axis_index("chip")
    core = lax.axis_index("core")
    pos_e = chip * CORES + core
    tokens = queries.shape[0]
    half_cols = own_kv.shape[1] // 2
    kv_heads = half_cols // HD
    head_count = queries.shape[1] // HD
    group_size = head_count // kv_heads
    heads_here = head_count // n_x
    q_cols = heads_here * HD
    per_prompt = tokens // (n_e // 2)
    block_len = prompt_cache.shape[1]
    model_width = residual.shape[1]
    col_width = model_width // n_x
    picks = route_ids.shape[1]
    experts_here = w_gate.shape[0]
    experts = experts_here * n_e
    capacity = min(tokens, 3 * tokens * picks // (2 * experts))

    cache = prompt_cache[0].reshape(block_len, 2, kv_heads, HD)
    by_head = jnp.transpose(cache, (2, 0, 1, 3)).reshape(kv_heads, block_len, 2 * HD)
    by_head = jnp.repeat(by_head, n_x // kv_heads, axis=0)
    cache_all = exchange(by_head, "tensor")

    w_own = out_weight.T
    mine = jnp.stack([w_own, across_chips(w_own)])
    shift = chips // 4
    while shift > 1:
        mine = jnp.concatenate([mine, along_chips(mine, shift)])
        shift //= 2
    mine_b = along_chips(mine, 1)
    theirs_a = other_core(mine)
    theirs_b = other_core(mine_b)

    kv_pos = (pos_x * heads_here) // group_size
    earlier = jnp.arange(tokens)[None, :] < jnp.arange(tokens)[:, None]
    same = token_prompt[:, None] == token_prompt[None, :]
    rank = jnp.sum((same & earlier).astype(i32), 1)
    chunks = (q_cols + 2 * HD + col_width) // HD
    entries = jnp.concatenate(
        [jnp.pad(token_prompt, (0, HD - tokens)), route_ids.reshape(-1)]
    )
    table_rows = -(-entries.shape[0] // (8 * HD)) * 8
    table = jnp.pad(entries, (0, HD * HD - entries.shape[0])).astype(bf16).reshape(HD, HD)
    size = 2 * chunks + table_rows
    place = token_prompt * size + rank * chunks
    token_rows = (place[None, :] + jnp.arange(chunks, dtype=i32)[:, None]).reshape(-1)
    spare = jnp.arange(HD, dtype=i32)
    target = jnp.stack(
        [
            jnp.pad(token_rows, (0, HD), constant_values=-1),
            jnp.concatenate(
                [
                    jnp.full((tokens * chunks,), -1, i32),
                    jnp.where(spare < table_rows, 2 * chunks + spare, -1),
                ]
            ),
        ]
    )
    places = jnp.stack([pos_x, kv_pos, kv_heads + kv_pos]).astype(i32)
    sent = build_payload(
        places, target, queries, own_kv, residual, table, q_cols, col_width, n_e * size
    )
    sent, cache_all = lax.optimization_barrier((sent, cache_all))
    got = exchange(sent.reshape(n_e, size, HD), EXPERT)
    table = got[:, 2 * chunks : 2 * chunks + 1 + tokens * picks // HD, :].astype(i32)
    prompts = table[:, 0, :tokens]
    routes = table[:, 1:, :].reshape(n_e, tokens, picks)

    owner = jnp.arange(n_e, dtype=i32)
    holds = jnp.any(prompts[None, :, :] == owner[:, None, None], -1)
    order = count_earlier(holds)
    peers = prompts[:, :, None] == prompts[:, None, :]
    rank_all = jnp.sum((peers & earlier[None]).astype(i32), 2)
    block_order = jnp.sum(
        jnp.where(prompts[:, :, None] == owner, order.T[:, None, :], 0), 2
    )
    source = jnp.where(prompts % CORES == core, 0, chips) + prompts // CORES
    source = source * tokens + block_order * per_prompt + rank_all

    at = jnp.concatenate([jnp.stack([pos_e]).astype(i32), prompt_len])
    attn, resid = attend(
        at, got.reshape(n_e * size, HD), cache_all, tokens, q_cols, col_width
    )
    at = jnp.stack([chip, core]).astype(i32)
    partial = project_out(at, attn, (mine, mine_b, theirs_a, theirs_b), n_x, col_width)
    parts = exchange(partial, "tensor")
    hidden = hidden_copies(parts, resid, chips)

    keep = pos_x % experts_here
    give = 1 - keep
    swap = [(i, i ^ 1) for i in range(n_x)]
    up_pair = jnp.stack(
        [
            lax.dynamic_index_in_dim(w_gate, give, 0, keepdims=False),
            lax.dynamic_index_in_dim(w_up, give, 0, keepdims=False),
        ]
    )
    got_up = lax.ppermute(up_pair, "tensor", swap)
    down = lax.dynamic_index_in_dim(w_down, give, 0, keepdims=False)
    got_down = lax.ppermute(down, "tensor", swap)

    near = exchange(hidden, "chip")
    across = other_core(near)
    mine_e = pos_e * experts_here + jnp.arange(experts_here, dtype=i32)
    named = jnp.any(routes[None] == mine_e[:, None, None, None], -1)
    slot = jnp.where(named, count_earlier(named), -1)
    filled = slot[:, :, None, :] == jnp.arange(capacity, dtype=i32)[None, None, :, None]
    expert_rows = jnp.sum(jnp.where(filled, source[None, :, None, :] + 1, 0), -1) - 1
    home_rows = lax.dynamic_index_in_dim(source, pos_e, 0, keepdims=False)
    by_dest, hidden_home = select_rows(
        expert_rows.reshape(-1, 1),
        home_rows.reshape(-1, 1),
        near.reshape(chips * tokens, col_width),
        across.reshape(chips * tokens, col_width),
        n_x,
        experts_here,
    )
    rows_in = exchange(by_dest, "tensor")

    out = run_expert(keep, rows_in, w_gate, w_up, w_down, got_up, got_down)
    parts = exchange(out, "tensor")
    parts = parts.reshape(n_x // experts_here, experts_here, n_e, capacity, col_width)
    summed = jnp.sum(parts.astype(f32), 0).astype(bf16)
    returned = exchange(jnp.transpose(summed, (1, 0, 2, 3)), EXPERT)

    hit = route_ids[:, :, None] == jnp.arange(experts, dtype=i32)
    marks = jnp.any(hit, 1)
    mark_weight = jnp.sum(jnp.where(hit, route_weights[:, :, None], 0.0), 1)
    slot = jnp.dot(
        earlier.astype(bf16), marks.astype(bf16), preferred_element_type=f32
    ).astype(i32)
    slot = jnp.where(marks, slot, -1)
    chosen = slot[:, :, None] == jnp.arange(capacity, dtype=i32)
    mix_rows = (chosen * mark_weight[:, :, None]).reshape(tokens, experts * capacity)
    expert_mix = jnp.dot(
        mix_rows,
        returned.reshape(experts * capacity, col_width).astype(f32),
        precision=lax.Precision.HIGHEST,
    )
    return (hidden_home.astype(f32) + expert_mix).astype(bf16)


def solution(mesh):
    split = Mesh(
        mesh.devices.reshape(
            mesh.shape["groups"],
            mesh.shape["expert"] // CORES,
            CORES,
            mesh.shape["tensor"],
        ),
        ("groups", *EXPERT, "tensor"),
    )
    whole = ("groups", *EXPERT)
    return jax.shard_map(
        layer,
        mesh=split,
        in_specs=(
            P(whole, None),
            P(whole, None),
            P(whole, "tensor", None),
            P(whole),
            P(whole),
            P(whole, None),
            P("tensor", EXPERT),
            P(whole, None),
            P(whole, None),
            P(EXPERT, None, "tensor"),
            P(EXPERT, None, "tensor"),
            P(EXPERT, "tensor", None),
        ),
        out_specs=P(whole, "tensor"),
        check_vma=False,
    )
```

```python
import jax
import jax.numpy as jnp
from jax import lax
from jax.experimental import pallas as pl
from jax.experimental.pallas import tpu as pltpu
from jax.sharding import Mesh
from jax.sharding import PartitionSpec as P

HD = 128
CORES = 2
EXPERT = ("chip", "core")
MASKED_SCORE = -1e30
f32, bf16, i32 = jnp.float32, jnp.bfloat16, jnp.int32


def exchange(tiles, axis):
    return lax.all_to_all(tiles, axis, split_axis=0, concat_axis=0, tiled=True)


def along_chips(x, shift):
    n = lax.axis_size("chip")
    moves = []
    for c in range(n):
        moves.append((c * CORES, (c - shift) % n * CORES))
        moves.append((c * CORES + 1, (c + shift) % n * CORES + 1))
    return lax.ppermute(x, EXPERT, moves)


def across_chips(x):
    n = lax.axis_size("chip")
    moves = []
    for c in range(n):
        moves.append((c * CORES, (c + 1) % n * CORES + 1))
        moves.append((c * CORES + 1, (c - 1) % n * CORES))
    return lax.ppermute(x, EXPERT, moves)


def other_core(x):
    return lax.ppermute(x, "core", [(0, 1), (1, 0)])


def count_earlier(marks):
    n = marks.shape[-1]
    before = (jnp.arange(n)[:, None] < jnp.arange(n)[None, :]).astype(bf16)
    return jnp.dot(marks.astype(bf16), before, preferred_element_type=f32).astype(i32)


def one_hot(at, shape, dim):
    return jnp.where(lax.broadcasted_iota(i32, shape, dim) == at, 1.0, 0.0).astype(bf16)


def grouped_iota(groups, size, lanes, dim):
    at = lax.broadcasted_iota(i32, (groups, size, lanes), dim)
    return at.reshape(groups * size, lanes)


def payload_kernel(places, target, q, k, v, resid, table, out):
    chunks = [q[:, c : c + HD] for c in range(0, q.shape[1], HD)]
    chunks += [k[...], v[...]]
    chunks += [resid[:, c : c + HD] for c in range(0, resid.shape[1], HD)]
    rows = jnp.concatenate([*chunks, table[...]], 0)
    count, depth = out.shape[0], rows.shape[0]
    groups = q.shape[0]
    whole = lax.broadcasted_iota(i32, (count, depth), 0) == target[0:1, :]
    local_row = grouped_iota(groups, count // groups, depth, 1) == target[1:2, :]
    chosen = jnp.where(whole | local_row, 1.0, 0.0).astype(bf16)
    out[...] = jnp.dot(chosen, rows, preferred_element_type=f32).astype(bf16)


def build_payload(places, target, queries, own_kv, residual, table, q_cols, col_width, count):
    tokens = queries.shape[0]

    def cols(width, which):
        return pl.BlockSpec((tokens, width), lambda i, at: (0, at[which]))

    def whole(x):
        return pl.BlockSpec(x.shape, lambda i, at: (0,) * x.ndim)

    return pl.pallas_call(
        payload_kernel,
        out_shape=jax.ShapeDtypeStruct((count, HD), bf16),
        grid_spec=pltpu.PrefetchScalarGridSpec(
            num_scalar_prefetch=1,
            grid=(1,),
            in_specs=[
                whole(target),
                cols(q_cols, 0),
                cols(HD, 1),
                cols(HD, 2),
                cols(col_width, 0),
                whole(table),
            ],
            out_specs=pl.BlockSpec((count, HD), lambda i, at: (0, 0)),
        ),
        cost_estimate=pl.CostEstimate(
            flops=2 * count * target.shape[1] * HD,
            bytes_accessed=4 * count * HD,
            transcendentals=0,
        ),
        compiler_params=pltpu.CompilerParams(vmem_limit_bytes=8 << 20),
        name="build_payload",
    )(places, target, queries, own_kv, own_kv, residual, table)


def attention_kernel(at, got, cache, attn, resid):
    tokens = attn.shape[0]
    heads = attn.shape[1] // HD
    chunks = heads + 2 + resid.shape[1] // HD
    blocks = tokens
    size = got.shape[0] // blocks
    rows = got[...]
    table_row = one_hot(
        lax.broadcasted_iota(i32, (blocks, got.shape[0]), 0) * size + 2 * chunks,
        (blocks, got.shape[0]),
        1,
    )
    prompts = jnp.dot(table_row, rows, preferred_element_type=f32)[:, :tokens]
    holds = jnp.max(jnp.where(prompts == at[0].astype(f32), 1.0, 0.0), 1, keepdims=True)
    before = jnp.where(
        lax.broadcasted_iota(i32, (blocks, blocks), 1)
        < lax.broadcasted_iota(i32, (blocks, blocks), 0),
        1.0,
        0.0,
    ).astype(bf16)
    wide = jnp.broadcast_to(holds, (blocks, HD)).astype(bf16)
    order = jnp.dot(before, wide, preferred_element_type=f32)
    order = jnp.where(wide > 0, order * 2.0, -1024.0).astype(bf16)
    spread = jnp.where(
        grouped_iota(blocks, size, blocks, 0)
        == lax.broadcasted_iota(i32, (blocks * size, blocks), 1),
        1.0,
        0.0,
    ).astype(bf16)
    order = jnp.dot(spread, order, preferred_element_type=f32)[:, :1].astype(i32)
    place = grouped_iota(blocks, size, 1, 1)
    second = jnp.where(place >= chunks, 1, 0)
    target = (place - second * chunks) * tokens + order + second
    target = jnp.where(place < 2 * chunks, target, -1)
    chosen = one_hot(target, (got.shape[0], chunks * tokens), 1)
    mine = lax.dot_general(
        chosen, rows, (((0,), (0,)), ((), ())), preferred_element_type=f32
    )

    def chunk(c):
        return mine[c * tokens : (c + 1) * tokens, :]

    k_own, v_own = chunk(heads), chunk(heads + 1)
    positions = cache.shape[0] * cache.shape[1]
    both = cache[...].reshape(positions, cache.shape[2])
    keys, values = both[:, :HD], both[:, HD:]
    inside = lax.broadcasted_iota(i32, (tokens, positions), 1) < at[1]
    scale = HD ** (-0.5)
    for h in range(heads):
        q = chunk(h)
        scores = (
            lax.dot_general(
                q.astype(bf16), keys, (((1,), (1,)), ((), ())), preferred_element_type=f32
            )
            * scale
        )
        scores = jnp.where(inside, scores, MASKED_SCORE)
        own = jnp.sum(q * k_own, 1, keepdims=True) * scale
        top = jnp.maximum(jnp.max(scores, 1, keepdims=True), own)
        weights = jnp.where(inside, jnp.exp(scores - top), 0.0)
        own_weight = jnp.exp(own - top)
        total = jnp.sum(weights, 1, keepdims=True) + own_weight
        mix = jnp.dot(weights.astype(bf16), values, preferred_element_type=f32)
        mix = (mix + own_weight * v_own) / total
        attn[:, h * HD : (h + 1) * HD] = mix.astype(bf16)
    for c in range(resid.shape[1] // HD):
        resid[:, c * HD : (c + 1) * HD] = chunk(heads + 2 + c).astype(bf16)


def attend(at, got, cache, tokens, q_cols, col_width):
    vmem = pl.BlockSpec(memory_space=pltpu.VMEM)
    return pl.pallas_call(
        attention_kernel,
        out_shape=(
            jax.ShapeDtypeStruct((tokens, q_cols), bf16),
            jax.ShapeDtypeStruct((tokens, col_width), bf16),
        ),
        in_specs=[pl.BlockSpec(memory_space=pltpu.SMEM), vmem, vmem],
        out_specs=(vmem, vmem),
        cost_estimate=pl.CostEstimate(
            flops=4 * got.size * 256, bytes_accessed=2 * got.size, transcendentals=0
        ),
        compiler_params=pltpu.CompilerParams(vmem_limit_bytes=8 << 20),
        name="attend",
    )(at, got, cache)


def hidden_kernel(parts, resid, out):
    hidden = resid[...].astype(f32)
    for s in range(parts.shape[0]):
        hidden = hidden + parts[s].astype(f32)
    hidden = hidden.astype(bf16)
    for d in range(out.shape[0]):
        out[d] = hidden


def hidden_copies(parts, resid, copies):
    vmem = pl.BlockSpec(memory_space=pltpu.VMEM)
    return pl.pallas_call(
        hidden_kernel,
        out_shape=jax.ShapeDtypeStruct((copies, *resid.shape), bf16),
        in_specs=[vmem, vmem],
        out_specs=vmem,
        cost_estimate=pl.CostEstimate(
            flops=parts.size, bytes_accessed=4 * parts.size, transcendentals=0
        ),
        compiler_params=pltpu.CompilerParams(vmem_limit_bytes=4 << 20),
        name="hidden_copies",
    )(parts, resid)


def select_kernel(experts_at, home_at, near, across, by_dest, home):
    half = near.shape[0]

    def picked(at):
        shape = (at.shape[0], half)
        return (
            jnp.dot(one_hot(at, shape, 1), near[...], preferred_element_type=f32)
            + jnp.dot(one_hot(at - half, shape, 1), across[...], preferred_element_type=f32)
        ).astype(bf16)

    home[...] = picked(home_at[...])
    count = by_dest.shape[1]
    kinds = experts_at.shape[0] // count
    for kind in range(kinds):
        rows = picked(experts_at[kind * count : (kind + 1) * count, :])
        for d in range(kind, by_dest.shape[0], kinds):
            by_dest[d] = rows


def select_rows(experts_at, home_at, near, across, n_x, kinds):
    vmem = pl.BlockSpec(memory_space=pltpu.VMEM)
    count, width = experts_at.shape[0] // kinds, near.shape[1]
    return pl.pallas_call(
        select_kernel,
        out_shape=(
            jax.ShapeDtypeStruct((n_x, count, width), bf16),
            jax.ShapeDtypeStruct((home_at.shape[0], width), bf16),
        ),
        in_specs=[vmem] * 4,
        out_specs=(vmem, vmem),
        cost_estimate=pl.CostEstimate(
            flops=4 * experts_at.shape[0] * near.size,
            bytes_accessed=4 * near.size,
            transcendentals=0,
        ),
        compiler_params=pltpu.CompilerParams(vmem_limit_bytes=8 << 20),
        name="select_rows",
    )(experts_at, home_at, near, across)


def projection_kernel(at, attn, mine_a, mine_b, theirs_a, theirs_b, out):
    half = mine_a.shape[0]
    chips = 2 * half
    first = at[1] == 0
    rows = attn[...]
    per_out = out.shape[2] // (2 * mine_a.shape[1])

    def block(use_zero, offset, kind):
        spot, n, bit = 0, 1, half // 2
        while bit:
            spot = spot + lax.rem(lax.div(offset, n), 2) * bit
            n, bit = 2 * n, bit // 2
        spot = spot * 2 + kind
        low = spot < half
        a, b = jnp.minimum(spot, half - 1), jnp.maximum(spot - half, 0)
        ours = jnp.where(low, mine_a[a], mine_b[b])
        return jnp.where(use_zero == first, ours, jnp.where(low, theirs_a[a], theirs_b[b]))

    for dest in range(out.shape[0]):
        blocks = []
        for near in range(per_out):
            ahead = lax.rem(dest * per_out + near + chips - at[0], chips)
            behind = lax.rem(chips - ahead, chips)
            zero = ahead < half
            blocks.append(
                block(zero, jnp.where(zero, ahead, behind - 1), jnp.where(zero, 0, 1))
            )
            one = (ahead >= 1) & (ahead <= half)
            blocks.append(
                block(one, jnp.where(one, ahead - 1, behind), jnp.where(one, 1, 0))
            )
        weight = jnp.concatenate(blocks, 0)
        out[dest] = lax.dot_general(
            rows, weight, (((1,), (1,)), ((), ())), preferred_element_type=f32
        ).astype(bf16)


def project_out(at, attn, halves, n_x, col_width):
    vmem = pl.BlockSpec(memory_space=pltpu.VMEM)
    size = sum(h.size for h in halves)
    return pl.pallas_call(
        projection_kernel,
        out_shape=jax.ShapeDtypeStruct((n_x, attn.shape[0], col_width), bf16),
        in_specs=[pl.BlockSpec(memory_space=pltpu.SMEM), *[vmem] * 5],
        out_specs=vmem,
        cost_estimate=pl.CostEstimate(
            flops=2 * attn.shape[0] * size, bytes_accessed=2 * size, transcendentals=0
        ),
        compiler_params=pltpu.CompilerParams(vmem_limit_bytes=8 << 20),
        name="project_out",
    )(at, attn, *halves)


def give_kernel(give, gate, up, down, out):
    out[0] = gate[0]
    out[1] = up[0]
    ff = down.shape[1]
    for t in range(down.shape[2] // HD):
        out[2, t * ff : (t + 1) * ff, :] = down[0, :, t * HD : (t + 1) * HD]


def give_weights(give, gate, up, down):
    def part(x):
        return pl.BlockSpec((1, *x.shape[1:]), lambda i, k: (k[0], 0, 0))

    shape = (3, *gate.shape[1:])
    return pl.pallas_call(
        give_kernel,
        out_shape=jax.ShapeDtypeStruct(shape, bf16),
        grid_spec=pltpu.PrefetchScalarGridSpec(
            num_scalar_prefetch=1,
            grid=(1,),
            in_specs=[part(gate), part(up), part(down)],
            out_specs=pl.BlockSpec(shape, lambda i, k: (0, 0, 0)),
        ),
        cost_estimate=pl.CostEstimate(
            flops=gate.size, bytes_accessed=6 * gate.size, transcendentals=0
        ),
        compiler_params=pltpu.CompilerParams(vmem_limit_bytes=12 << 20),
        name="give_weights",
    )(jnp.reshape(give, (1,)).astype(i32), gate, up, down)


def expert_kernel(keep, rows, gate, up, got, down_hbm, out, down, sem):
    n_x, count, col_width = rows.shape
    ff = gate.shape[2]
    copy = pltpu.make_async_copy(down_hbm.at[keep[0]], down, sem)
    copy.start()
    total = jnp.zeros((count, 4 * ff), f32)
    for s in range(n_x):
        at = pl.ds(s * col_width, col_width)
        weight = jnp.concatenate(
            [gate[0, at, :], got[0, at, :], up[0, at, :], got[1, at, :]], 1
        )
        total = total + jnp.dot(rows[s], weight, preferred_element_type=f32)
    gates, ups = total[:, : 2 * ff], total[:, 2 * ff :]
    act = (gates / (1.0 + jnp.exp(-gates)) * ups).astype(bf16)
    copy.wait()
    tiles = col_width // HD
    for d in range(n_x):
        theirs = [
            got[2, pl.ds((d * tiles + t) * ff, ff), :] for t in range(tiles)
        ]
        weight = jnp.concatenate(
            [down[:, pl.ds(d * col_width, col_width)], jnp.concatenate(theirs, 1)], 0
        )
        out[d] = jnp.dot(act, weight, preferred_element_type=f32).astype(bf16)


def run_expert(keep, rows, gate, up, down, got):
    def whole(x):
        return pl.BlockSpec(x.shape, lambda i, k: (0,) * x.ndim)

    def kept(x):
        return pl.BlockSpec((1, *x.shape[1:]), lambda i, k: (k[0], 0, 0))

    flops = 2 * rows.size * gate.shape[2] * 6
    moved = 2 * (2 * rows.size + got.size) + 3 * gate.size
    return pl.pallas_call(
        expert_kernel,
        out_shape=jax.ShapeDtypeStruct(rows.shape, bf16),
        grid_spec=pltpu.PrefetchScalarGridSpec(
            num_scalar_prefetch=1,
            grid=(1,),
            in_specs=[
                whole(rows),
                kept(gate),
                kept(up),
                whole(got),
                pl.BlockSpec(memory_space=pl.ANY),
            ],
            out_specs=whole(rows),
            scratch_shapes=[
                pltpu.VMEM(down.shape[1:], bf16),
                pltpu.SemaphoreType.DMA,
            ],
        ),
        cost_estimate=pl.CostEstimate(
            flops=flops, bytes_accessed=moved, transcendentals=rows.shape[1] * 2 * HD
        ),
        compiler_params=pltpu.CompilerParams(vmem_limit_bytes=16 << 20),
        name="run_expert",
    )(jnp.reshape(keep, (1,)).astype(i32), rows, gate, up, got, down)


def layer(
    queries,
    own_kv,
    prompt_cache,
    prompt_len,
    token_prompt,
    residual,
    out_weight,
    route_ids,
    route_weights,
    w_gate,
    w_up,
    w_down,
):
    n_e = lax.axis_size(EXPERT)
    n_x = lax.axis_size("tensor")
    chips = lax.axis_size("chip")
    pos_x = lax.axis_index("tensor")
    chip = lax.axis_index("chip")
    core = lax.axis_index("core")
    pos_e = chip * CORES + core
    tokens = queries.shape[0]
    half_cols = own_kv.shape[1] // 2
    kv_heads = half_cols // HD
    head_count = queries.shape[1] // HD
    group_size = head_count // kv_heads
    heads_here = head_count // n_x
    q_cols = heads_here * HD
    per_prompt = tokens // (n_e // 2)
    block_len = prompt_cache.shape[1]
    model_width = residual.shape[1]
    col_width = model_width // n_x
    picks = route_ids.shape[1]
    experts_here = w_gate.shape[0]
    experts = experts_here * n_e
    capacity = min(tokens, 3 * tokens * picks // (2 * experts))

    cache = prompt_cache[0].reshape(block_len, 2, kv_heads, HD)
    by_head = jnp.transpose(cache, (2, 0, 1, 3)).reshape(kv_heads, block_len, 2 * HD)
    by_head = jnp.repeat(by_head, n_x // kv_heads, axis=0)
    cache_all = exchange(by_head, "tensor")

    w_own = out_weight.T
    mine = jnp.stack([w_own, across_chips(w_own)])
    shift = chips // 4
    while shift > 1:
        mine = jnp.concatenate([mine, along_chips(mine, shift)])
        shift //= 2
    mine_b = along_chips(mine, 1)
    theirs_a = other_core(mine)
    theirs_b = other_core(mine_b)

    kv_pos = (pos_x * heads_here) // group_size
    earlier = jnp.arange(tokens)[None, :] < jnp.arange(tokens)[:, None]
    same = token_prompt[:, None] == token_prompt[None, :]
    rank = jnp.sum((same & earlier).astype(i32), 1)
    chunks = (q_cols + 2 * HD + col_width) // HD
    entries = jnp.concatenate(
        [jnp.pad(token_prompt, (0, HD - tokens)), route_ids.reshape(-1)]
    )
    table_rows = -(-entries.shape[0] // (8 * HD)) * 8
    table = jnp.pad(entries, (0, HD * HD - entries.shape[0])).astype(bf16).reshape(HD, HD)
    size = 2 * chunks + table_rows
    place = token_prompt * size + rank * chunks
    token_rows = (place[None, :] + jnp.arange(chunks, dtype=i32)[:, None]).reshape(-1)
    spare = jnp.arange(HD, dtype=i32)
    target = jnp.stack(
        [
            jnp.pad(token_rows, (0, HD), constant_values=-1),
            jnp.concatenate(
                [
                    jnp.full((tokens * chunks,), -1, i32),
                    jnp.where(spare < table_rows, 2 * chunks + spare, -1),
                ]
            ),
        ]
    )
    places = jnp.stack([pos_x, kv_pos, kv_heads + kv_pos]).astype(i32)
    sent = build_payload(
        places, target, queries, own_kv, residual, table, q_cols, col_width, n_e * size
    )
    sent, cache_all = lax.optimization_barrier((sent, cache_all))
    got = exchange(sent.reshape(n_e, size, HD), EXPERT)
    table = got[:, 2 * chunks : 2 * chunks + 1 + tokens * picks // HD, :].astype(i32)
    prompts = table[:, 0, :tokens]
    routes = table[:, 1:, :].reshape(n_e, tokens, picks)

    owner = jnp.arange(n_e, dtype=i32)
    holds = jnp.any(prompts[None, :, :] == owner[:, None, None], -1)
    order = count_earlier(holds)
    peers = prompts[:, :, None] == prompts[:, None, :]
    rank_all = jnp.sum((peers & earlier[None]).astype(i32), 2)
    block_order = jnp.sum(
        jnp.where(prompts[:, :, None] == owner, order.T[:, None, :], 0), 2
    )
    source = jnp.where(prompts % CORES == core, 0, chips) + prompts // CORES
    source = source * tokens + block_order * per_prompt + rank_all

    at = jnp.concatenate([jnp.stack([pos_e]).astype(i32), prompt_len])
    attn, resid = attend(
        at, got.reshape(n_e * size, HD), cache_all, tokens, q_cols, col_width
    )
    at = jnp.stack([chip, core]).astype(i32)
    partial = project_out(at, attn, (mine, mine_b, theirs_a, theirs_b), n_x, col_width)
    parts = exchange(partial, "tensor")
    hidden = hidden_copies(parts, resid, chips)

    keep = pos_x % experts_here
    give = 1 - keep
    swap = [(i, i ^ 1) for i in range(n_x)]
    giving = give_weights(give, w_gate, w_up, w_down)
    got_weights = lax.ppermute(giving, "tensor", swap)

    near = exchange(hidden, "chip")
    across = other_core(near)
    mine_e = pos_e * experts_here + jnp.arange(experts_here, dtype=i32)
    named = jnp.any(routes[None] == mine_e[:, None, None, None], -1)
    slot = jnp.where(named, count_earlier(named), -1)
    filled = slot[:, :, None, :] == jnp.arange(capacity, dtype=i32)[None, None, :, None]
    expert_rows = jnp.sum(jnp.where(filled, source[None, :, None, :] + 1, 0), -1) - 1
    home_rows = lax.dynamic_index_in_dim(source, pos_e, 0, keepdims=False)
    by_dest, hidden_home = select_rows(
        expert_rows.reshape(-1, 1),
        home_rows.reshape(-1, 1),
        near.reshape(chips * tokens, col_width),
        across.reshape(chips * tokens, col_width),
        n_x,
        experts_here,
    )
    rows_in = exchange(by_dest, "tensor")

    out = run_expert(keep, rows_in, w_gate, w_up, w_down, got_weights)
    parts = exchange(out, "tensor")
    parts = parts.reshape(n_x // experts_here, experts_here, n_e, capacity, col_width)
    summed = jnp.sum(parts.astype(f32), 0).astype(bf16)
    returned = exchange(jnp.transpose(summed, (1, 0, 2, 3)), EXPERT)

    hit = route_ids[:, :, None] == jnp.arange(experts, dtype=i32)
    marks = jnp.any(hit, 1)
    mark_weight = jnp.sum(jnp.where(hit, route_weights[:, :, None], 0.0), 1)
    slot = jnp.dot(
        earlier.astype(bf16), marks.astype(bf16), preferred_element_type=f32
    ).astype(i32)
    slot = jnp.where(marks, slot, -1)
    chosen = slot[:, :, None] == jnp.arange(capacity, dtype=i32)
    mix_rows = (chosen * mark_weight[:, :, None]).reshape(tokens, experts * capacity)
    expert_mix = jnp.dot(
        mix_rows,
        returned.reshape(experts * capacity, col_width).astype(f32),
        precision=lax.Precision.HIGHEST,
    )
    return (hidden_home.astype(f32) + expert_mix).astype(bf16)


def solution(mesh):
    split = Mesh(
        mesh.devices.reshape(
            mesh.shape["groups"],
            mesh.shape["expert"] // CORES,
            CORES,
            mesh.shape["tensor"],
        ),
        ("groups", *EXPERT, "tensor"),
    )
    whole = ("groups", *EXPERT)
    return jax.shard_map(
        layer,
        mesh=split,
        in_specs=(
            P(whole, None),
            P(whole, None),
            P(whole, "tensor", None),
            P(whole),
            P(whole),
            P(whole, None),
            P("tensor", EXPERT),
            P(whole, None),
            P(whole, None),
            P(EXPERT, None, "tensor"),
            P(EXPERT, None, "tensor"),
            P(EXPERT, "tensor", None),
        ),
        out_specs=P(whole, "tensor"),
        check_vma=False,
    )
```

```python
import jax
import jax.numpy as jnp
from jax import lax
from jax.experimental import pallas as pl
from jax.experimental.pallas import tpu as pltpu
from jax.sharding import Mesh
from jax.sharding import PartitionSpec as P

HD = 128
CORES = 2
EXPERT = ("chip", "core")
MASKED_SCORE = -1e30
f32, bf16, i32 = jnp.float32, jnp.bfloat16, jnp.int32


def exchange(tiles, axis):
    return lax.all_to_all(tiles, axis, split_axis=0, concat_axis=0, tiled=True)


def along_chips(x, shift):
    n = lax.axis_size("chip")
    moves = []
    for c in range(n):
        moves.append((c * CORES, (c - shift) % n * CORES))
        moves.append((c * CORES + 1, (c + shift) % n * CORES + 1))
    return lax.ppermute(x, EXPERT, moves)


def across_chips(x):
    n = lax.axis_size("chip")
    moves = []
    for c in range(n):
        moves.append((c * CORES, (c + 1) % n * CORES + 1))
        moves.append((c * CORES + 1, (c - 1) % n * CORES))
    return lax.ppermute(x, EXPERT, moves)


def other_core(x):
    return lax.ppermute(x, "core", [(0, 1), (1, 0)])


def count_earlier(marks):
    n = marks.shape[-1]
    before = (jnp.arange(n)[:, None] < jnp.arange(n)[None, :]).astype(bf16)
    return jnp.dot(marks.astype(bf16), before, preferred_element_type=f32).astype(i32)


def in_hbm(*arrays):
    return [pltpu.with_memory_space_constraint(x, pltpu.HBM) for x in arrays]


def one_hot(at, shape, dim):
    return jnp.where(lax.broadcasted_iota(i32, shape, dim) == at, 1.0, 0.0).astype(bf16)


def grouped_iota(groups, size, lanes, dim):
    at = lax.broadcasted_iota(i32, (groups, size, lanes), dim)
    return at.reshape(groups * size, lanes)


def payload_kernel(at, prompts, routes, queries, own_kv, residual, out, q, kv, resid, sem):
    tokens, q_cols = q.shape
    col_width = resid.shape[1]

    def cols(start, width):
        return pl.ds(pl.multiple_of(start, HD), width)

    copies = [
        pltpu.make_async_copy(queries.at[:, cols(at[0] * q_cols, q_cols)], q, sem.at[0]),
        pltpu.make_async_copy(own_kv.at[:, cols(at[1] * HD, HD)], kv.at[0], sem.at[1]),
        pltpu.make_async_copy(own_kv.at[:, cols(at[2] * HD, HD)], kv.at[1], sem.at[2]),
        pltpu.make_async_copy(
            residual.at[:, cols(at[0] * col_width, col_width)], resid, sem.at[3]
        ),
    ]
    for copy in copies:
        copy.start()
    count = out.shape[0]
    size = count // tokens
    chunks = (q_cols + 2 * HD + col_width) // HD
    depth = chunks * tokens + HD
    prompt = jnp.broadcast_to(prompts[...].astype(f32), (tokens, tokens))
    sub = lax.broadcasted_iota(i32, (tokens, tokens), 0)
    lane = lax.broadcasted_iota(i32, (tokens, tokens), 1)
    alike = (prompt == prompt.T) & (sub < lane)
    rank = jnp.sum(jnp.where(alike, 1.0, 0.0), 0, keepdims=True)
    both = jnp.concatenate(
        [jnp.broadcast_to(x, (8, tokens)) for x in (prompt[:1], rank)], 0
    )
    lanes = lax.broadcasted_iota(i32, (tokens, depth), 1)
    repeat = jnp.where(
        lax.rem(lanes, tokens) == lax.broadcasted_iota(i32, (tokens, depth), 0), 1.0, 0.0
    )
    spread = jnp.dot(both.astype(bf16), repeat.astype(bf16), preferred_element_type=f32)
    lanes = lax.broadcasted_iota(i32, (1, depth), 1)
    chunk = lax.div(lanes, tokens)
    place = spread[:1].astype(i32) * size + spread[8:9].astype(i32) * chunks + chunk
    place = jnp.where(chunk < chunks, place, -1)
    spare = lanes - chunks * tokens
    spare = jnp.where((spare >= 0) & (spare < size - 2 * chunks), 2 * chunks + spare, -1)
    whole = lax.broadcasted_iota(i32, (count, depth), 0) == place
    local_row = grouped_iota(tokens, size, depth, 1) == spare
    chosen = jnp.where(whole | local_row, 1.0, 0.0).astype(bf16)
    picks = routes.shape[0]
    at_lane = lax.broadcasted_iota(i32, (tokens, HD), 1)
    at_sub = lax.broadcasted_iota(i32, (tokens, HD), 0)
    first = jnp.where(at_lane == at_sub, 1.0, 0.0).astype(bf16)
    second = jnp.where(at_lane == at_sub + tokens, 1.0, 0.0).astype(bf16)
    table = jnp.dot(
        routes[...].astype(f32).astype(bf16), first, preferred_element_type=f32
    ) + jnp.dot(
        jnp.broadcast_to(prompt[:1], (picks, tokens)).astype(bf16),
        second,
        preferred_element_type=f32,
    )
    table = jnp.concatenate([table, jnp.zeros((HD - picks, HD), f32)], 0).astype(bf16)
    for copy in copies:
        copy.wait()
    rows = [q[:, c : c + HD] for c in range(0, q_cols, HD)]
    rows += [kv[0], kv[1]]
    rows += [resid[:, c : c + HD] for c in range(0, col_width, HD)]
    rows = jnp.concatenate([*rows, table], 0)
    out[...] = jnp.dot(chosen, rows, preferred_element_type=f32).astype(bf16)


def build_payload(at, prompts, routes, queries, own_kv, residual, q_cols, col_width, count):
    vmem = pl.BlockSpec(memory_space=pltpu.VMEM)
    hbm = pl.BlockSpec(memory_space=pltpu.HBM)
    tokens = queries.shape[0]
    return pl.pallas_call(
        payload_kernel,
        out_shape=jax.ShapeDtypeStruct((count, HD), bf16),
        in_specs=[pl.BlockSpec(memory_space=pltpu.SMEM), vmem, vmem, hbm, hbm, hbm],
        out_specs=vmem,
        scratch_shapes=[
            pltpu.VMEM((tokens, q_cols), bf16),
            pltpu.VMEM((2, tokens, HD), bf16),
            pltpu.VMEM((tokens, col_width), bf16),
            pltpu.SemaphoreType.DMA((4,)),
        ],
        cost_estimate=pl.CostEstimate(
            flops=2 * count * 384 * HD, bytes_accessed=4 * count * HD, transcendentals=0
        ),
        compiler_params=pltpu.CompilerParams(vmem_limit_bytes=6 << 20),
        name="build_payload",
    )(at, *in_hbm(prompts, routes, queries, own_kv, residual))


def cache_kernel(cache, out):
    copies, _, width = out.shape
    heads = cache.shape[2] // width
    for x in range(copies):
        g = x * heads // copies
        out[x, :, :HD] = cache[0, :, g * HD : (g + 1) * HD]
        out[x, :, HD:] = cache[0, :, (heads + g) * HD : (heads + g + 1) * HD]


def split_cache(cache, n_x):
    vmem = pl.BlockSpec(memory_space=pltpu.VMEM)
    return pl.pallas_call(
        cache_kernel,
        out_shape=jax.ShapeDtypeStruct((n_x, cache.shape[1], 2 * HD), bf16),
        in_specs=[vmem],
        out_specs=vmem,
        cost_estimate=pl.CostEstimate(
            flops=cache.size, bytes_accessed=6 * cache.size, transcendentals=0
        ),
        compiler_params=pltpu.CompilerParams(vmem_limit_bytes=2 << 20),
        name="split_cache",
    )(*in_hbm(cache))


def attention_kernel(at, got, cache, attn, resid):
    tokens = attn.shape[0]
    heads = attn.shape[1] // HD
    chunks = heads + 2 + resid.shape[1] // HD
    blocks = tokens
    size = got.shape[0] // blocks
    rows = got[...]
    table_row = one_hot(
        lax.broadcasted_iota(i32, (blocks, got.shape[0]), 0) * size + 2 * chunks,
        (blocks, got.shape[0]),
        1,
    )
    prompts = jnp.dot(table_row, rows, preferred_element_type=f32)
    lane = lax.broadcasted_iota(i32, prompts.shape, 1)
    prompts = jnp.where((lane >= tokens) & (lane < 2 * tokens), prompts, -1.0)
    holds = jnp.max(jnp.where(prompts == at[0].astype(f32), 1.0, 0.0), 1, keepdims=True)
    before = jnp.where(
        lax.broadcasted_iota(i32, (blocks, blocks), 1)
        < lax.broadcasted_iota(i32, (blocks, blocks), 0),
        1.0,
        0.0,
    ).astype(bf16)
    wide = jnp.broadcast_to(holds, (blocks, HD)).astype(bf16)
    order = jnp.dot(before, wide, preferred_element_type=f32)
    order = jnp.where(wide > 0, order * 2.0, -1024.0).astype(bf16)
    spread = jnp.where(
        grouped_iota(blocks, size, blocks, 0)
        == lax.broadcasted_iota(i32, (blocks * size, blocks), 1),
        1.0,
        0.0,
    ).astype(bf16)
    order = jnp.dot(spread, order, preferred_element_type=f32)[:, :1].astype(i32)
    place = grouped_iota(blocks, size, 1, 1)
    second = jnp.where(place >= chunks, 1, 0)
    target = (place - second * chunks) * tokens + order + second
    target = jnp.where(place < 2 * chunks, target, -1)
    chosen = one_hot(target, (got.shape[0], chunks * tokens), 1)
    mine = lax.dot_general(
        chosen, rows, (((0,), (0,)), ((), ())), preferred_element_type=f32
    )

    def chunk(c):
        return mine[c * tokens : (c + 1) * tokens, :]

    k_own, v_own = chunk(heads), chunk(heads + 1)
    positions = cache.shape[0] * cache.shape[1]
    both = cache[...].reshape(positions, cache.shape[2])
    keys, values = both[:, :HD], both[:, HD:]
    inside = lax.broadcasted_iota(i32, (tokens, positions), 1) < at[1]
    scale = HD ** (-0.5)
    for h in range(heads):
        q = chunk(h)
        scores = (
            lax.dot_general(
                q.astype(bf16), keys, (((1,), (1,)), ((), ())), preferred_element_type=f32
            )
            * scale
        )
        scores = jnp.where(inside, scores, MASKED_SCORE)
        own = jnp.sum(q * k_own, 1, keepdims=True) * scale
        top = jnp.maximum(jnp.max(scores, 1, keepdims=True), own)
        weights = jnp.where(inside, jnp.exp(scores - top), 0.0)
        own_weight = jnp.exp(own - top)
        total = jnp.sum(weights, 1, keepdims=True) + own_weight
        mix = jnp.dot(weights.astype(bf16), values, preferred_element_type=f32)
        mix = (mix + own_weight * v_own) / total
        attn[:, h * HD : (h + 1) * HD] = mix.astype(bf16)
    for c in range(resid.shape[1] // HD):
        resid[:, c * HD : (c + 1) * HD] = chunk(heads + 2 + c).astype(bf16)


def attend(at, got, cache, tokens, q_cols, col_width):
    vmem = pl.BlockSpec(memory_space=pltpu.VMEM)
    return pl.pallas_call(
        attention_kernel,
        out_shape=(
            jax.ShapeDtypeStruct((tokens, q_cols), bf16),
            jax.ShapeDtypeStruct((tokens, col_width), bf16),
        ),
        in_specs=[pl.BlockSpec(memory_space=pltpu.SMEM), vmem, vmem],
        out_specs=(vmem, vmem),
        cost_estimate=pl.CostEstimate(
            flops=4 * got.size * 256, bytes_accessed=2 * got.size, transcendentals=0
        ),
        compiler_params=pltpu.CompilerParams(vmem_limit_bytes=8 << 20),
        name="attend",
    )(at, got, cache)


def hidden_kernel(parts, resid, out):
    hidden = resid[...].astype(f32)
    for s in range(parts.shape[0]):
        hidden = hidden + parts[s].astype(f32)
    hidden = hidden.astype(bf16)
    for d in range(out.shape[0]):
        out[d] = hidden


def hidden_copies(parts, resid, copies):
    vmem = pl.BlockSpec(memory_space=pltpu.VMEM)
    return pl.pallas_call(
        hidden_kernel,
        out_shape=jax.ShapeDtypeStruct((copies, *resid.shape), bf16),
        in_specs=[vmem, vmem],
        out_specs=vmem,
        cost_estimate=pl.CostEstimate(
            flops=parts.size, bytes_accessed=4 * parts.size, transcendentals=0
        ),
        compiler_params=pltpu.CompilerParams(vmem_limit_bytes=4 << 20),
        name="hidden_copies",
    )(parts, resid)


def select_kernel(experts_at, home_at, near, across, by_dest, home):
    half = near.shape[0]

    def picked(at):
        shape = (at.shape[0], half)
        return (
            jnp.dot(one_hot(at, shape, 1), near[...], preferred_element_type=f32)
            + jnp.dot(one_hot(at - half, shape, 1), across[...], preferred_element_type=f32)
        ).astype(bf16)

    home[...] = picked(home_at[...])
    count = by_dest.shape[1]
    kinds = experts_at.shape[0] // count
    for kind in range(kinds):
        rows = picked(experts_at[kind * count : (kind + 1) * count, :])
        for d in range(kind, by_dest.shape[0], kinds):
            by_dest[d] = rows


def select_rows(experts_at, home_at, near, across, n_x, kinds):
    vmem = pl.BlockSpec(memory_space=pltpu.VMEM)
    count, width = experts_at.shape[0] // kinds, near.shape[1]
    return pl.pallas_call(
        select_kernel,
        out_shape=(
            jax.ShapeDtypeStruct((n_x, count, width), bf16),
            jax.ShapeDtypeStruct((home_at.shape[0], width), bf16),
        ),
        in_specs=[vmem] * 4,
        out_specs=(vmem, vmem),
        cost_estimate=pl.CostEstimate(
            flops=4 * experts_at.shape[0] * near.size,
            bytes_accessed=4 * near.size,
            transcendentals=0,
        ),
        compiler_params=pltpu.CompilerParams(vmem_limit_bytes=8 << 20),
        name="select_rows",
    )(experts_at, home_at, near, across)


def projection_kernel(at, attn, mine_a, mine_b, theirs_a, theirs_b, out):
    half = mine_a.shape[0]
    chips = 2 * half
    first = at[1] == 0
    rows = attn[...]
    per_out = out.shape[2] // (2 * mine_a.shape[1])

    def block(use_zero, offset, kind):
        spot, n, bit = 0, 1, half // 2
        while bit:
            spot = spot + lax.rem(lax.div(offset, n), 2) * bit
            n, bit = 2 * n, bit // 2
        spot = spot * 2 + kind
        low = spot < half
        a, b = jnp.minimum(spot, half - 1), jnp.maximum(spot - half, 0)
        ours = jnp.where(low, mine_a[a], mine_b[b])
        return jnp.where(use_zero == first, ours, jnp.where(low, theirs_a[a], theirs_b[b]))

    for dest in range(out.shape[0]):
        blocks = []
        for near in range(per_out):
            ahead = lax.rem(dest * per_out + near + chips - at[0], chips)
            behind = lax.rem(chips - ahead, chips)
            zero = ahead < half
            blocks.append(
                block(zero, jnp.where(zero, ahead, behind - 1), jnp.where(zero, 0, 1))
            )
            one = (ahead >= 1) & (ahead <= half)
            blocks.append(
                block(one, jnp.where(one, ahead - 1, behind), jnp.where(one, 1, 0))
            )
        weight = jnp.concatenate(blocks, 0)
        out[dest] = lax.dot_general(
            rows, weight, (((1,), (1,)), ((), ())), preferred_element_type=f32
        ).astype(bf16)


def project_out(at, attn, halves, n_x, col_width):
    vmem = pl.BlockSpec(memory_space=pltpu.VMEM)
    size = sum(h.size for h in halves)
    return pl.pallas_call(
        projection_kernel,
        out_shape=jax.ShapeDtypeStruct((n_x, attn.shape[0], col_width), bf16),
        in_specs=[pl.BlockSpec(memory_space=pltpu.SMEM), *[vmem] * 5],
        out_specs=vmem,
        cost_estimate=pl.CostEstimate(
            flops=2 * attn.shape[0] * size, bytes_accessed=2 * size, transcendentals=0
        ),
        compiler_params=pltpu.CompilerParams(vmem_limit_bytes=8 << 20),
        name="project_out",
    )(at, attn, *halves)


def give_kernel(give, gate, up, down, out, mid, sem):
    ff = down.shape[1]
    third = pltpu.make_async_copy(down.at[give[0]], mid, sem.at[0])
    copies = [
        pltpu.make_async_copy(gate.at[give[0]], out.at[0], sem.at[1]),
        pltpu.make_async_copy(up.at[give[0]], out.at[1], sem.at[2]),
    ]
    third.start()
    for copy in copies:
        copy.start()
    third.wait()
    for t in range(down.shape[2] // HD):
        out[2, t * ff : (t + 1) * ff, :] = mid[:, t * HD : (t + 1) * HD]
    for copy in copies:
        copy.wait()


def give_weights(give, gate, up, down):
    hbm = pl.BlockSpec(memory_space=pltpu.HBM)
    return pl.pallas_call(
        give_kernel,
        out_shape=jax.ShapeDtypeStruct((3, *gate.shape[1:]), bf16),
        in_specs=[pl.BlockSpec(memory_space=pltpu.SMEM), hbm, hbm, hbm],
        out_specs=pl.BlockSpec(memory_space=pltpu.VMEM),
        scratch_shapes=[
            pltpu.VMEM(down.shape[1:], bf16),
            pltpu.SemaphoreType.DMA((3,)),
        ],
        cost_estimate=pl.CostEstimate(
            flops=gate.size, bytes_accessed=6 * gate.size, transcendentals=0
        ),
        compiler_params=pltpu.CompilerParams(vmem_limit_bytes=6 << 20),
        name="give_weights",
    )(jnp.reshape(give, (1,)).astype(i32), *in_hbm(gate, up, down))


def expert_kernel(keep, rows, got, gate_hbm, up_hbm, down_hbm, out, pair, down, sem):
    n_x, count, col_width = rows.shape
    ff = pair.shape[2]
    copies = [
        pltpu.make_async_copy(gate_hbm.at[keep[0]], pair.at[0], sem.at[0]),
        pltpu.make_async_copy(up_hbm.at[keep[0]], pair.at[1], sem.at[1]),
        pltpu.make_async_copy(down_hbm.at[keep[0]], down, sem.at[2]),
    ]
    for copy in copies:
        copy.start()
    copies[0].wait()
    copies[1].wait()
    total = jnp.zeros((count, 4 * ff), f32)
    for s in range(n_x):
        at = pl.ds(s * col_width, col_width)
        weight = jnp.concatenate(
            [pair[0, at, :], got[0, at, :], pair[1, at, :], got[1, at, :]], 1
        )
        total = total + jnp.dot(rows[s], weight, preferred_element_type=f32)
    gates, ups = total[:, : 2 * ff], total[:, 2 * ff :]
    act = (gates / (1.0 + jnp.exp(-gates)) * ups).astype(bf16)
    copies[2].wait()
    tiles = col_width // HD
    for d in range(n_x):
        theirs = [
            got[2, pl.ds((d * tiles + t) * ff, ff), :] for t in range(tiles)
        ]
        weight = jnp.concatenate(
            [down[:, pl.ds(d * col_width, col_width)], jnp.concatenate(theirs, 1)], 0
        )
        out[d] = jnp.dot(act, weight, preferred_element_type=f32).astype(bf16)


def run_expert(keep, rows, gate, up, down, got):
    vmem = pl.BlockSpec(memory_space=pltpu.VMEM)
    hbm = pl.BlockSpec(memory_space=pltpu.HBM)
    flops = 2 * rows.size * gate.shape[2] * 6
    moved = 2 * (2 * rows.size + got.size) + 3 * gate.size
    return pl.pallas_call(
        expert_kernel,
        out_shape=jax.ShapeDtypeStruct(rows.shape, bf16),
        in_specs=[pl.BlockSpec(memory_space=pltpu.SMEM), vmem, vmem, hbm, hbm, hbm],
        out_specs=vmem,
        scratch_shapes=[
            pltpu.VMEM((2, *gate.shape[1:]), bf16),
            pltpu.VMEM(down.shape[1:], bf16),
            pltpu.SemaphoreType.DMA((3,)),
        ],
        cost_estimate=pl.CostEstimate(
            flops=flops, bytes_accessed=moved, transcendentals=rows.shape[1] * 2 * HD
        ),
        compiler_params=pltpu.CompilerParams(vmem_limit_bytes=12 << 20),
        name="run_expert",
    )(jnp.reshape(keep, (1,)).astype(i32), rows, got, *in_hbm(gate, up, down))


def layer(
    queries,
    own_kv,
    prompt_cache,
    prompt_len,
    token_prompt,
    residual,
    out_weight,
    route_ids,
    route_weights,
    w_gate,
    w_up,
    w_down,
):
    n_e = lax.axis_size(EXPERT)
    n_x = lax.axis_size("tensor")
    chips = lax.axis_size("chip")
    pos_x = lax.axis_index("tensor")
    chip = lax.axis_index("chip")
    core = lax.axis_index("core")
    pos_e = chip * CORES + core
    tokens = queries.shape[0]
    half_cols = own_kv.shape[1] // 2
    kv_heads = half_cols // HD
    head_count = queries.shape[1] // HD
    group_size = head_count // kv_heads
    heads_here = head_count // n_x
    q_cols = heads_here * HD
    per_prompt = tokens // (n_e // 2)
    model_width = residual.shape[1]
    col_width = model_width // n_x
    picks = route_ids.shape[1]
    experts_here = w_gate.shape[0]
    experts = experts_here * n_e
    capacity = min(tokens, 3 * tokens * picks // (2 * experts))

    by_head = split_cache(prompt_cache, n_x)
    cache_all = exchange(by_head, "tensor")

    w_own = out_weight.T
    mine = jnp.stack([w_own, across_chips(w_own)])
    shift = chips // 4
    while shift > 1:
        mine = jnp.concatenate([mine, along_chips(mine, shift)])
        shift //= 2
    mine_b = along_chips(mine, 1)
    theirs_a = other_core(mine)
    theirs_b = other_core(mine_b)

    kv_pos = (pos_x * heads_here) // group_size
    earlier = jnp.arange(tokens)[None, :] < jnp.arange(tokens)[:, None]
    chunks = (q_cols + 2 * HD + col_width) // HD
    size = 2 * chunks + picks
    at = jnp.stack([pos_x, kv_pos, kv_heads + kv_pos]).astype(i32)
    sent = build_payload(
        at,
        token_prompt.reshape(1, tokens),
        route_ids.T,
        queries,
        own_kv,
        residual,
        q_cols,
        col_width,
        n_e * size,
    )
    sent, cache_all = lax.optimization_barrier((sent, cache_all))
    got = exchange(sent.reshape(n_e, size, HD), EXPERT)
    table = got[:, 2 * chunks :, :].astype(i32)
    prompts = table[:, 0, tokens : 2 * tokens]
    routes = table[:, :, :tokens]

    owner = jnp.arange(n_e, dtype=i32)
    holds = jnp.any(prompts[None, :, :] == owner[:, None, None], -1)
    order = count_earlier(holds)
    peers = prompts[:, :, None] == prompts[:, None, :]
    rank_all = jnp.sum((peers & earlier[None]).astype(i32), 2)
    block_order = jnp.sum(
        jnp.where(prompts[:, :, None] == owner, order.T[:, None, :], 0), 2
    )
    source = jnp.where(prompts % CORES == core, 0, chips) + prompts // CORES
    source = source * tokens + block_order * per_prompt + rank_all

    at = jnp.concatenate([jnp.stack([pos_e]).astype(i32), prompt_len])
    attn, resid = attend(
        at, got.reshape(n_e * size, HD), cache_all, tokens, q_cols, col_width
    )
    at = jnp.stack([chip, core]).astype(i32)
    partial = project_out(at, attn, (mine, mine_b, theirs_a, theirs_b), n_x, col_width)
    parts = exchange(partial, "tensor")
    hidden = hidden_copies(parts, resid, chips)

    keep = pos_x % experts_here
    give = 1 - keep
    swap = [(i, i ^ 1) for i in range(n_x)]
    giving = give_weights(give, w_gate, w_up, w_down)
    got_weights = lax.ppermute(giving, "tensor", swap)

    near = exchange(hidden, "chip")
    across = other_core(near)
    mine_e = pos_e * experts_here + jnp.arange(experts_here, dtype=i32)
    named = jnp.any(routes[None] == mine_e[:, None, None, None], 2)
    slot = jnp.where(named, count_earlier(named), -1)
    filled = slot[:, :, None, :] == jnp.arange(capacity, dtype=i32)[None, None, :, None]
    expert_rows = jnp.sum(jnp.where(filled, source[None, :, None, :] + 1, 0), -1) - 1
    home_rows = lax.dynamic_index_in_dim(source, pos_e, 0, keepdims=False)
    by_dest, hidden_home = select_rows(
        expert_rows.reshape(-1, 1),
        home_rows.reshape(-1, 1),
        near.reshape(chips * tokens, col_width),
        across.reshape(chips * tokens, col_width),
        n_x,
        experts_here,
    )
    rows_in = exchange(by_dest, "tensor")

    out = run_expert(keep, rows_in, w_gate, w_up, w_down, got_weights)
    parts = exchange(out, "tensor")
    parts = parts.reshape(n_x // experts_here, experts_here, n_e, capacity, col_width)
    summed = jnp.sum(parts.astype(f32), 0).astype(bf16)
    returned = exchange(jnp.transpose(summed, (1, 0, 2, 3)), EXPERT)

    hit = route_ids[:, :, None] == jnp.arange(experts, dtype=i32)
    marks = jnp.any(hit, 1)
    mark_weight = jnp.sum(jnp.where(hit, route_weights[:, :, None], 0.0), 1)
    slot = jnp.dot(
        earlier.astype(bf16), marks.astype(bf16), preferred_element_type=f32
    ).astype(i32)
    slot = jnp.where(marks, slot, -1)
    chosen = slot[:, :, None] == jnp.arange(capacity, dtype=i32)
    mix_rows = (chosen * mark_weight[:, :, None]).reshape(tokens, experts * capacity)
    expert_mix = jnp.dot(
        mix_rows,
        returned.reshape(experts * capacity, col_width).astype(f32),
        precision=lax.Precision.HIGHEST,
    )
    return (hidden_home.astype(f32) + expert_mix).astype(bf16)


def solution(mesh):
    split = Mesh(
        mesh.devices.reshape(
            mesh.shape["groups"],
            mesh.shape["expert"] // CORES,
            CORES,
            mesh.shape["tensor"],
        ),
        ("groups", *EXPERT, "tensor"),
    )
    whole = ("groups", *EXPERT)
    return jax.shard_map(
        layer,
        mesh=split,
        in_specs=(
            P(whole, None),
            P(whole, None),
            P(whole, "tensor", None),
            P(whole),
            P(whole),
            P(whole, None),
            P("tensor", EXPERT),
            P(whole, None),
            P(whole, None),
            P(EXPERT, None, "tensor"),
            P(EXPERT, None, "tensor"),
            P(EXPERT, "tensor", None),
        ),
        out_specs=P(whole, "tensor"),
        check_vma=False,
    )
```

```python
import jax
import jax.numpy as jnp
from jax import lax
from jax.experimental import pallas as pl
from jax.experimental.pallas import tpu as pltpu
from jax.sharding import Mesh
from jax.sharding import PartitionSpec as P

HD = 128
CORES = 2
EXPERT = ("chip", "core")
MASKED_SCORE = -1e30
f32, bf16, i32 = jnp.float32, jnp.bfloat16, jnp.int32


def exchange(tiles, axis):
    return lax.all_to_all(tiles, axis, split_axis=0, concat_axis=0, tiled=True)


def along_chips(x, shift):
    n = lax.axis_size("chip")
    moves = []
    for c in range(n):
        moves.append((c * CORES, (c - shift) % n * CORES))
        moves.append((c * CORES + 1, (c + shift) % n * CORES + 1))
    return lax.ppermute(x, EXPERT, moves)


def across_chips(x, shift):
    n = lax.axis_size("chip")
    moves = []
    for c in range(n):
        moves.append((c * CORES, (c + shift) % n * CORES + 1))
        moves.append((c * CORES + 1, (c - shift) % n * CORES))
    return lax.ppermute(x, EXPERT, moves)


def other_core(x):
    return lax.ppermute(x, "core", [(0, 1), (1, 0)])


def count_earlier(marks):
    n = marks.shape[-1]
    before = (jnp.arange(n)[:, None] < jnp.arange(n)[None, :]).astype(bf16)
    return jnp.dot(marks.astype(bf16), before, preferred_element_type=f32).astype(i32)


def in_hbm(*arrays):
    return [pltpu.with_memory_space_constraint(x, pltpu.HBM) for x in arrays]


def one_hot(at, shape, dim):
    return jnp.where(lax.broadcasted_iota(i32, shape, dim) == at, 1.0, 0.0).astype(bf16)


def grouped_iota(groups, size, lanes, dim):
    at = lax.broadcasted_iota(i32, (groups, size, lanes), dim)
    return at.reshape(groups * size, lanes)


def payload_kernel(at, prompts, routes, queries, own_kv, residual, out, q, kv, resid, sem):
    tokens, q_cols = q.shape
    col_width = resid.shape[1]

    def cols(start, width):
        return pl.ds(pl.multiple_of(start, HD), width)

    copies = [
        pltpu.make_async_copy(queries.at[:, cols(at[0] * q_cols, q_cols)], q, sem.at[0]),
        pltpu.make_async_copy(own_kv.at[:, cols(at[1] * HD, HD)], kv.at[0], sem.at[1]),
        pltpu.make_async_copy(own_kv.at[:, cols(at[2] * HD, HD)], kv.at[1], sem.at[2]),
        pltpu.make_async_copy(
            residual.at[:, cols(at[0] * col_width, col_width)], resid, sem.at[3]
        ),
    ]
    for copy in copies:
        copy.start()
    count = out.shape[0]
    size = count // tokens
    chunks = (q_cols + 2 * HD + col_width) // HD
    depth = chunks * tokens + HD
    prompt = jnp.broadcast_to(prompts[...].astype(f32), (tokens, tokens))
    sub = lax.broadcasted_iota(i32, (tokens, tokens), 0)
    lane = lax.broadcasted_iota(i32, (tokens, tokens), 1)
    alike = (prompt == prompt.T) & (sub < lane)
    rank = jnp.sum(jnp.where(alike, 1.0, 0.0), 0, keepdims=True)
    both = jnp.concatenate(
        [jnp.broadcast_to(x, (8, tokens)) for x in (prompt[:1], rank)], 0
    )
    lanes = lax.broadcasted_iota(i32, (tokens, depth), 1)
    repeat = jnp.where(
        lax.rem(lanes, tokens) == lax.broadcasted_iota(i32, (tokens, depth), 0), 1.0, 0.0
    )
    spread = jnp.dot(both.astype(bf16), repeat.astype(bf16), preferred_element_type=f32)
    lanes = lax.broadcasted_iota(i32, (1, depth), 1)
    chunk = lax.div(lanes, tokens)
    place = spread[:1].astype(i32) * size + spread[8:9].astype(i32) * chunks + chunk
    place = jnp.where(chunk < chunks, place, -1)
    spare = lanes - chunks * tokens
    spare = jnp.where((spare >= 0) & (spare < size - 2 * chunks), 2 * chunks + spare, -1)
    whole = lax.broadcasted_iota(i32, (count, depth), 0) == place
    local_row = grouped_iota(tokens, size, depth, 1) == spare
    chosen = jnp.where(whole | local_row, 1.0, 0.0).astype(bf16)
    picks = routes.shape[0]
    at_lane = lax.broadcasted_iota(i32, (tokens, HD), 1)
    at_sub = lax.broadcasted_iota(i32, (tokens, HD), 0)
    first = jnp.where(at_lane == at_sub, 1.0, 0.0).astype(bf16)
    second = jnp.where(at_lane == at_sub + tokens, 1.0, 0.0).astype(bf16)
    table = jnp.dot(
        routes[...].astype(f32).astype(bf16), first, preferred_element_type=f32
    ) + jnp.dot(
        jnp.broadcast_to(prompt[:1], (picks, tokens)).astype(bf16),
        second,
        preferred_element_type=f32,
    )
    table = jnp.concatenate([table, jnp.zeros((HD - picks, HD), f32)], 0).astype(bf16)
    for copy in copies:
        copy.wait()
    rows = [q[:, c : c + HD] for c in range(0, q_cols, HD)]
    rows += [kv[0], kv[1]]
    rows += [resid[:, c : c + HD] for c in range(0, col_width, HD)]
    rows = jnp.concatenate([*rows, table], 0)
    out[...] = jnp.dot(chosen, rows, preferred_element_type=f32).astype(bf16)


def build_payload(at, prompts, routes, queries, own_kv, residual, q_cols, col_width, count):
    vmem = pl.BlockSpec(memory_space=pltpu.VMEM)
    hbm = pl.BlockSpec(memory_space=pltpu.HBM)
    tokens = queries.shape[0]
    return pl.pallas_call(
        payload_kernel,
        out_shape=jax.ShapeDtypeStruct((count, HD), bf16),
        in_specs=[pl.BlockSpec(memory_space=pltpu.SMEM), vmem, vmem, hbm, hbm, hbm],
        out_specs=vmem,
        scratch_shapes=[
            pltpu.VMEM((tokens, q_cols), bf16),
            pltpu.VMEM((2, tokens, HD), bf16),
            pltpu.VMEM((tokens, col_width), bf16),
            pltpu.SemaphoreType.DMA((4,)),
        ],
        cost_estimate=pl.CostEstimate(
            flops=2 * count * 384 * HD, bytes_accessed=4 * count * HD, transcendentals=0
        ),
        compiler_params=pltpu.CompilerParams(vmem_limit_bytes=6 << 20),
        name="build_payload",
    )(at, *in_hbm(prompts, routes, queries, own_kv, residual))


def cache_kernel(cache, out):
    copies, _, width = out.shape
    heads = cache.shape[2] // width
    for x in range(copies):
        g = x * heads // copies
        out[x, :, :HD] = cache[0, :, g * HD : (g + 1) * HD]
        out[x, :, HD:] = cache[0, :, (heads + g) * HD : (heads + g + 1) * HD]


def split_cache(cache, n_x):
    vmem = pl.BlockSpec(memory_space=pltpu.VMEM)
    return pl.pallas_call(
        cache_kernel,
        out_shape=jax.ShapeDtypeStruct((n_x, cache.shape[1], 2 * HD), bf16),
        in_specs=[vmem],
        out_specs=vmem,
        cost_estimate=pl.CostEstimate(
            flops=cache.size, bytes_accessed=6 * cache.size, transcendentals=0
        ),
        compiler_params=pltpu.CompilerParams(vmem_limit_bytes=2 << 20),
        name="split_cache",
    )(*in_hbm(cache))


def attention_kernel(at, got, cache, attn, resid):
    tokens = attn.shape[0]
    heads = attn.shape[1] // HD
    chunks = heads + 2 + resid.shape[1] // HD
    blocks = tokens
    size = got.shape[0] // blocks
    rows = got[...]
    table_row = one_hot(
        lax.broadcasted_iota(i32, (blocks, got.shape[0]), 0) * size + 2 * chunks,
        (blocks, got.shape[0]),
        1,
    )
    prompts = jnp.dot(table_row, rows, preferred_element_type=f32)
    lane = lax.broadcasted_iota(i32, prompts.shape, 1)
    prompts = jnp.where((lane >= tokens) & (lane < 2 * tokens), prompts, -1.0)
    holds = jnp.max(jnp.where(prompts == at[0].astype(f32), 1.0, 0.0), 1, keepdims=True)
    before = jnp.where(
        lax.broadcasted_iota(i32, (blocks, blocks), 1)
        < lax.broadcasted_iota(i32, (blocks, blocks), 0),
        1.0,
        0.0,
    ).astype(bf16)
    wide = jnp.broadcast_to(holds, (blocks, HD)).astype(bf16)
    order = jnp.dot(before, wide, preferred_element_type=f32)
    order = jnp.where(wide > 0, order * 2.0, -1024.0).astype(bf16)
    spread = jnp.where(
        grouped_iota(blocks, size, blocks, 0)
        == lax.broadcasted_iota(i32, (blocks * size, blocks), 1),
        1.0,
        0.0,
    ).astype(bf16)
    order = jnp.dot(spread, order, preferred_element_type=f32)[:, :1].astype(i32)
    place = grouped_iota(blocks, size, 1, 1)
    second = jnp.where(place >= chunks, 1, 0)
    target = (place - second * chunks) * tokens + order + second
    target = jnp.where(place < 2 * chunks, target, -1)
    chosen = one_hot(target, (got.shape[0], chunks * tokens), 1)
    mine = lax.dot_general(
        chosen, rows, (((0,), (0,)), ((), ())), preferred_element_type=f32
    )

    def chunk(c):
        return mine[c * tokens : (c + 1) * tokens, :]

    k_own, v_own = chunk(heads), chunk(heads + 1)
    positions = cache.shape[0] * cache.shape[1]
    both = cache[...].reshape(positions, cache.shape[2])
    keys, values = both[:, :HD], both[:, HD:]
    inside = lax.broadcasted_iota(i32, (tokens, positions), 1) < at[1]
    scale = HD ** (-0.5)
    for h in range(heads):
        q = chunk(h)
        scores = (
            lax.dot_general(
                q.astype(bf16), keys, (((1,), (1,)), ((), ())), preferred_element_type=f32
            )
            * scale
        )
        scores = jnp.where(inside, scores, MASKED_SCORE)
        own = jnp.sum(q * k_own, 1, keepdims=True) * scale
        top = jnp.maximum(jnp.max(scores, 1, keepdims=True), own)
        weights = jnp.where(inside, jnp.exp(scores - top), 0.0)
        own_weight = jnp.exp(own - top)
        total = jnp.sum(weights, 1, keepdims=True) + own_weight
        mix = jnp.dot(weights.astype(bf16), values, preferred_element_type=f32)
        mix = (mix + own_weight * v_own) / total
        attn[:, h * HD : (h + 1) * HD] = mix.astype(bf16)
    for c in range(resid.shape[1] // HD):
        resid[:, c * HD : (c + 1) * HD] = chunk(heads + 2 + c).astype(bf16)


def attend(at, got, cache, tokens, q_cols, col_width):
    vmem = pl.BlockSpec(memory_space=pltpu.VMEM)
    return pl.pallas_call(
        attention_kernel,
        out_shape=(
            jax.ShapeDtypeStruct((tokens, q_cols), bf16),
            jax.ShapeDtypeStruct((tokens, col_width), bf16),
        ),
        in_specs=[pl.BlockSpec(memory_space=pltpu.SMEM), vmem, vmem],
        out_specs=(vmem, vmem),
        cost_estimate=pl.CostEstimate(
            flops=4 * got.size * 256, bytes_accessed=2 * got.size, transcendentals=0
        ),
        compiler_params=pltpu.CompilerParams(vmem_limit_bytes=8 << 20),
        name="attend",
    )(at, got, cache)


def hidden_kernel(parts, resid, out):
    hidden = resid[...].astype(f32)
    for s in range(parts.shape[0]):
        hidden = hidden + parts[s].astype(f32)
    hidden = hidden.astype(bf16)
    for d in range(out.shape[0]):
        out[d] = hidden


def hidden_copies(parts, resid, copies):
    vmem = pl.BlockSpec(memory_space=pltpu.VMEM)
    return pl.pallas_call(
        hidden_kernel,
        out_shape=jax.ShapeDtypeStruct((copies, *resid.shape), bf16),
        in_specs=[vmem, vmem],
        out_specs=vmem,
        cost_estimate=pl.CostEstimate(
            flops=parts.size, bytes_accessed=4 * parts.size, transcendentals=0
        ),
        compiler_params=pltpu.CompilerParams(vmem_limit_bytes=4 << 20),
        name="hidden_copies",
    )(parts, resid)


def select_kernel(experts_at, home_at, near, across, by_dest, home):
    half = near.shape[0]

    def picked(at):
        shape = (at.shape[0], half)
        return (
            jnp.dot(one_hot(at, shape, 1), near[...], preferred_element_type=f32)
            + jnp.dot(one_hot(at - half, shape, 1), across[...], preferred_element_type=f32)
        ).astype(bf16)

    home[...] = picked(home_at[...])
    count = by_dest.shape[1]
    kinds = experts_at.shape[0] // count
    for kind in range(kinds):
        rows = picked(experts_at[kind * count : (kind + 1) * count, :])
        for d in range(kind, by_dest.shape[0], kinds):
            by_dest[d] = rows


def select_rows(experts_at, home_at, near, across, n_x, kinds):
    vmem = pl.BlockSpec(memory_space=pltpu.VMEM)
    count, width = experts_at.shape[0] // kinds, near.shape[1]
    return pl.pallas_call(
        select_kernel,
        out_shape=(
            jax.ShapeDtypeStruct((n_x, count, width), bf16),
            jax.ShapeDtypeStruct((home_at.shape[0], width), bf16),
        ),
        in_specs=[vmem] * 4,
        out_specs=(vmem, vmem),
        cost_estimate=pl.CostEstimate(
            flops=4 * experts_at.shape[0] * near.size,
            bytes_accessed=4 * near.size,
            transcendentals=0,
        ),
        compiler_params=pltpu.CompilerParams(vmem_limit_bytes=8 << 20),
        name="select_rows",
    )(experts_at, home_at, near, across)


def projection_kernel(at, attn, mine_a, mine_b, theirs_a, theirs_b, out):
    half = mine_a.shape[0]
    chips = 2 * half
    first = at[1] == 0
    rows = attn[...]
    per_out = out.shape[2] // (2 * mine_a.shape[1])

    def block(use_zero, offset, kind):
        spot, n, bit = 0, 1, half // 2
        while bit:
            spot = spot + lax.rem(lax.div(offset, n), 2) * bit
            n, bit = 2 * n, bit // 2
        spot = spot * 2 + kind
        low = spot < half
        a, b = jnp.minimum(spot, half - 1), jnp.maximum(spot - half, 0)
        ours = jnp.where(low, mine_a[a], mine_b[b])
        return jnp.where(use_zero == first, ours, jnp.where(low, theirs_a[a], theirs_b[b]))

    for dest in range(out.shape[0]):
        blocks = []
        for near in range(per_out):
            ahead = lax.rem(dest * per_out + near + chips - at[0], chips)
            behind = lax.rem(chips - ahead, chips)
            zero = ahead < half
            blocks.append(
                block(zero, jnp.where(zero, ahead, behind - 1), jnp.where(zero, 0, 1))
            )
            one = (ahead >= 1) & (ahead <= half)
            blocks.append(
                block(one, jnp.where(one, ahead - 1, behind), jnp.where(one, 1, 0))
            )
        weight = jnp.concatenate(blocks, 0)
        out[dest] = lax.dot_general(
            rows, weight, (((1,), (1,)), ((), ())), preferred_element_type=f32
        ).astype(bf16)


def project_out(at, attn, halves, n_x, col_width):
    vmem = pl.BlockSpec(memory_space=pltpu.VMEM)
    size = sum(h.size for h in halves)
    return pl.pallas_call(
        projection_kernel,
        out_shape=jax.ShapeDtypeStruct((n_x, attn.shape[0], col_width), bf16),
        in_specs=[pl.BlockSpec(memory_space=pltpu.SMEM), *[vmem] * 5],
        out_specs=vmem,
        cost_estimate=pl.CostEstimate(
            flops=2 * attn.shape[0] * size, bytes_accessed=2 * size, transcendentals=0
        ),
        compiler_params=pltpu.CompilerParams(vmem_limit_bytes=8 << 20),
        name="project_out",
    )(at, attn, *halves)


def part_kernel(which, gate, up, down, give, keep, mid, sem):
    ff = down.shape[1]
    copies = []
    for k, out in enumerate((give, keep)):
        copies += [
            pltpu.make_async_copy(down.at[which[k]], mid.at[k], sem.at[3 * k]),
            pltpu.make_async_copy(gate.at[which[k]], out.at[0], sem.at[3 * k + 1]),
            pltpu.make_async_copy(up.at[which[k]], out.at[1], sem.at[3 * k + 2]),
        ]
    for copy in copies:
        copy.start()
    for k, out in enumerate((give, keep)):
        copies[3 * k].wait()
        for t in range(down.shape[2] // HD):
            out[2, t * ff : (t + 1) * ff, :] = mid[k, :, t * HD : (t + 1) * HD]
    for k in (0, 1):
        copies[3 * k + 1].wait()
        copies[3 * k + 2].wait()


def part_weights(which, gate, up, down):
    hbm = pl.BlockSpec(memory_space=pltpu.HBM)
    vmem = pl.BlockSpec(memory_space=pltpu.VMEM)
    half = jax.ShapeDtypeStruct((3, *gate.shape[1:]), bf16)
    return pl.pallas_call(
        part_kernel,
        out_shape=(half, half),
        in_specs=[pl.BlockSpec(memory_space=pltpu.SMEM), hbm, hbm, hbm],
        out_specs=(vmem, vmem),
        scratch_shapes=[
            pltpu.VMEM((2, *down.shape[1:]), bf16),
            pltpu.SemaphoreType.DMA((6,)),
        ],
        cost_estimate=pl.CostEstimate(
            flops=gate.size, bytes_accessed=12 * gate.size, transcendentals=0
        ),
        compiler_params=pltpu.CompilerParams(vmem_limit_bytes=8 << 20),
        name="part_weights",
    )(which, *in_hbm(gate, up, down))


def expert_kernel(rows, kept, got, out):
    n_x, count, col_width = rows.shape
    ff = kept.shape[2]
    total = jnp.zeros((count, 4 * ff), f32)
    for s in range(n_x):
        at = pl.ds(s * col_width, col_width)
        weight = jnp.concatenate(
            [kept[0, at, :], got[0, at, :], kept[1, at, :], got[1, at, :]], 1
        )
        total = total + jnp.dot(rows[s], weight, preferred_element_type=f32)
    gates, ups = total[:, : 2 * ff], total[:, 2 * ff :]
    act = (gates / (1.0 + jnp.exp(-gates)) * ups).astype(bf16)
    tiles = col_width // HD
    for d in range(n_x):
        halves = [
            jnp.concatenate(
                [w[2, pl.ds((d * tiles + t) * ff, ff), :] for t in range(tiles)], 1
            )
            for w in (kept, got)
        ]
        weight = jnp.concatenate(halves, 0)
        out[d] = jnp.dot(act, weight, preferred_element_type=f32).astype(bf16)


def run_expert(rows, kept, got):
    vmem = pl.BlockSpec(memory_space=pltpu.VMEM)
    ff = kept.shape[2]
    return pl.pallas_call(
        expert_kernel,
        out_shape=jax.ShapeDtypeStruct(rows.shape, bf16),
        in_specs=[vmem, vmem, vmem],
        out_specs=vmem,
        cost_estimate=pl.CostEstimate(
            flops=12 * rows.size * ff,
            bytes_accessed=4 * (rows.size + got.size),
            transcendentals=rows.shape[1] * 2 * ff,
        ),
        compiler_params=pltpu.CompilerParams(vmem_limit_bytes=12 << 20),
        name="run_expert",
    )(rows, kept, got)


def layer(
    queries,
    own_kv,
    prompt_cache,
    prompt_len,
    token_prompt,
    residual,
    out_weight,
    route_ids,
    route_weights,
    w_gate,
    w_up,
    w_down,
):
    n_e = lax.axis_size(EXPERT)
    n_x = lax.axis_size("tensor")
    chips = lax.axis_size("chip")
    pos_x = lax.axis_index("tensor")
    chip = lax.axis_index("chip")
    core = lax.axis_index("core")
    pos_e = chip * CORES + core
    tokens = queries.shape[0]
    half_cols = own_kv.shape[1] // 2
    kv_heads = half_cols // HD
    head_count = queries.shape[1] // HD
    group_size = head_count // kv_heads
    heads_here = head_count // n_x
    q_cols = heads_here * HD
    per_prompt = tokens // (n_e // 2)
    model_width = residual.shape[1]
    col_width = model_width // n_x
    picks = route_ids.shape[1]
    experts_here = w_gate.shape[0]
    experts = experts_here * n_e
    capacity = min(tokens, 3 * tokens * picks // (2 * experts))

    by_head = split_cache(prompt_cache, n_x)
    cache_all = exchange(by_head, "tensor")

    w_own = out_weight.T
    far = chips // 4
    own_far = along_chips(w_own, far)
    pair = across_chips(w_own, 1)
    pair_far = across_chips(w_own, far + 1)
    mine = jnp.stack([w_own, pair, own_far, pair_far])
    mine = jnp.concatenate([mine, along_chips(mine, far // 2)])
    mine_b = along_chips(mine, 1)
    theirs_a = other_core(mine)
    theirs_b = other_core(mine_b)

    kv_pos = (pos_x * heads_here) // group_size
    earlier = jnp.arange(tokens)[None, :] < jnp.arange(tokens)[:, None]
    chunks = (q_cols + 2 * HD + col_width) // HD
    size = 2 * chunks + picks
    at = jnp.stack([pos_x, kv_pos, kv_heads + kv_pos]).astype(i32)
    sent = build_payload(
        at,
        token_prompt.reshape(1, tokens),
        route_ids.T,
        queries,
        own_kv,
        residual,
        q_cols,
        col_width,
        n_e * size,
    )
    sent, cache_all = lax.optimization_barrier((sent, cache_all))
    got = exchange(sent.reshape(n_e, size, HD), EXPERT)
    table = got[:, 2 * chunks :, :].astype(i32)
    prompts = table[:, 0, tokens : 2 * tokens]
    routes = table[:, :, :tokens]

    owner = jnp.arange(n_e, dtype=i32)
    holds = jnp.any(prompts[None, :, :] == owner[:, None, None], -1)
    order = count_earlier(holds)
    peers = prompts[:, :, None] == prompts[:, None, :]
    rank_all = jnp.sum((peers & earlier[None]).astype(i32), 2)
    block_order = jnp.sum(
        jnp.where(prompts[:, :, None] == owner, order.T[:, None, :], 0), 2
    )
    source = jnp.where(prompts % CORES == core, 0, chips) + prompts // CORES
    source = source * tokens + block_order * per_prompt + rank_all

    at = jnp.concatenate([jnp.stack([pos_e]).astype(i32), prompt_len])
    attn, resid = attend(
        at, got.reshape(n_e * size, HD), cache_all, tokens, q_cols, col_width
    )
    at = jnp.stack([chip, core]).astype(i32)
    partial = project_out(at, attn, (mine, mine_b, theirs_a, theirs_b), n_x, col_width)
    parts = exchange(partial, "tensor")
    hidden = hidden_copies(parts, resid, chips)

    keep = pos_x % experts_here
    give = 1 - keep
    swap = [(i, i ^ 1) for i in range(n_x)]
    which = jnp.stack([give, keep]).astype(i32)
    giving, keeping = part_weights(which, w_gate, w_up, w_down)
    got_weights = lax.ppermute(giving, "tensor", swap)

    near = exchange(hidden, "chip")
    across = other_core(near)
    mine_e = pos_e * experts_here + jnp.arange(experts_here, dtype=i32)
    named = jnp.any(routes[None] == mine_e[:, None, None, None], 2)
    slot = jnp.where(named, count_earlier(named), -1)
    filled = slot[:, :, None, :] == jnp.arange(capacity, dtype=i32)[None, None, :, None]
    expert_rows = jnp.sum(jnp.where(filled, source[None, :, None, :] + 1, 0), -1) - 1
    home_rows = lax.dynamic_index_in_dim(source, pos_e, 0, keepdims=False)
    by_dest, hidden_home = select_rows(
        expert_rows.reshape(-1, 1),
        home_rows.reshape(-1, 1),
        near.reshape(chips * tokens, col_width),
        across.reshape(chips * tokens, col_width),
        n_x,
        experts_here,
    )
    rows_in = exchange(by_dest, "tensor")

    out = run_expert(rows_in, keeping, got_weights)
    parts = exchange(out, "tensor")
    parts = parts.reshape(n_x // experts_here, experts_here, n_e, capacity, col_width)
    summed = jnp.sum(parts.astype(f32), 0).astype(bf16)
    returned = exchange(jnp.transpose(summed, (1, 0, 2, 3)), EXPERT)

    hit = route_ids[:, :, None] == jnp.arange(experts, dtype=i32)
    marks = jnp.any(hit, 1)
    mark_weight = jnp.sum(jnp.where(hit, route_weights[:, :, None], 0.0), 1)
    slot = jnp.dot(
        earlier.astype(bf16), marks.astype(bf16), preferred_element_type=f32
    ).astype(i32)
    slot = jnp.where(marks, slot, -1)
    chosen = slot[:, :, None] == jnp.arange(capacity, dtype=i32)
    mix_rows = (chosen * mark_weight[:, :, None]).reshape(tokens, experts * capacity)
    expert_mix = jnp.dot(
        mix_rows,
        returned.reshape(experts * capacity, col_width).astype(f32),
        precision=lax.Precision.HIGHEST,
    )
    return (hidden_home.astype(f32) + expert_mix).astype(bf16)


def solution(mesh):
    split = Mesh(
        mesh.devices.reshape(
            mesh.shape["groups"],
            mesh.shape["expert"] // CORES,
            CORES,
            mesh.shape["tensor"],
        ),
        ("groups", *EXPERT, "tensor"),
    )
    whole = ("groups", *EXPERT)
    return jax.shard_map(
        layer,
        mesh=split,
        in_specs=(
            P(whole, None),
            P(whole, None),
            P(whole, "tensor", None),
            P(whole),
            P(whole),
            P(whole, None),
            P("tensor", EXPERT),
            P(whole, None),
            P(whole, None),
            P(EXPERT, None, "tensor"),
            P(EXPERT, None, "tensor"),
            P(EXPERT, "tensor", None),
        ),
        out_specs=P(whole, "tensor"),
        check_vma=False,
    )
```

```python
import jax
import jax.numpy as jnp
from jax import lax
from jax.experimental import pallas as pl
from jax.experimental.pallas import tpu as pltpu
from jax.sharding import Mesh
from jax.sharding import PartitionSpec as P

HD = 128
CORES = 2
EXPERT = ("chip", "core")
MASKED_SCORE = -1e30
f32, bf16, i32 = jnp.float32, jnp.bfloat16, jnp.int32


def exchange(tiles, axis):
    return lax.all_to_all(tiles, axis, split_axis=0, concat_axis=0, tiled=True)


def along_chips(x, shift):
    n = lax.axis_size("chip")
    moves = []
    for c in range(n):
        moves.append((c * CORES, (c - shift) % n * CORES))
        moves.append((c * CORES + 1, (c + shift) % n * CORES + 1))
    return lax.ppermute(x, EXPERT, moves)


def across_chips(x):
    n = lax.axis_size("chip")
    moves = []
    for c in range(n):
        moves.append((c * CORES, (c + 1) % n * CORES + 1))
        moves.append((c * CORES + 1, (c - 1) % n * CORES))
    return lax.ppermute(x, EXPERT, moves)


def other_core(x):
    return lax.ppermute(x, "core", [(0, 1), (1, 0)])


def count_earlier(marks):
    n = marks.shape[-1]
    before = (jnp.arange(n)[:, None] < jnp.arange(n)[None, :]).astype(bf16)
    return jnp.dot(marks.astype(bf16), before, preferred_element_type=f32).astype(i32)


def in_hbm(*arrays):
    return [pltpu.with_memory_space_constraint(x, pltpu.HBM) for x in arrays]


def one_hot(at, shape, dim):
    return jnp.where(lax.broadcasted_iota(i32, shape, dim) == at, 1.0, 0.0).astype(bf16)


def grouped_iota(groups, size, lanes, dim):
    at = lax.broadcasted_iota(i32, (groups, size, lanes), dim)
    return at.reshape(groups * size, lanes)


def payload_kernel(at, prompts, routes, queries, own_kv, residual, out, q, kv, resid, sem):
    tokens, q_cols = q.shape
    col_width = resid.shape[1]

    def cols(start, width):
        return pl.ds(pl.multiple_of(start, HD), width)

    copies = [
        pltpu.make_async_copy(queries.at[:, cols(at[0] * q_cols, q_cols)], q, sem.at[0]),
        pltpu.make_async_copy(own_kv.at[:, cols(at[1] * HD, HD)], kv.at[0], sem.at[1]),
        pltpu.make_async_copy(own_kv.at[:, cols(at[2] * HD, HD)], kv.at[1], sem.at[2]),
        pltpu.make_async_copy(
            residual.at[:, cols(at[0] * col_width, col_width)], resid, sem.at[3]
        ),
    ]
    for copy in copies:
        copy.start()
    count = out.shape[0]
    size = count // tokens
    chunks = (q_cols + 2 * HD + col_width) // HD
    depth = chunks * tokens + HD
    prompt = jnp.broadcast_to(prompts[...].astype(f32), (tokens, tokens))
    sub = lax.broadcasted_iota(i32, (tokens, tokens), 0)
    lane = lax.broadcasted_iota(i32, (tokens, tokens), 1)
    alike = (prompt == prompt.T) & (sub < lane)
    rank = jnp.sum(jnp.where(alike, 1.0, 0.0), 0, keepdims=True)
    both = jnp.concatenate(
        [jnp.broadcast_to(x, (8, tokens)) for x in (prompt[:1], rank)], 0
    )
    lanes = lax.broadcasted_iota(i32, (tokens, depth), 1)
    repeat = jnp.where(
        lax.rem(lanes, tokens) == lax.broadcasted_iota(i32, (tokens, depth), 0), 1.0, 0.0
    )
    spread = jnp.dot(both.astype(bf16), repeat.astype(bf16), preferred_element_type=f32)
    lanes = lax.broadcasted_iota(i32, (1, depth), 1)
    chunk = lax.div(lanes, tokens)
    place = spread[:1].astype(i32) * size + spread[8:9].astype(i32) * chunks + chunk
    place = jnp.where(chunk < chunks, place, -1)
    spare = lanes - chunks * tokens
    spare = jnp.where((spare >= 0) & (spare < size - 2 * chunks), 2 * chunks + spare, -1)
    whole = lax.broadcasted_iota(i32, (count, depth), 0) == place
    local_row = grouped_iota(tokens, size, depth, 1) == spare
    chosen = jnp.where(whole | local_row, 1.0, 0.0).astype(bf16)
    picks = routes.shape[0]
    at_lane = lax.broadcasted_iota(i32, (tokens, HD), 1)
    at_sub = lax.broadcasted_iota(i32, (tokens, HD), 0)
    first = jnp.where(at_lane == at_sub, 1.0, 0.0).astype(bf16)
    second = jnp.where(at_lane == at_sub + tokens, 1.0, 0.0).astype(bf16)
    table = jnp.dot(
        routes[...].astype(f32).astype(bf16), first, preferred_element_type=f32
    ) + jnp.dot(
        jnp.broadcast_to(prompt[:1], (picks, tokens)).astype(bf16),
        second,
        preferred_element_type=f32,
    )
    table = jnp.concatenate([table, jnp.zeros((HD - picks, HD), f32)], 0).astype(bf16)
    for copy in copies:
        copy.wait()
    rows = [q[:, c : c + HD] for c in range(0, q_cols, HD)]
    rows += [kv[0], kv[1]]
    rows += [resid[:, c : c + HD] for c in range(0, col_width, HD)]
    rows = jnp.concatenate([*rows, table], 0)
    out[...] = jnp.dot(chosen, rows, preferred_element_type=f32).astype(bf16)


def build_payload(at, prompts, routes, queries, own_kv, residual, q_cols, col_width, count):
    vmem = pl.BlockSpec(memory_space=pltpu.VMEM)
    hbm = pl.BlockSpec(memory_space=pltpu.HBM)
    tokens = queries.shape[0]
    return pl.pallas_call(
        payload_kernel,
        out_shape=jax.ShapeDtypeStruct((count, HD), bf16),
        in_specs=[pl.BlockSpec(memory_space=pltpu.SMEM), vmem, vmem, hbm, hbm, hbm],
        out_specs=vmem,
        scratch_shapes=[
            pltpu.VMEM((tokens, q_cols), bf16),
            pltpu.VMEM((2, tokens, HD), bf16),
            pltpu.VMEM((tokens, col_width), bf16),
            pltpu.SemaphoreType.DMA((4,)),
        ],
        cost_estimate=pl.CostEstimate(
            flops=2 * count * 384 * HD, bytes_accessed=4 * count * HD, transcendentals=0
        ),
        compiler_params=pltpu.CompilerParams(vmem_limit_bytes=6 << 20),
        name="build_payload",
    )(at, *in_hbm(prompts, routes, queries, own_kv, residual))


def cache_kernel(cache, out):
    copies, _, width = out.shape
    heads = cache.shape[2] // width
    for x in range(copies):
        g = x * heads // copies
        out[x, :, :HD] = cache[0, :, g * HD : (g + 1) * HD]
        out[x, :, HD:] = cache[0, :, (heads + g) * HD : (heads + g + 1) * HD]


def split_cache(cache, n_x):
    vmem = pl.BlockSpec(memory_space=pltpu.VMEM)
    return pl.pallas_call(
        cache_kernel,
        out_shape=jax.ShapeDtypeStruct((n_x, cache.shape[1], 2 * HD), bf16),
        in_specs=[vmem],
        out_specs=vmem,
        cost_estimate=pl.CostEstimate(
            flops=cache.size, bytes_accessed=6 * cache.size, transcendentals=0
        ),
        compiler_params=pltpu.CompilerParams(vmem_limit_bytes=2 << 20),
        name="split_cache",
    )(*in_hbm(cache))


def attention_kernel(at, got, cache, attn, resid):
    tokens = attn.shape[0]
    heads = attn.shape[1] // HD
    chunks = heads + 2 + resid.shape[1] // HD
    blocks = tokens
    size = got.shape[0] // blocks
    rows = got[...]
    table_row = one_hot(
        lax.broadcasted_iota(i32, (blocks, got.shape[0]), 0) * size + 2 * chunks,
        (blocks, got.shape[0]),
        1,
    )
    prompts = jnp.dot(table_row, rows, preferred_element_type=f32)
    lane = lax.broadcasted_iota(i32, prompts.shape, 1)
    prompts = jnp.where((lane >= tokens) & (lane < 2 * tokens), prompts, -1.0)
    holds = jnp.max(jnp.where(prompts == at[0].astype(f32), 1.0, 0.0), 1, keepdims=True)
    before = jnp.where(
        lax.broadcasted_iota(i32, (blocks, blocks), 1)
        < lax.broadcasted_iota(i32, (blocks, blocks), 0),
        1.0,
        0.0,
    ).astype(bf16)
    wide = jnp.broadcast_to(holds, (blocks, HD)).astype(bf16)
    order = jnp.dot(before, wide, preferred_element_type=f32)
    order = jnp.where(wide > 0, order * 2.0, -1024.0).astype(bf16)
    spread = jnp.where(
        grouped_iota(blocks, size, blocks, 0)
        == lax.broadcasted_iota(i32, (blocks * size, blocks), 1),
        1.0,
        0.0,
    ).astype(bf16)
    order = jnp.dot(spread, order, preferred_element_type=f32)[:, :1].astype(i32)
    place = grouped_iota(blocks, size, 1, 1)
    second = jnp.where(place >= chunks, 1, 0)
    target = (place - second * chunks) * tokens + order + second
    target = jnp.where(place < 2 * chunks, target, -1)
    chosen = one_hot(target, (got.shape[0], chunks * tokens), 1)
    mine = lax.dot_general(
        chosen, rows, (((0,), (0,)), ((), ())), preferred_element_type=f32
    )

    def chunk(c):
        return mine[c * tokens : (c + 1) * tokens, :]

    k_own, v_own = chunk(heads), chunk(heads + 1)
    positions = cache.shape[0] * cache.shape[1]
    both = cache[...].reshape(positions, cache.shape[2])
    keys, values = both[:, :HD], both[:, HD:]
    inside = lax.broadcasted_iota(i32, (tokens, positions), 1) < at[1]
    scale = HD ** (-0.5)
    for h in range(heads):
        q = chunk(h)
        scores = (
            lax.dot_general(
                q.astype(bf16), keys, (((1,), (1,)), ((), ())), preferred_element_type=f32
            )
            * scale
        )
        scores = jnp.where(inside, scores, MASKED_SCORE)
        own = jnp.sum(q * k_own, 1, keepdims=True) * scale
        top = jnp.maximum(jnp.max(scores, 1, keepdims=True), own)
        weights = jnp.where(inside, jnp.exp(scores - top), 0.0)
        own_weight = jnp.exp(own - top)
        total = jnp.sum(weights, 1, keepdims=True) + own_weight
        mix = jnp.dot(weights.astype(bf16), values, preferred_element_type=f32)
        mix = (mix + own_weight * v_own) / total
        attn[:, h * HD : (h + 1) * HD] = mix.astype(bf16)
    for c in range(resid.shape[1] // HD):
        resid[:, c * HD : (c + 1) * HD] = chunk(heads + 2 + c).astype(bf16)


def attend(at, got, cache, tokens, q_cols, col_width):
    vmem = pl.BlockSpec(memory_space=pltpu.VMEM)
    return pl.pallas_call(
        attention_kernel,
        out_shape=(
            jax.ShapeDtypeStruct((tokens, q_cols), bf16),
            jax.ShapeDtypeStruct((tokens, col_width), bf16),
        ),
        in_specs=[pl.BlockSpec(memory_space=pltpu.SMEM), vmem, vmem],
        out_specs=(vmem, vmem),
        cost_estimate=pl.CostEstimate(
            flops=4 * got.size * 256, bytes_accessed=2 * got.size, transcendentals=0
        ),
        compiler_params=pltpu.CompilerParams(vmem_limit_bytes=8 << 20),
        name="attend",
    )(at, got, cache)


def hidden_kernel(parts, resid, out):
    hidden = resid[...].astype(f32)
    for s in range(parts.shape[0]):
        hidden = hidden + parts[s].astype(f32)
    hidden = hidden.astype(bf16)
    for d in range(out.shape[0]):
        out[d] = hidden


def hidden_copies(parts, resid, copies):
    vmem = pl.BlockSpec(memory_space=pltpu.VMEM)
    return pl.pallas_call(
        hidden_kernel,
        out_shape=jax.ShapeDtypeStruct((copies, *resid.shape), bf16),
        in_specs=[vmem, vmem],
        out_specs=vmem,
        cost_estimate=pl.CostEstimate(
            flops=parts.size, bytes_accessed=4 * parts.size, transcendentals=0
        ),
        compiler_params=pltpu.CompilerParams(vmem_limit_bytes=4 << 20),
        name="hidden_copies",
    )(parts, resid)


def select_kernel(experts_at, home_at, near, across, by_dest, home):
    half = near.shape[0]

    def picked(at):
        shape = (at.shape[0], half)
        return (
            jnp.dot(one_hot(at, shape, 1), near[...], preferred_element_type=f32)
            + jnp.dot(one_hot(at - half, shape, 1), across[...], preferred_element_type=f32)
        ).astype(bf16)

    home[...] = picked(home_at[...])
    count = by_dest.shape[1]
    kinds = experts_at.shape[0] // count
    for kind in range(kinds):
        rows = picked(experts_at[kind * count : (kind + 1) * count, :])
        for d in range(kind, by_dest.shape[0], kinds):
            by_dest[d] = rows


def select_rows(experts_at, home_at, near, across, n_x, kinds):
    vmem = pl.BlockSpec(memory_space=pltpu.VMEM)
    count, width = experts_at.shape[0] // kinds, near.shape[1]
    return pl.pallas_call(
        select_kernel,
        out_shape=(
            jax.ShapeDtypeStruct((n_x, count, width), bf16),
            jax.ShapeDtypeStruct((home_at.shape[0], width), bf16),
        ),
        in_specs=[vmem] * 4,
        out_specs=(vmem, vmem),
        cost_estimate=pl.CostEstimate(
            flops=4 * experts_at.shape[0] * near.size,
            bytes_accessed=4 * near.size,
            transcendentals=0,
        ),
        compiler_params=pltpu.CompilerParams(vmem_limit_bytes=8 << 20),
        name="select_rows",
    )(experts_at, home_at, near, across)


def projection_kernel(at, attn, mine_a, mine_b, theirs_a, theirs_b, out):
    half = mine_a.shape[0]
    chips = 2 * half
    first = at[1] == 0
    rows = attn[...]
    per_out = out.shape[2] // (2 * mine_a.shape[1])

    def block(use_zero, offset, kind):
        spot, n, bit = 0, 1, half // 2
        while bit:
            spot = spot + lax.rem(lax.div(offset, n), 2) * bit
            n, bit = 2 * n, bit // 2
        spot = spot * 2 + kind
        low = spot < half
        a, b = jnp.minimum(spot, half - 1), jnp.maximum(spot - half, 0)
        ours = jnp.where(low, mine_a[a], mine_b[b])
        return jnp.where(use_zero == first, ours, jnp.where(low, theirs_a[a], theirs_b[b]))

    for dest in range(out.shape[0]):
        blocks = []
        for near in range(per_out):
            ahead = lax.rem(dest * per_out + near + chips - at[0], chips)
            behind = lax.rem(chips - ahead, chips)
            zero = ahead < half
            blocks.append(
                block(zero, jnp.where(zero, ahead, behind - 1), jnp.where(zero, 0, 1))
            )
            one = (ahead >= 1) & (ahead <= half)
            blocks.append(
                block(one, jnp.where(one, ahead - 1, behind), jnp.where(one, 1, 0))
            )
        weight = jnp.concatenate(blocks, 0)
        out[dest] = lax.dot_general(
            rows, weight, (((1,), (1,)), ((), ())), preferred_element_type=f32
        ).astype(bf16)


def project_out(at, attn, halves, n_x, col_width):
    vmem = pl.BlockSpec(memory_space=pltpu.VMEM)
    size = sum(h.size for h in halves)
    return pl.pallas_call(
        projection_kernel,
        out_shape=jax.ShapeDtypeStruct((n_x, attn.shape[0], col_width), bf16),
        in_specs=[pl.BlockSpec(memory_space=pltpu.SMEM), *[vmem] * 5],
        out_specs=vmem,
        cost_estimate=pl.CostEstimate(
            flops=2 * attn.shape[0] * size, bytes_accessed=2 * size, transcendentals=0
        ),
        compiler_params=pltpu.CompilerParams(vmem_limit_bytes=8 << 20),
        name="project_out",
    )(at, attn, *halves)


def part_kernel(which, gate, up, down, give, keep, mid, sem):
    ff = down.shape[1]
    copies = []
    for k, out in enumerate((give, keep)):
        copies += [
            pltpu.make_async_copy(down.at[which[k]], mid.at[k], sem.at[3 * k]),
            pltpu.make_async_copy(gate.at[which[k]], out.at[0], sem.at[3 * k + 1]),
            pltpu.make_async_copy(up.at[which[k]], out.at[1], sem.at[3 * k + 2]),
        ]
    for copy in copies:
        copy.start()
    for k, out in enumerate((give, keep)):
        copies[3 * k].wait()
        for t in range(down.shape[2] // HD):
            out[2, t * ff : (t + 1) * ff, :] = mid[k, :, t * HD : (t + 1) * HD]
    for k in (0, 1):
        copies[3 * k + 1].wait()
        copies[3 * k + 2].wait()


def part_weights(which, gate, up, down):
    hbm = pl.BlockSpec(memory_space=pltpu.HBM)
    vmem = pl.BlockSpec(memory_space=pltpu.VMEM)
    half = jax.ShapeDtypeStruct((3, *gate.shape[1:]), bf16)
    return pl.pallas_call(
        part_kernel,
        out_shape=(half, half),
        in_specs=[pl.BlockSpec(memory_space=pltpu.SMEM), hbm, hbm, hbm],
        out_specs=(vmem, vmem),
        scratch_shapes=[
            pltpu.VMEM((2, *down.shape[1:]), bf16),
            pltpu.SemaphoreType.DMA((6,)),
        ],
        cost_estimate=pl.CostEstimate(
            flops=gate.size, bytes_accessed=12 * gate.size, transcendentals=0
        ),
        compiler_params=pltpu.CompilerParams(vmem_limit_bytes=8 << 20),
        name="part_weights",
    )(which, *in_hbm(gate, up, down))


def expert_kernel(rows, kept, got, out):
    n_x, count, col_width = rows.shape
    ff = kept.shape[2]
    total = jnp.zeros((count, 4 * ff), f32)
    for s in range(n_x):
        at = pl.ds(s * col_width, col_width)
        weight = jnp.concatenate(
            [kept[0, at, :], got[0, at, :], kept[1, at, :], got[1, at, :]], 1
        )
        total = total + jnp.dot(rows[s], weight, preferred_element_type=f32)
    gates, ups = total[:, : 2 * ff], total[:, 2 * ff :]
    act = (gates / (1.0 + jnp.exp(-gates)) * ups).astype(bf16)
    tiles = col_width // HD
    for d in range(n_x):
        halves = [
            jnp.concatenate(
                [w[2, pl.ds((d * tiles + t) * ff, ff), :] for t in range(tiles)], 1
            )
            for w in (kept, got)
        ]
        weight = jnp.concatenate(halves, 0)
        out[d] = jnp.dot(act, weight, preferred_element_type=f32).astype(bf16)


def run_expert(rows, kept, got):
    vmem = pl.BlockSpec(memory_space=pltpu.VMEM)
    ff = kept.shape[2]
    return pl.pallas_call(
        expert_kernel,
        out_shape=jax.ShapeDtypeStruct(rows.shape, bf16),
        in_specs=[vmem, vmem, vmem],
        out_specs=vmem,
        cost_estimate=pl.CostEstimate(
            flops=12 * rows.size * ff,
            bytes_accessed=4 * (rows.size + got.size),
            transcendentals=rows.shape[1] * 2 * ff,
        ),
        compiler_params=pltpu.CompilerParams(vmem_limit_bytes=12 << 20),
        name="run_expert",
    )(rows, kept, got)


def layer(
    queries,
    own_kv,
    prompt_cache,
    prompt_len,
    token_prompt,
    residual,
    out_weight,
    route_ids,
    route_weights,
    w_gate,
    w_up,
    w_down,
):
    n_e = lax.axis_size(EXPERT)
    n_x = lax.axis_size("tensor")
    chips = lax.axis_size("chip")
    pos_x = lax.axis_index("tensor")
    chip = lax.axis_index("chip")
    core = lax.axis_index("core")
    pos_e = chip * CORES + core
    tokens = queries.shape[0]
    half_cols = own_kv.shape[1] // 2
    kv_heads = half_cols // HD
    head_count = queries.shape[1] // HD
    group_size = head_count // kv_heads
    heads_here = head_count // n_x
    q_cols = heads_here * HD
    per_prompt = tokens // (n_e // 2)
    model_width = residual.shape[1]
    col_width = model_width // n_x
    picks = route_ids.shape[1]
    experts_here = w_gate.shape[0]
    experts = experts_here * n_e
    capacity = min(tokens, 3 * tokens * picks // (2 * experts))

    by_head = split_cache(prompt_cache, n_x)
    cache_all = exchange(by_head, "tensor")

    w_own = out_weight.T
    mine = jnp.stack([w_own, across_chips(w_own)])
    shift = chips // 4
    while shift > 1:
        mine = jnp.concatenate([mine, along_chips(mine, shift)])
        shift //= 2
    mine_b = along_chips(mine, 1)
    theirs_a = other_core(mine)
    theirs_b = other_core(mine_b)

    kv_pos = (pos_x * heads_here) // group_size
    earlier = jnp.arange(tokens)[None, :] < jnp.arange(tokens)[:, None]
    chunks = (q_cols + 2 * HD + col_width) // HD
    size = 2 * chunks + picks
    at = jnp.stack([pos_x, kv_pos, kv_heads + kv_pos]).astype(i32)
    sent = build_payload(
        at,
        token_prompt.reshape(1, tokens),
        route_ids.T,
        queries,
        own_kv,
        residual,
        q_cols,
        col_width,
        n_e * size,
    )
    sent, cache_all = lax.optimization_barrier((sent, cache_all))
    got = exchange(sent.reshape(n_e, size, HD), EXPERT)
    table = got[:, 2 * chunks :, :].astype(i32)
    prompts = table[:, 0, tokens : 2 * tokens]
    routes = table[:, :, :tokens]

    owner = jnp.arange(n_e, dtype=i32)
    holds = jnp.any(prompts[None, :, :] == owner[:, None, None], -1)
    order = count_earlier(holds)
    peers = prompts[:, :, None] == prompts[:, None, :]
    rank_all = jnp.sum((peers & earlier[None]).astype(i32), 2)
    block_order = jnp.sum(
        jnp.where(prompts[:, :, None] == owner, order.T[:, None, :], 0), 2
    )
    source = jnp.where(prompts % CORES == core, 0, chips) + prompts // CORES
    source = source * tokens + block_order * per_prompt + rank_all

    at = jnp.concatenate([jnp.stack([pos_e]).astype(i32), prompt_len])
    attn, resid = attend(
        at, got.reshape(n_e * size, HD), cache_all, tokens, q_cols, col_width
    )
    at = jnp.stack([chip, core]).astype(i32)
    partial = project_out(at, attn, (mine, mine_b, theirs_a, theirs_b), n_x, col_width)
    parts = exchange(partial, "tensor")
    hidden = hidden_copies(parts, resid, chips)

    keep = pos_x % experts_here
    give = 1 - keep
    swap = []
    for i in range(n_x):
        swap.append((i, i ^ 1))
        swap.append((n_x + i, n_x + (i + (1 if i % 2 else -1)) % n_x))
    which = jnp.stack([give, keep]).astype(i32)
    giving, keeping = part_weights(which, w_gate, w_up, w_down)
    got_weights = lax.ppermute(giving, ("core", "tensor"), swap)

    near = exchange(hidden, "chip")
    across = other_core(near)
    mine_e = pos_e * experts_here + jnp.arange(experts_here, dtype=i32)
    named = jnp.any(routes[None] == mine_e[:, None, None, None], 2)
    slot = jnp.where(named, count_earlier(named), -1)
    filled = slot[:, :, None, :] == jnp.arange(capacity, dtype=i32)[None, None, :, None]
    expert_rows = jnp.sum(jnp.where(filled, source[None, :, None, :] + 1, 0), -1) - 1
    home_rows = lax.dynamic_index_in_dim(source, pos_e, 0, keepdims=False)
    by_dest, hidden_home = select_rows(
        expert_rows.reshape(-1, 1),
        home_rows.reshape(-1, 1),
        near.reshape(chips * tokens, col_width),
        across.reshape(chips * tokens, col_width),
        n_x,
        experts_here,
    )
    rows_in = exchange(by_dest, "tensor")

    out = run_expert(rows_in, keeping, got_weights)
    parts = exchange(out, "tensor")
    parts = parts.reshape(n_x // experts_here, experts_here, n_e, capacity, col_width)
    summed = jnp.sum(parts.astype(f32), 0).astype(bf16)
    returned = exchange(jnp.transpose(summed, (1, 0, 2, 3)), EXPERT)

    hit = route_ids[:, :, None] == jnp.arange(experts, dtype=i32)
    marks = jnp.any(hit, 1)
    mark_weight = jnp.sum(jnp.where(hit, route_weights[:, :, None], 0.0), 1)
    slot = jnp.dot(
        earlier.astype(bf16), marks.astype(bf16), preferred_element_type=f32
    ).astype(i32)
    slot = jnp.where(marks, slot, -1)
    chosen = slot[:, :, None] == jnp.arange(capacity, dtype=i32)
    mix_rows = (chosen * mark_weight[:, :, None]).reshape(tokens, experts * capacity)
    expert_mix = jnp.dot(
        mix_rows,
        returned.reshape(experts * capacity, col_width).astype(f32),
        precision=lax.Precision.HIGHEST,
    )
    return (hidden_home.astype(f32) + expert_mix).astype(bf16)


def solution(mesh):
    split = Mesh(
        mesh.devices.reshape(
            mesh.shape["groups"],
            mesh.shape["expert"] // CORES,
            CORES,
            mesh.shape["tensor"],
        ),
        ("groups", *EXPERT, "tensor"),
    )
    whole = ("groups", *EXPERT)
    return jax.shard_map(
        layer,
        mesh=split,
        in_specs=(
            P(whole, None),
            P(whole, None),
            P(whole, "tensor", None),
            P(whole),
            P(whole),
            P(whole, None),
            P("tensor", EXPERT),
            P(whole, None),
            P(whole, None),
            P(EXPERT, None, "tensor"),
            P(EXPERT, None, "tensor"),
            P(EXPERT, "tensor", None),
        ),
        out_specs=P(whole, "tensor"),
        check_vma=False,
    )
```

```python
import jax
import jax.numpy as jnp
from jax import lax
from jax.experimental import pallas as pl
from jax.experimental.pallas import tpu as pltpu
from jax.sharding import Mesh
from jax.sharding import PartitionSpec as P

HD = 128
CORES = 2
EXPERT = ("chip", "core")
MASKED_SCORE = -1e30
f32, bf16, i32 = jnp.float32, jnp.bfloat16, jnp.int32


def exchange(tiles, axis):
    return lax.all_to_all(tiles, axis, split_axis=0, concat_axis=0, tiled=True)


def along_chips(x, shift):
    n = lax.axis_size("chip")
    moves = []
    for c in range(n):
        moves.append((c * CORES, (c - shift) % n * CORES))
        moves.append((c * CORES + 1, (c + shift) % n * CORES + 1))
    return lax.ppermute(x, EXPERT, moves)


def other_core(x):
    return lax.ppermute(x, "core", [(0, 1), (1, 0)])


def count_earlier(marks):
    n = marks.shape[-1]
    before = (jnp.arange(n)[:, None] < jnp.arange(n)[None, :]).astype(bf16)
    return jnp.dot(marks.astype(bf16), before, preferred_element_type=f32).astype(i32)


def in_hbm(*arrays):
    return [pltpu.with_memory_space_constraint(x, pltpu.HBM) for x in arrays]


def one_hot(at, shape, dim):
    return jnp.where(lax.broadcasted_iota(i32, shape, dim) == at, 1.0, 0.0).astype(bf16)


def grouped_iota(groups, size, lanes, dim):
    at = lax.broadcasted_iota(i32, (groups, size, lanes), dim)
    return at.reshape(groups * size, lanes)


def payload_kernel(at, prompts, routes, queries, own_kv, residual, out, q, kv, resid, sem):
    tokens, q_cols = q.shape
    col_width = resid.shape[1]

    def cols(start, width):
        return pl.ds(pl.multiple_of(start, HD), width)

    copies = [
        pltpu.make_async_copy(queries.at[:, cols(at[0] * q_cols, q_cols)], q, sem.at[0]),
        pltpu.make_async_copy(own_kv.at[:, cols(at[1] * HD, HD)], kv.at[0], sem.at[1]),
        pltpu.make_async_copy(own_kv.at[:, cols(at[2] * HD, HD)], kv.at[1], sem.at[2]),
        pltpu.make_async_copy(
            residual.at[:, cols(at[0] * col_width, col_width)], resid, sem.at[3]
        ),
    ]
    for copy in copies:
        copy.start()
    count = out.shape[0]
    size = count // tokens
    chunks = (q_cols + 2 * HD + col_width) // HD
    depth = chunks * tokens + HD
    prompt = jnp.broadcast_to(prompts[...].astype(f32), (tokens, tokens))
    sub = lax.broadcasted_iota(i32, (tokens, tokens), 0)
    lane = lax.broadcasted_iota(i32, (tokens, tokens), 1)
    alike = (prompt == prompt.T) & (sub < lane)
    rank = jnp.sum(jnp.where(alike, 1.0, 0.0), 0, keepdims=True)
    both = jnp.concatenate(
        [jnp.broadcast_to(x, (8, tokens)) for x in (prompt[:1], rank)], 0
    )
    lanes = lax.broadcasted_iota(i32, (tokens, depth), 1)
    repeat = jnp.where(
        lax.rem(lanes, tokens) == lax.broadcasted_iota(i32, (tokens, depth), 0), 1.0, 0.0
    )
    spread = jnp.dot(both.astype(bf16), repeat.astype(bf16), preferred_element_type=f32)
    lanes = lax.broadcasted_iota(i32, (1, depth), 1)
    chunk = lax.div(lanes, tokens)
    place = spread[:1].astype(i32) * size + spread[8:9].astype(i32) * chunks + chunk
    place = jnp.where(chunk < chunks, place, -1)
    spare = lanes - chunks * tokens
    spare = jnp.where((spare >= 0) & (spare < size - 2 * chunks), 2 * chunks + spare, -1)
    whole = lax.broadcasted_iota(i32, (count, depth), 0) == place
    local_row = grouped_iota(tokens, size, depth, 1) == spare
    chosen = jnp.where(whole | local_row, 1.0, 0.0).astype(bf16)
    picks = routes.shape[0]
    at_lane = lax.broadcasted_iota(i32, (tokens, HD), 1)
    at_sub = lax.broadcasted_iota(i32, (tokens, HD), 0)
    first = jnp.where(at_lane == at_sub, 1.0, 0.0).astype(bf16)
    second = jnp.where(at_lane == at_sub + tokens, 1.0, 0.0).astype(bf16)
    table = jnp.dot(
        routes[...].astype(f32).astype(bf16), first, preferred_element_type=f32
    ) + jnp.dot(
        jnp.broadcast_to(prompt[:1], (picks, tokens)).astype(bf16),
        second,
        preferred_element_type=f32,
    )
    table = jnp.concatenate([table, jnp.zeros((HD - picks, HD), f32)], 0).astype(bf16)
    for copy in copies:
        copy.wait()
    rows = [q[:, c : c + HD] for c in range(0, q_cols, HD)]
    rows += [kv[0], kv[1]]
    rows += [resid[:, c : c + HD] for c in range(0, col_width, HD)]
    rows = jnp.concatenate([*rows, table], 0)
    out[...] = jnp.dot(chosen, rows, preferred_element_type=f32).astype(bf16)


def build_payload(at, prompts, routes, queries, own_kv, residual, q_cols, col_width, count):
    vmem = pl.BlockSpec(memory_space=pltpu.VMEM)
    hbm = pl.BlockSpec(memory_space=pltpu.HBM)
    tokens = queries.shape[0]
    return pl.pallas_call(
        payload_kernel,
        out_shape=jax.ShapeDtypeStruct((count, HD), bf16),
        in_specs=[pl.BlockSpec(memory_space=pltpu.SMEM), vmem, vmem, hbm, hbm, hbm],
        out_specs=vmem,
        scratch_shapes=[
            pltpu.VMEM((tokens, q_cols), bf16),
            pltpu.VMEM((2, tokens, HD), bf16),
            pltpu.VMEM((tokens, col_width), bf16),
            pltpu.SemaphoreType.DMA((4,)),
        ],
        cost_estimate=pl.CostEstimate(
            flops=2 * count * 384 * HD, bytes_accessed=4 * count * HD, transcendentals=0
        ),
        compiler_params=pltpu.CompilerParams(vmem_limit_bytes=6 << 20),
        name="build_payload",
    )(at, *in_hbm(prompts, routes, queries, own_kv, residual))


def cache_kernel(cache, out):
    copies, _, width = out.shape
    heads = cache.shape[2] // width
    for x in range(copies):
        g = x * heads // copies
        out[x, :, :HD] = cache[0, :, g * HD : (g + 1) * HD]
        out[x, :, HD:] = cache[0, :, (heads + g) * HD : (heads + g + 1) * HD]


def split_cache(cache, n_x):
    vmem = pl.BlockSpec(memory_space=pltpu.VMEM)
    return pl.pallas_call(
        cache_kernel,
        out_shape=jax.ShapeDtypeStruct((n_x, cache.shape[1], 2 * HD), bf16),
        in_specs=[vmem],
        out_specs=vmem,
        cost_estimate=pl.CostEstimate(
            flops=cache.size, bytes_accessed=6 * cache.size, transcendentals=0
        ),
        compiler_params=pltpu.CompilerParams(vmem_limit_bytes=2 << 20),
        name="split_cache",
    )(*in_hbm(cache))


def attention_kernel(at, got, cache, send, resid):
    tokens, width = resid.shape
    heads = (send.shape[1] - width) // HD
    chunks = heads + 2 + 2 * width // HD
    blocks = tokens
    size = got.shape[0] // blocks
    rows = got[...]
    table_row = one_hot(
        lax.broadcasted_iota(i32, (blocks, got.shape[0]), 0) * size + 2 * chunks,
        (blocks, got.shape[0]),
        1,
    )
    prompts = jnp.dot(table_row, rows, preferred_element_type=f32)
    lane = lax.broadcasted_iota(i32, prompts.shape, 1)
    prompts = jnp.where((lane >= tokens) & (lane < 2 * tokens), prompts, -1.0)
    holds = jnp.max(jnp.where(prompts == at[0].astype(f32), 1.0, 0.0), 1, keepdims=True)
    before = jnp.where(
        lax.broadcasted_iota(i32, (blocks, blocks), 1)
        < lax.broadcasted_iota(i32, (blocks, blocks), 0),
        1.0,
        0.0,
    ).astype(bf16)
    wide = jnp.broadcast_to(holds, (blocks, HD)).astype(bf16)
    order = jnp.dot(before, wide, preferred_element_type=f32)
    order = jnp.where(wide > 0, order * 2.0, -1024.0).astype(bf16)
    spread = jnp.where(
        grouped_iota(blocks, size, blocks, 0)
        == lax.broadcasted_iota(i32, (blocks * size, blocks), 1),
        1.0,
        0.0,
    ).astype(bf16)
    order = jnp.dot(spread, order, preferred_element_type=f32)[:, :1].astype(i32)
    place = grouped_iota(blocks, size, 1, 1)
    second = jnp.where(place >= chunks, 1, 0)
    target = (place - second * chunks) * tokens + order + second
    target = jnp.where(place < 2 * chunks, target, -1)
    chosen = one_hot(target, (got.shape[0], chunks * tokens), 1)
    mine = lax.dot_general(
        chosen, rows, (((0,), (0,)), ((), ())), preferred_element_type=f32
    )

    def chunk(c):
        return mine[c * tokens : (c + 1) * tokens, :]

    k_own, v_own = chunk(heads), chunk(heads + 1)
    positions = cache.shape[0] * cache.shape[1]
    both = cache[...].reshape(positions, cache.shape[2])
    keys, values = both[:, :HD], both[:, HD:]
    inside = lax.broadcasted_iota(i32, (tokens, positions), 1) < at[1]
    scale = HD ** (-0.5)
    for h in range(heads):
        q = chunk(h)
        scores = (
            lax.dot_general(
                q.astype(bf16), keys, (((1,), (1,)), ((), ())), preferred_element_type=f32
            )
            * scale
        )
        scores = jnp.where(inside, scores, MASKED_SCORE)
        own = jnp.sum(q * k_own, 1, keepdims=True) * scale
        top = jnp.maximum(jnp.max(scores, 1, keepdims=True), own)
        weights = jnp.where(inside, jnp.exp(scores - top), 0.0)
        own_weight = jnp.exp(own - top)
        total = jnp.sum(weights, 1, keepdims=True) + own_weight
        mix = jnp.dot(weights.astype(bf16), values, preferred_element_type=f32)
        mix = (mix + own_weight * v_own) / total
        send[:, h * HD : (h + 1) * HD] = mix.astype(bf16)
    left, right = chunk(heads + 2), chunk(heads + 3)
    block = width // 2
    even = jnp.concatenate([left[:, :block], right[:, :block]], 1)
    odd = jnp.concatenate([left[:, block:], right[:, block:]], 1)
    first = at[2] == 0
    resid[...] = jnp.where(first, even, odd).astype(bf16)
    send[:, heads * HD :] = jnp.where(first, odd, even).astype(bf16)


def attend(at, got, cache, tokens, q_cols, col_width):
    vmem = pl.BlockSpec(memory_space=pltpu.VMEM)
    return pl.pallas_call(
        attention_kernel,
        out_shape=(
            jax.ShapeDtypeStruct((tokens, q_cols + col_width // 2), bf16),
            jax.ShapeDtypeStruct((tokens, col_width // 2), bf16),
        ),
        in_specs=[pl.BlockSpec(memory_space=pltpu.SMEM), vmem, vmem],
        out_specs=(vmem, vmem),
        cost_estimate=pl.CostEstimate(
            flops=4 * got.size * 256, bytes_accessed=2 * got.size, transcendentals=0
        ),
        compiler_params=pltpu.CompilerParams(vmem_limit_bytes=8 << 20),
        name="attend",
    )(at, got, cache)


def hidden_kernel(at, parts, resid, got, out):
    width = resid.shape[1]
    own, other = resid[...], got[:, got.shape[1] - width :]
    first = at[1] == 0
    hidden = jnp.concatenate(
        [jnp.where(first, own, other), jnp.where(first, other, own)], 0
    ).astype(f32)
    for s in range(parts.shape[0]):
        hidden = hidden + parts[s].astype(f32)
    hidden = hidden.astype(bf16)
    for d in range(out.shape[0]):
        out[d] = hidden


def hidden_copies(at, parts, resid, got, copies):
    vmem = pl.BlockSpec(memory_space=pltpu.VMEM)
    return pl.pallas_call(
        hidden_kernel,
        out_shape=jax.ShapeDtypeStruct((copies, *parts.shape[1:]), bf16),
        in_specs=[pl.BlockSpec(memory_space=pltpu.SMEM), vmem, vmem, vmem],
        out_specs=vmem,
        cost_estimate=pl.CostEstimate(
            flops=parts.size, bytes_accessed=4 * parts.size, transcendentals=0
        ),
        compiler_params=pltpu.CompilerParams(vmem_limit_bytes=4 << 20),
        name="hidden_copies",
    )(at, parts, resid, got)


def select_kernel(at, experts_at, home_at, near, across, by_dest, home):
    total, width = near.shape
    both = jnp.concatenate([near[...], across[...]], 1)
    first = at[1] == 0
    block = width // 2

    def picked(rows_at):
        rows = jnp.dot(
            one_hot(rows_at, (rows_at.shape[0], total), 1),
            both,
            preferred_element_type=f32,
        )
        ours, theirs = rows[:, :width], rows[:, width:]
        even, odd = jnp.where(first, ours, theirs), jnp.where(first, theirs, ours)
        return jnp.concatenate(
            [even[:, :block], odd[:, :block], even[:, block:], odd[:, block:]], 1
        ).astype(bf16)

    home[...] = picked(home_at[...])
    count = by_dest.shape[1]
    kinds = experts_at.shape[0] // count
    for kind in range(kinds):
        rows = picked(experts_at[kind * count : (kind + 1) * count, :])
        for d in range(kind, by_dest.shape[0], kinds):
            by_dest[d] = rows


def select_rows(at, experts_at, home_at, near, across, n_x, kinds):
    vmem = pl.BlockSpec(memory_space=pltpu.VMEM)
    count, width = experts_at.shape[0] // kinds, 2 * near.shape[1]
    return pl.pallas_call(
        select_kernel,
        out_shape=(
            jax.ShapeDtypeStruct((n_x, count, width), bf16),
            jax.ShapeDtypeStruct((home_at.shape[0], width), bf16),
        ),
        in_specs=[pl.BlockSpec(memory_space=pltpu.SMEM), *[vmem] * 4],
        out_specs=(vmem, vmem),
        cost_estimate=pl.CostEstimate(
            flops=4 * experts_at.shape[0] * near.size,
            bytes_accessed=4 * near.size,
            transcendentals=0,
        ),
        compiler_params=pltpu.CompilerParams(vmem_limit_bytes=8 << 20),
        name="select_rows",
    )(at, experts_at, home_at, near, across)


def projection_kernel(at, own, other, mine_a, mine_b, out):
    half = mine_a.shape[0]
    chips = 2 * half
    first = at[1] == 0
    width = mine_a.shape[2]
    a, b = own[:, :width], other[:, :width]
    rows = jnp.concatenate([jnp.where(first, a, b), jnp.where(first, b, a)], 0)
    per_out = out.shape[2] // mine_a.shape[1]
    for dest in range(out.shape[0]):
        blocks = []
        for near in range(per_out):
            ahead = lax.rem(dest * per_out + near + chips - at[0], chips)
            offset = jnp.where(first, ahead, lax.rem(chips - ahead, chips))
            spot, n, bit = 0, 1, half
            while bit:
                spot = spot + lax.rem(lax.div(offset, n), 2) * bit
                n, bit = 2 * n, bit // 2
            early = mine_a[jnp.minimum(spot, half - 1)]
            late = mine_b[jnp.maximum(spot - half, 0)]
            blocks.append(jnp.where(spot < half, early, late))
        weight = jnp.concatenate(blocks, 0)
        out[dest] = lax.dot_general(
            rows, weight, (((1,), (1,)), ((), ())), preferred_element_type=f32
        ).astype(bf16)


def project_out(at, own, other, mine_a, mine_b, n_x, width):
    vmem = pl.BlockSpec(memory_space=pltpu.VMEM)
    size = mine_a.size + mine_b.size
    return pl.pallas_call(
        projection_kernel,
        out_shape=jax.ShapeDtypeStruct((n_x, 2 * own.shape[0], width), bf16),
        in_specs=[pl.BlockSpec(memory_space=pltpu.SMEM), *[vmem] * 4],
        out_specs=vmem,
        cost_estimate=pl.CostEstimate(
            flops=4 * own.shape[0] * size, bytes_accessed=2 * size, transcendentals=0
        ),
        compiler_params=pltpu.CompilerParams(vmem_limit_bytes=8 << 20),
        name="project_out",
    )(at, own, other, mine_a, mine_b)


def part_kernel(which, gate, up, down, give, keep, mid, sem):
    ff = down.shape[1]
    copies = []
    for k, out in enumerate((give, keep)):
        copies += [
            pltpu.make_async_copy(down.at[which[k]], mid.at[k], sem.at[3 * k]),
            pltpu.make_async_copy(gate.at[which[k]], out.at[0], sem.at[3 * k + 1]),
            pltpu.make_async_copy(up.at[which[k]], out.at[1], sem.at[3 * k + 2]),
        ]
    for copy in copies:
        copy.start()
    for k, out in enumerate((give, keep)):
        copies[3 * k].wait()
        for t in range(down.shape[2] // HD):
            out[2, t * ff : (t + 1) * ff, :] = mid[k, :, t * HD : (t + 1) * HD]
    for k in (0, 1):
        copies[3 * k + 1].wait()
        copies[3 * k + 2].wait()


def part_weights(which, gate, up, down):
    hbm = pl.BlockSpec(memory_space=pltpu.HBM)
    vmem = pl.BlockSpec(memory_space=pltpu.VMEM)
    half = jax.ShapeDtypeStruct((3, *gate.shape[1:]), bf16)
    return pl.pallas_call(
        part_kernel,
        out_shape=(half, half),
        in_specs=[pl.BlockSpec(memory_space=pltpu.SMEM), hbm, hbm, hbm],
        out_specs=(vmem, vmem),
        scratch_shapes=[
            pltpu.VMEM((2, *down.shape[1:]), bf16),
            pltpu.SemaphoreType.DMA((6,)),
        ],
        cost_estimate=pl.CostEstimate(
            flops=gate.size, bytes_accessed=12 * gate.size, transcendentals=0
        ),
        compiler_params=pltpu.CompilerParams(vmem_limit_bytes=8 << 20),
        name="part_weights",
    )(which, *in_hbm(gate, up, down))


def expert_kernel(rows, kept, got, out):
    n_x, count, col_width = rows.shape
    ff = kept.shape[2]
    total = jnp.zeros((count, 4 * ff), f32)
    for s in range(n_x):
        at = pl.ds(s * col_width, col_width)
        weight = jnp.concatenate(
            [kept[0, at, :], got[0, at, :], kept[1, at, :], got[1, at, :]], 1
        )
        total = total + jnp.dot(rows[s], weight, preferred_element_type=f32)
    gates, ups = total[:, : 2 * ff], total[:, 2 * ff :]
    act = (gates / (1.0 + jnp.exp(-gates)) * ups).astype(bf16)
    tiles = col_width // HD
    for d in range(n_x):
        halves = [
            jnp.concatenate(
                [w[2, pl.ds((d * tiles + t) * ff, ff), :] for t in range(tiles)], 1
            )
            for w in (kept, got)
        ]
        weight = jnp.concatenate(halves, 0)
        out[d] = jnp.dot(act, weight, preferred_element_type=f32).astype(bf16)


def run_expert(rows, kept, got):
    vmem = pl.BlockSpec(memory_space=pltpu.VMEM)
    ff = kept.shape[2]
    return pl.pallas_call(
        expert_kernel,
        out_shape=jax.ShapeDtypeStruct(rows.shape, bf16),
        in_specs=[vmem, vmem, vmem],
        out_specs=vmem,
        cost_estimate=pl.CostEstimate(
            flops=12 * rows.size * ff,
            bytes_accessed=4 * (rows.size + got.size),
            transcendentals=rows.shape[1] * 2 * ff,
        ),
        compiler_params=pltpu.CompilerParams(vmem_limit_bytes=12 << 20),
        name="run_expert",
    )(rows, kept, got)


def layer(
    queries,
    own_kv,
    prompt_cache,
    prompt_len,
    token_prompt,
    residual,
    out_weight,
    route_ids,
    route_weights,
    w_gate,
    w_up,
    w_down,
):
    n_e = lax.axis_size(EXPERT)
    n_x = lax.axis_size("tensor")
    chips = lax.axis_size("chip")
    pos_x = lax.axis_index("tensor")
    chip = lax.axis_index("chip")
    core = lax.axis_index("core")
    pos_e = chip * CORES + core
    tokens = queries.shape[0]
    half_cols = own_kv.shape[1] // 2
    kv_heads = half_cols // HD
    head_count = queries.shape[1] // HD
    group_size = head_count // kv_heads
    heads_here = head_count // n_x
    q_cols = heads_here * HD
    per_prompt = tokens // (n_e // 2)
    model_width = residual.shape[1]
    col_width = model_width // n_x
    picks = route_ids.shape[1]
    experts_here = w_gate.shape[0]
    experts = experts_here * n_e
    capacity = min(tokens, 3 * tokens * picks // (2 * experts))

    by_head = split_cache(prompt_cache, n_x)
    cache_all = exchange(by_head, "tensor")

    mine = out_weight.T[None]
    shift = chips // 2
    while shift > 1:
        mine = jnp.concatenate([mine, along_chips(mine, shift)])
        shift //= 2
    mine_b = along_chips(mine, 1)

    kv_pos = (pos_x * heads_here) // group_size
    earlier = jnp.arange(tokens)[None, :] < jnp.arange(tokens)[:, None]
    chunks = (q_cols + 2 * HD + col_width) // HD
    size = 2 * chunks + picks
    at = jnp.stack([pos_x, kv_pos, kv_heads + kv_pos]).astype(i32)
    sent = build_payload(
        at,
        token_prompt.reshape(1, tokens),
        route_ids.T,
        queries,
        own_kv,
        residual,
        q_cols,
        col_width,
        n_e * size,
    )
    sent, cache_all = lax.optimization_barrier((sent, cache_all))
    got = exchange(sent.reshape(n_e, size, HD), EXPERT)
    table = got[:, 2 * chunks :, :].astype(i32)
    prompts = table[:, 0, tokens : 2 * tokens]
    routes = table[:, :, :tokens]

    owner = jnp.arange(n_e, dtype=i32)
    holds = jnp.any(prompts[None, :, :] == owner[:, None, None], -1)
    order = count_earlier(holds)
    peers = prompts[:, :, None] == prompts[:, None, :]
    rank_all = jnp.sum((peers & earlier[None]).astype(i32), 2)
    block_order = jnp.sum(
        jnp.where(prompts[:, :, None] == owner, order.T[:, None, :], 0), 2
    )
    source = prompts * tokens + block_order * per_prompt + rank_all

    at = jnp.stack([pos_e.astype(i32), prompt_len[0], core.astype(i32)])
    own, resid = attend(
        at, got.reshape(n_e * size, HD), cache_all, tokens, q_cols, col_width
    )
    other = other_core(own)
    at = jnp.stack([chip, core]).astype(i32)
    partial = project_out(at, own, other, mine, mine_b, n_x, col_width // CORES)
    parts = exchange(partial, "tensor")
    hidden = hidden_copies(at, parts, resid, other, chips)

    keep = pos_x % experts_here
    give = 1 - keep
    swap = []
    for i in range(n_x):
        swap.append((i, i ^ 1))
        swap.append((n_x + i, n_x + (i + (1 if i % 2 else -1)) % n_x))
    which = jnp.stack([give, keep]).astype(i32)
    giving, keeping = part_weights(which, w_gate, w_up, w_down)
    got_weights = lax.ppermute(giving, ("core", "tensor"), swap)

    near = exchange(hidden, "chip")
    across = other_core(near)
    mine_e = pos_e * experts_here + jnp.arange(experts_here, dtype=i32)
    named = jnp.any(routes[None] == mine_e[:, None, None, None], 2)
    slot = jnp.where(named, count_earlier(named), -1)
    filled = slot[:, :, None, :] == jnp.arange(capacity, dtype=i32)[None, None, :, None]
    expert_rows = jnp.sum(jnp.where(filled, source[None, :, None, :] + 1, 0), -1) - 1
    home_rows = lax.dynamic_index_in_dim(source, pos_e, 0, keepdims=False)
    by_dest, hidden_home = select_rows(
        at,
        expert_rows.reshape(-1, 1),
        home_rows.reshape(-1, 1),
        near.reshape(n_e * tokens, col_width // CORES),
        across.reshape(n_e * tokens, col_width // CORES),
        n_x,
        experts_here,
    )
    rows_in = exchange(by_dest, "tensor")

    out = run_expert(rows_in, keeping, got_weights)
    parts = exchange(out, "tensor")
    parts = parts.reshape(n_x // experts_here, experts_here, n_e, capacity, col_width)
    summed = jnp.sum(parts.astype(f32), 0).astype(bf16)
    returned = exchange(jnp.transpose(summed, (1, 0, 2, 3)), EXPERT)

    hit = route_ids[:, :, None] == jnp.arange(experts, dtype=i32)
    marks = jnp.any(hit, 1)
    mark_weight = jnp.sum(jnp.where(hit, route_weights[:, :, None], 0.0), 1)
    slot = jnp.dot(
        earlier.astype(bf16), marks.astype(bf16), preferred_element_type=f32
    ).astype(i32)
    slot = jnp.where(marks, slot, -1)
    chosen = slot[:, :, None] == jnp.arange(capacity, dtype=i32)
    mix_rows = (chosen * mark_weight[:, :, None]).reshape(tokens, experts * capacity)
    expert_mix = jnp.dot(
        mix_rows,
        returned.reshape(experts * capacity, col_width).astype(f32),
        precision=lax.Precision.HIGHEST,
    )
    return (hidden_home.astype(f32) + expert_mix).astype(bf16)


def solution(mesh):
    split = Mesh(
        mesh.devices.reshape(
            mesh.shape["groups"],
            mesh.shape["expert"] // CORES,
            CORES,
            mesh.shape["tensor"],
        ),
        ("groups", *EXPERT, "tensor"),
    )
    whole = ("groups", *EXPERT)
    return jax.shard_map(
        layer,
        mesh=split,
        in_specs=(
            P(whole, None),
            P(whole, None),
            P(whole, "tensor", None),
            P(whole),
            P(whole),
            P(whole, None),
            P("tensor", EXPERT),
            P(whole, None),
            P(whole, None),
            P(EXPERT, None, "tensor"),
            P(EXPERT, None, "tensor"),
            P(EXPERT, "tensor", None),
        ),
        out_specs=P(whole, "tensor"),
        check_vma=False,
    )
```
